256 devices in a mesh: rep: 2 (over y), ep: 128 (over x, z, core).
Axes of the slice: x: 4, y: 2, z: 16, core: 2. Of those that a mesh axis runs over, the one named last changes fastest.
The devices are a block of a 4x16x16 slice.
Arguments:
- cache_kv: bfloat16 [512, 2048, 576], P(('rep', 'ep')), parts along dimension 0, may hold values from -6 to 6
- new_kv: bfloat16 [512, 2, 576], P(('rep', 'ep')), parts along dimension 0, may hold values from -6 to 6
- queries: bfloat16 [512, 2, 64, 576], P(('rep', 'ep')), parts along dimension 0, may hold values from -256 to 256
- lengths: int32 [512], P(('rep', 'ep')), parts along dimension 0, may hold values from 256 to 2048
- resid: bfloat16 [512, 2, 7168], P(('rep', 'ep')), parts along dimension 0, may hold values from -18 to 18
- value_up: bfloat16 [512, 8192], P(None, 'ep'), may hold values from -1.5 to 1.5
- out_proj: bfloat16 [8192, 7168], P('ep'), may hold values from -0.09375 to 0.09375
- norm_gain: bfloat16 [7168], replicated, may hold values from 0.25 to 1.75
- router: bfloat16 [7168, 16], replicated, may hold values from -0.0625 to 0.0625
- expert_ids: int32 [512, 2, 8], P(('rep', 'ep')), parts along dimension 0, may hold values from 0 to 15, as said below
- slots: int32 [512, 2, 8], P(('rep', 'ep')), parts along dimension 0, may hold values from 0 to 3, as said below
- w_gate: bfloat16 [7168, 16384], P(None, 'ep'), may hold values from -0.0625 to 0.0625
- w_up: bfloat16 [7168, 16384], P(None, 'ep'), may hold values from -0.0625 to 0.0625
- w_down: bfloat16 [16384, 7168], P('ep'), may hold values from -0.1875 to 0.1875
Outputs:
- mixed: bfloat16 [512, 2, 7168], P(('rep', 'ep')), parts along dimension 0
The draws below stay inside these ranges and needn't reach their ends.
There are 2 independent parts, one for each index of `rep`. The reference program is written for one: setup_inputs(seed, part) draws one part's arguments, and reference() takes and returns one part's arrays. A program takes and returns all parts, laid end to end along the dimension named above; an argument that names none is the same for every part. Nothing has to cross between parts.
Inputs may be any that keep to these rules, and one draw needn't show every extreme that they name: `expert_ids`: each row names 8 different experts. In each aligned block of 4 rows (the rows of one device), the rows that name the same expert carry the distinct slots 0 up to their number minus one for it; in every block some expert is named by all 4 rows.
All inputs are finite; a program needn't handle non-finite values.
Results may differ from the reference program's by a relative error of at most 0.0065.
Values may be sent and summed in bfloat16 or wider, within the bound.
A program may use at most 128 MiB of HBM per device.

```python
import jax
import jax.numpy as jnp
from jax import lax

D = 7168
H = 64
LAT = 512
VH = 128
FFW = 1024
EXPERTS = 16
TOP = 8
CAP = 2
STEPS = 2
CACHE = 2048
KV = 576
QK = 192
TOK_DEV = 4
BATCH = 256
N_EP = 128


def attention_pair(key):
    cache_part = jax.random.truncated_normal(jax.random.fold_in(key, 21), -6.0, 6.0, (BATCH, CACHE, KV), jnp.float32)
    query_part = jax.random.truncated_normal(jax.random.fold_in(key, 22), -6.0, 6.0, (BATCH, STEPS, H, KV), jnp.float32)
    return (cache_part, query_part)


def draw_cache_kv(key, part):
    return attention_pair(key)[0].astype(jnp.bfloat16)


def draw_queries(key, part):
    return attention_pair(key)[1].astype(jnp.bfloat16)


def draw_resid(key, part):
    columns = jnp.exp(jax.random.uniform(jax.random.fold_in(key, 31), (D,), jnp.float32, jnp.log(0.3), jnp.log(3.0)))
    base = jax.random.truncated_normal(jax.random.fold_in(key, 34), -6.0, 6.0, (BATCH, STEPS, D), jnp.float32)
    return (base * columns).astype(jnp.bfloat16)


def routing_pair(key):
    rows_all = BATCH * STEPS
    blocks = rows_all // TOK_DEV
    expert_range = jnp.arange(EXPERTS, dtype=jnp.int32)
    base = jax.random.randint(jax.random.fold_in(key, 41), (rows_all, EXPERTS), 0, 1 << 20)
    order = jax.random.permutation(jax.random.fold_in(key, 42), EXPERTS).astype(jnp.int32)
    forced = jax.random.randint(jax.random.fold_in(key, 43), (blocks,), 0, EXPERTS)
    forced_rows = jnp.repeat(forced, TOK_DEV)
    boost = jnp.where(expert_range[None, :] == forced_rows[:, None], 1 << 24, 0)
    scores = (base + order[None, :] * (1 << 16) + boost) * EXPERTS + expert_range[None, :]
    _, chosen = lax.top_k(scores, TOP)
    chosen = chosen.astype(jnp.int32)
    row_in_block = jnp.arange(rows_all, dtype=jnp.int32) % TOK_DEV
    priority = jax.random.randint(jax.random.fold_in(key, 44), (rows_all, EXPERTS), 0, 1 << 20) * TOK_DEV + row_in_block[:, None]
    named = jnp.any(chosen[:, :, None] == expert_range[None, None, :], axis=1)
    named_block = named.reshape(blocks, TOK_DEV, EXPERTS)
    priority_block = priority.reshape(blocks, TOK_DEV, EXPERTS)
    earlier = named_block[:, None, :, :] & (priority_block[:, None, :, :] < priority_block[:, :, None, :])
    rank = jnp.sum(earlier.astype(jnp.int32), axis=2).reshape(rows_all, EXPERTS)
    slot_values = jnp.take_along_axis(rank, chosen, axis=1)
    return (chosen.reshape(BATCH, STEPS, TOP), slot_values.reshape(BATCH, STEPS, TOP))


def draw_expert_ids(key, part):
    return routing_pair(key)[0]


def draw_slots(key, part):
    return routing_pair(key)[1]


def set_ends(drawn, rng, least, high):
    longest = drawn.shape.index(max(drawn.shape))
    spots = []
    for shift in (0, 1):
        where = [jax.random.randint(jax.random.fold_in(rng, axis), (), 0, length) for axis, length in enumerate(drawn.shape)]
        where[longest] = (where[longest] + shift) % drawn.shape[longest]
        spots.append(tuple(where))
    return drawn.at[spots[0]].set(least).at[spots[1]].set(high)


def steps_of(rng, extent, cuts, smallest, top_value):
    factor_of, own = 1.0, jax.random.fold_in(rng, 6)
    for position, blocks in cuts:
        steps = jnp.exp(jax.random.uniform(jax.random.fold_in(own, position), (blocks,), jnp.float32, smallest / len(cuts), top_value / len(cuts)))
        factor_of = factor_of * jnp.repeat(steps, extent[position] // blocks).reshape([-1 if axis == position else 1 for axis in range(len(extent))])
    return factor_of


def normal_values(own_key, dims, deviation, bound, pieces=(), held_as=jnp.bfloat16):
    loudness = steps_of(own_key, dims, pieces, -0.22, 0.18) if pieces else 1.0
    values = jax.random.normal(own_key, dims, jnp.float32) * deviation * loudness
    return jnp.minimum(jnp.maximum(values, -bound), bound).astype(held_as)


def setup_inputs(seed: int = 0, part: int = 0) -> dict:
    key_list = jax.random.split(jax.random.key(seed), 15)
    part_splits = jax.random.split(jax.random.fold_in(key_list[14], part), 15)
    cache_kv = draw_cache_kv(jax.random.fold_in(jax.random.fold_in(key_list[14], part), 71), part)
    new_kv = normal_values(part_splits[1], (BATCH, STEPS, KV), 1.0, 6.0, ((0, 128),))
    queries = draw_queries(jax.random.fold_in(jax.random.fold_in(key_list[14], part), 71), part)
    lengths = set_ends(jax.random.randint(part_splits[3], (BATCH,), CACHE // 8, CACHE + 1), jax.random.fold_in(part_splits[3], 1), CACHE // 8, CACHE).astype(jnp.int32)
    resid = draw_resid(jax.random.fold_in(jax.random.fold_in(key_list[14], part), 71), part)
    value_up = normal_values(key_list[5], (LAT, H * VH), (max(1, LAT // 32)) ** -0.5, 1.5, ((1, 128),))
    out_proj = normal_values(key_list[6], (H * VH, D), (H * VH // 2) ** -0.5, 0.09375, ((0, 128),))
    norm_gain = jnp.clip(1.0 + 0.15 * jax.random.normal(key_list[7], (D,), jnp.float32), 0.25, 1.75).astype(jnp.bfloat16)
    router = normal_values(key_list[8], (D, EXPERTS), D ** -0.5, 0.0625)
    expert_ids = draw_expert_ids(jax.random.fold_in(jax.random.fold_in(key_list[14], part), 71), part)
    slots = draw_slots(jax.random.fold_in(jax.random.fold_in(key_list[14], part), 71), part)
    w_gate = normal_values(key_list[11], (D, EXPERTS * FFW), D ** -0.5, 0.0625, ((1, 128),))
    w_up = normal_values(key_list[12], (D, EXPERTS * FFW), D ** -0.5, 0.0625, ((1, 128),))
    w_down = normal_values(key_list[13], (EXPERTS * FFW, D), FFW ** -0.5, 0.1875, ((0, 128),))
    return dict(cache_kv=cache_kv, new_kv=new_kv, queries=queries, lengths=lengths, resid=resid, value_up=value_up, out_proj=out_proj, norm_gain=norm_gain, router=router, expert_ids=expert_ids, slots=slots, w_gate=w_gate, w_up=w_up, w_down=w_down)


route_scale = 2.827
norm_eps = 1e-06

def attend_one(packed):
    cache_rows, new_rows, query_rows, length = packed
    score_scale = 1.0 / QK ** 0.5
    query_full = query_rows.astype(jnp.float32)
    cache_full = cache_rows.astype(jnp.float32)
    new_full = new_rows.astype(jnp.float32)
    score_cache = jnp.einsum('shk,pk->shp', query_full, cache_full) * score_scale
    is_live = jnp.arange(CACHE, dtype=jnp.int32) < length
    score_cache = jnp.where(is_live[None, None, :], score_cache, -jnp.inf)
    score_new = jnp.einsum('shk,tk->sht', query_full, new_full) * score_scale
    step_ids = jnp.arange(STEPS, dtype=jnp.int32)
    causal = step_ids[None, :] <= step_ids[:, None]
    score_new = jnp.where(causal[:, None, :], score_new, -jnp.inf)
    row_peak = jnp.maximum(lax.optimization_barrier(jnp.max(score_cache, axis=-1)), lax.optimization_barrier(jnp.max(score_new, axis=-1)))
    exp_cache = jnp.exp(score_cache - row_peak[..., None])
    exp_new = jnp.exp(score_new - row_peak[..., None])
    exp_total = lax.optimization_barrier(jnp.sum(exp_cache, axis=-1)) + lax.optimization_barrier(jnp.sum(exp_new, axis=-1))
    prob_cache = (exp_cache / exp_total[..., None]).astype(jnp.bfloat16)
    prob_new = (exp_new / exp_total[..., None]).astype(jnp.bfloat16)
    context = jnp.einsum('shp,pc->shc', prob_cache.astype(jnp.float32), cache_full[:, :LAT])
    context = context + jnp.einsum('sht,tc->shc', prob_new.astype(jnp.float32), new_full[:, :LAT])
    return context.astype(jnp.bfloat16)

def reference(cache_kv, new_kv, queries, lengths, resid, value_up, out_proj, norm_gain, router, expert_ids, slots, w_gate, w_up, w_down):
    contexts = lax.map(attend_one, (cache_kv, new_kv, queries, lengths))
    values = jnp.einsum('bshc,chv->bshv', contexts.astype(jnp.float32), value_up.reshape(LAT, H, VH).astype(jnp.float32)).astype(jnp.bfloat16)
    rows_all = BATCH * STEPS
    attended = jnp.dot(values.reshape(rows_all, H * VH), out_proj, preferred_element_type=jnp.float32)
    hidden = resid.reshape(rows_all, D).astype(jnp.float32) + attended
    mean_square = lax.optimization_barrier(jnp.mean(hidden * hidden, axis=-1, keepdims=True))
    normed = (hidden * lax.rsqrt(mean_square + norm_eps) * norm_gain.astype(jnp.float32)).astype(jnp.bfloat16)
    logits = jnp.dot(normed, router, preferred_element_type=jnp.float32)
    route_ids = expert_ids.reshape(rows_all, TOP).astype(jnp.int32)
    route_slots = slots.reshape(rows_all, TOP).astype(jnp.int32)
    picked = jnp.take_along_axis(logits, route_ids, axis=1)
    gates = jax.nn.sigmoid(picked)
    weights = route_scale * gates / lax.optimization_barrier(jnp.sum(gates, axis=1, keepdims=True))
    is_kept = route_slots < CAP
    token_index = jnp.broadcast_to(jnp.arange(rows_all, dtype=jnp.int32)[:, None], (rows_all, TOP))
    source = token_index // TOK_DEV
    slot_total = EXPERTS * N_EP * CAP
    flat_slot = route_ids * (N_EP * CAP) + source * CAP + route_slots
    flat_slot = jnp.where(is_kept, flat_slot, slot_total).astype(jnp.int32)
    owner_row = jnp.full((slot_total + 1,), rows_all, dtype=jnp.int32).at[flat_slot.reshape(-1)].set(token_index.reshape(-1))
    share_row = jnp.zeros((slot_total + 1,), jnp.float32).at[flat_slot.reshape(-1)].set(weights.reshape(-1))
    owner_row = owner_row[:slot_total].reshape(EXPERTS, N_EP * CAP)
    share_row = share_row[:slot_total].reshape(EXPERTS, N_EP * CAP)
    padded = jnp.concatenate([normed, jnp.zeros((1, D), jnp.bfloat16)], axis=0)

    def expert_step(expert_mix, packed):
        expert_index, owners, shares = packed
        token_rows = padded[owners]
        gate_cols = lax.dynamic_slice_in_dim(w_gate, expert_index * FFW, FFW, 1)
        up_cols = lax.dynamic_slice_in_dim(w_up, expert_index * FFW, FFW, 1)
        down_rows = lax.dynamic_slice_in_dim(w_down, expert_index * FFW, FFW, 0)
        gate = jnp.dot(token_rows, gate_cols, preferred_element_type=jnp.float32)
        upward = jnp.dot(token_rows, up_cols, preferred_element_type=jnp.float32)
        act = (jax.nn.silu(gate) * upward).astype(jnp.bfloat16)
        produced = jnp.dot(act, down_rows, preferred_element_type=jnp.float32) * shares[:, None]
        return (expert_mix.at[owners].add(produced), None)
    start_mix = jnp.zeros((rows_all + 1, D), jnp.float32)
    expert_mix, _ = lax.scan(expert_step, start_mix, (jnp.arange(EXPERTS, dtype=jnp.int32), owner_row, share_row))
    mixed = (hidden + expert_mix[:rows_all]).astype(jnp.bfloat16)
    return mixed.reshape(BATCH, STEPS, D)
```

```python
import functools
import math

import jax
import jax.numpy as jnp
from jax import lax
from jax.experimental import pallas as pl
from jax.experimental.pallas import tpu as pltpu
from jax.sharding import PartitionSpec as P

NX, NZ, NC = 4, 16, 2
DEV = NX * NC
HALF = NZ // 2

D = 7168
H = 64
LAT = 512
VH = 128
KV = 576
EXPERTS = 16
TOP = 8
CAP = 2
QK = 192
TOK = 4
UNITS = 128
ROW = DEV * TOK
SLOT = DEV * CAP
DX = D // NX
EXT = 128
DC = DX + EXT
JX = DX // 128
MSG = 64
LANE_SUM = 32
LANE_TAB = 64
QUAD = EXPERTS // NX
CHIPS_PER = NZ // QUAD

route_scale = 2.827
norm_eps = 1e-06

SUBS = ((0, 640), (640, 640), (1280, 512))
SUBS_AG = ((0, 640), (640, 640), (1280, 640))
NS = len(SUBS)

F32 = jnp.float32
BF16 = jnp.bfloat16


def mo(value, by):
    return pl.multiple_of(value, by)


def nt(a, b):
    return lax.dot_general(a, b, (((1,), (1,)), ((), ())), preferred_element_type=F32)


def nn(a, b):
    return lax.dot_general(a, b, (((1,), (0,)), ((), ())), preferred_element_type=F32)


def iota(shape, axis):
    return lax.broadcasted_iota(jnp.int32, shape, axis)


def kernel(
    cache_h, new_ref, q_h, len_ref, resid_ref, vu_h, wo_h, gain_ref, router_h, ids_ref, slots_ref, wg_h, wu_h, wd_h,
    out_ref,
    cache_v, q_v, score_v, stage_v, ctx_v, arr_v, arrf_v, vu_v, val_v, wo_v, rs_in, rs_out, hid_v, tab_s, tab_v,
    ress_v, resf_v, res_v, resw_v, rout_v, ag_v, dsp_v, d_v, wgu_v, act_s, act_v, wd_v, rs2_in, rs2_out, fin_v, fin_s, at_v,
    l_cache, l_misc, l_weights,
    s_ctx, s_small, s_w, s_wd, s_val, s_rs, s_ag, s_dsp, s_act, s_rs2, s_out,
    r_ctx, r_small, r_wo, r_vu, r_gu, r_wd, r_val, r_rs, r_ag, r_dsp, r_act, r_rs2, r_out,
    go_sem,
):
    me = lax.axis_index("ep")
    c = lax.rem(me, NC)
    z = lax.rem(me // NC, NZ)
    x = me // (NC * NZ)
    dev = x * NC + c
    quad = z // CHIPS_PER

    def idx(xx, zz, cc):
        return {"ep": (xx * NZ + zz) * NC + cc}

    def wrap(zz):
        return lax.rem(zz + 2 * NZ, NZ)

    def xwrap(xx):
        return lax.rem(xx, NX)

    def send(src, dst, ssem, rsem, to):
        pltpu.make_async_remote_copy(src_ref=src, dst_ref=dst, send_sem=ssem, recv_sem=rsem, device_id=to).start()

    def arrived(ref, sem):
        pltpu.make_async_copy(ref, ref, sem).wait()

    main = c == 1
    side = c == 0

    bar = pltpu.get_barrier_semaphore()

    @pl.when(main)
    def _():
        def greet(i, carry):
            @pl.when(i != me)
            def _():
                pl.semaphore_signal(bar, inc=1, device_id={"ep": i})
            return carry
        lax.fori_loop(0, NX * NZ * NC, greet, 0)

    @pl.when(side)
    def _():
        for xx in range(NX):
            pl.semaphore_signal(bar, inc=1, device_id=idx(xx, z, 1))

    loads = [pltpu.make_async_copy(q_h, q_v, l_misc)]
    loads += [pltpu.make_async_copy(cache_h.at[b], cache_v.at[b], l_cache.at[b]) for b in range(2)]
    for load in loads:
        load.start()

    rows8, lanes8 = iota((8, 128), 0), iota((8, 128), 1)
    table = jnp.zeros((8, 128), F32)
    for t in range(TOK):
        for k in range(TOP):
            hit = (rows8 == t) & (lanes8 == ids_ref[t // 2, t % 2, k] + LANE_TAB)
            table = jnp.where(hit, (slots_ref[t // 2, t % 2, k] + 1).astype(F32), table)
    tab_s[...] = table

    resf_v[...] = jnp.zeros_like(resf_v)
    for t in range(TOK):
        row = resid_ref[t // 2, pl.ds(t % 2, 1), :].astype(F32)
        for xx in range(NX):
            for j in range(JX):
                col = xx * DX + j * 128
                resf_v[pl.ds(xx * MSG + t * JX + j, 1), :] = row[:, col:col + 128]
    ress_v[...] = resf_v[pl.ds(0, NX * MSG), :].reshape(NX, MSG, 128).astype(BF16)

    scale = 1.0 / math.sqrt(QK)
    blk = 512
    nblk = cache_v.shape[2] // blk
    loads[0].wait()
    for b in range(2):
        qb = q_v[b]
        qf = qb.astype(F32)
        step_of = iota((2 * H, 1), 0) // H
        new_rows = [new_ref[b, pl.ds(t, 1), :].astype(F32) for t in range(2)]
        s_new = [jnp.sum(qf * row, axis=1, keepdims=True) * scale for row in new_rows]
        s_new[1] = jnp.where(step_of >= 1, s_new[1], -jnp.inf)
        peak = jnp.maximum(s_new[0], s_new[1])
        loads[1 + b].wait()
        for p in range(nblk):
            sc = nn(qb, cache_v[b, :, pl.ds(p * blk, blk)]) * scale
            pos = iota((2 * H, blk), 1) + p * blk
            sc = jnp.where(pos < len_ref[b], sc, -jnp.inf)
            score_v[:, pl.ds(p * blk, blk)] = sc
            peak = jnp.maximum(peak, jnp.max(sc, axis=1, keepdims=True))
        p_new = [jnp.exp(s - peak) for s in s_new]
        total = p_new[0] + p_new[1]
        acc = p_new[0].astype(BF16).astype(F32) * new_rows[0][:, :LAT]
        acc = acc + p_new[1].astype(BF16).astype(F32) * new_rows[1][:, :LAT]
        for p in range(nblk):
            pr = jnp.exp(score_v[:, pl.ds(p * blk, blk)] - peak)
            total = total + jnp.sum(pr, axis=1, keepdims=True)
            acc = acc + nt(pr.astype(BF16), cache_v[b, pl.ds(0, LAT), pl.ds(p * blk, blk)])
        ctx = acc / total
        for s in range(2):
            for j in range(LAT // 128):
                stage_v[pl.ds(j * TOK + b * 2 + s, H, stride=16), :] = ctx[s * H:(s + 1) * H, j * 128:(j + 1) * 128]
    ctx_v[...] = stage_v[...].reshape(H, 16, 128).astype(BF16)

    @pl.when(main)
    def _():
        pl.semaphore_wait(bar, NX * NZ - 1 + NX)

    @pl.when(side)
    def _():
        pl.semaphore_wait(bar, NX * NZ)

    def ctx_send(o, carry):
        far = HALF - (o + 1) // 2
        zz = wrap(jnp.where(lax.rem(o, 2) == 1, z + far, z - far))
        for i in range(NX):
            xx = xwrap(x + i + 1)
            own = main & (zz == z) & (xx == x)

            @pl.when(jnp.logical_not(own))
            def _():
                send(ctx_v.at[xx * NZ + zz], arr_v.at[z, dev], s_ctx, r_ctx.at[z], idx(xx, zz, 1))

            @pl.when(own)
            def _():
                arr_v[z, dev] = ctx_v[xx * NZ + zz]
        return carry
    lax.fori_loop(0, NZ, ctx_send, 0)

    wo_row = mo(x * VH + c * (VH // NC), VH // NC)
    for xx in range(NX):
        other = jnp.logical_not(main & (x == xx))
        columns = pl.ds(xx * DX, DX)

        @pl.when(other)
        def _():
            send(tab_s, tab_v.at[dev], s_small.at[0], r_small.at[0], idx(xx, z, 1))
            send(ress_v.at[xx], res_v.at[dev], s_small.at[1], r_small.at[1], idx(xx, z, 1))
            send(wo_h.at[:, columns], wo_v.at[pl.ds(wo_row, VH // NC), :], s_w.at[0], r_wo, idx(xx, z, 1))

        @pl.when(jnp.logical_not(other))
        def _():
            tab_v[dev] = tab_s[...]
            res_v[dev] = ress_v[xx]
            pltpu.make_async_copy(wo_h.at[:, columns], wo_v.at[pl.ds(wo_row, VH // NC), :], l_weights.at[0]).start()

    gate_at = pl.ds(mo(c * UNITS, UNITS), UNITS)
    up_at = pl.ds(mo((NC + c) * UNITS, UNITS), UNITS)
    wd_row = mo((x * NC + c) * UNITS, UNITS)

    def wd_send():
        for xx in range(NX):
            columns = pl.ds(xx * DX, DX)
            other = jnp.logical_not(main & (x == xx))

            @pl.when(other)
            def _():
                send(wd_h.at[:, columns], wd_v.at[pl.ds(wd_row, UNITS), :], s_wd, r_wd, idx(xx, z, 1))

            @pl.when(jnp.logical_not(other))
            def _():
                pltpu.make_async_copy(wd_h.at[:, columns], wd_v.at[pl.ds(wd_row, UNITS), :], l_weights.at[3]).start()

    def pick_lanes():
        jj, lane = iota((NX * SLOT, 128), 0), iota((NX * SLOT, 128), 1)
        return jnp.where(lane == LANE_TAB + (jj // SLOT) * QUAD + quad, 1.0, 0.0).astype(BF16)

    @pl.when(main)
    def _main():
        vu_copy = pltpu.make_async_copy(vu_h, vu_v.at[pl.ds(VH // NC, VH // NC), :], l_misc)
        vu_copy.start()
        send(wg_h, wgu_v.at[:, gate_at], s_w.at[1], r_gu, idx(x, z, 0))
        send(wu_h, wgu_v.at[:, up_at], s_w.at[2], r_gu, idx(x, z, 0))
        rout_v[...] = jnp.zeros_like(rout_v)
        rout_copy = pltpu.make_async_copy(
            router_h.at[:, pl.ds(mo(x * DX, 128), DX)], rout_v.at[pl.ds(0, EXPERTS), :], l_weights.at[1]
        )
        rout_copy.start()
        vu_copy.wait()
        arrived(vu_v.at[pl.ds(0, VH // NC), :], r_vu)

        own_lanes = pl.ds(mo(x * VH, VH), VH)

        def ctx_row(r):
            @pl.when(r == z)
            def _():
                arrived(arr_v.at[r, pl.ds(0, DEV - 1)], r_ctx.at[r])

            @pl.when(r != z)
            def _():
                arrived(arr_v.at[r], r_ctx.at[r])

            arrf_v[...] = arr_v[r].reshape(DEV * 16, 128).astype(F32)
            cols = []
            for j in range(LAT // 128):
                cols.append(jnp.concatenate(
                    [arrf_v[pl.ds(j * TOK + t, DEV, stride=16), :] for t in range(TOK)], axis=0))
            rows = jnp.concatenate(cols, axis=1).astype(BF16)
            val_v[r, :, own_lanes] = nt(rows, vu_v[...]).astype(BF16)
            for i in range(NX - 1):
                send(val_v.at[r, :, own_lanes], val_v.at[r, :, own_lanes], s_val, r_val.at[r],
                     idx(xwrap(x + i + 1), z, 1))

        def val_wait(r):
            arrived(val_v.at[r, :, pl.ds(0, (NX - 1) * VH)], r_val.at[r])

        def chain(rows2, weights, in_ref, out_buf, ssem, rsem, s):
            up, down = idx(x, wrap(z + 1), 1), idx(x, wrap(z - 1), 1)
            for i, (o, w) in enumerate(SUBS):
                part = nn(rows2, weights[:, o:o + w])

                @pl.when(s >= 1)
                def _():
                    arrived(in_ref.at[0, s, :, pl.ds(o, w)], rsem.at[0, s, i])
                first = part[:ROW] + in_ref[0, s, :, pl.ds(o, w)].astype(F32)
                out_buf[0, s, :, pl.ds(o, w)] = first.astype(BF16)
                send(out_buf.at[0, s, :, pl.ds(o, w)], in_ref.at[0, s + 1, :, pl.ds(o, w)], ssem.at[0],
                     rsem.at[0, s + 1, i], up)

                @pl.when(s >= 2)
                def _():
                    arrived(in_ref.at[1, s, :, pl.ds(o, w)], rsem.at[1, s, i])

                @pl.when(s >= 1)
                def _():
                    second = part[ROW:] + in_ref[1, s, :, pl.ds(o, w)].astype(F32)
                    out_buf[1, s, :, pl.ds(o, w)] = second.astype(BF16)
                    send(out_buf.at[1, s, :, pl.ds(o, w)], in_ref.at[1, s + 1, :, pl.ds(o, w)], ssem.at[1],
                         rsem.at[1, s + 1, i], down)

        def chain_end(in_ref, rsem, o, w, i):
            for d in range(2):
                arrived(in_ref.at[d, HALF, :, pl.ds(o, w)], rsem.at[d, HALF, i])
            return in_ref[0, HALF, :, pl.ds(o, w)].astype(F32) + in_ref[1, HALF, :, pl.ds(o, w)].astype(F32)

        def chain_zero(in_ref):
            in_ref[0, 0] = jnp.zeros((ROW, DX), BF16)
            in_ref[1, 1] = jnp.zeros((ROW, DX), BF16)

        chain_zero(rs_in)
        chain_zero(rs2_in)

        ctx_row(wrap(z + HALF))
        ctx_row(wrap(z + HALF - 1))
        ctx_row(wrap(z - HALF + 1))
        pltpu.make_async_copy(
            wo_h.at[:, pl.ds(0, DX)], wo_v.at[pl.ds(wo_row, VH // NC), :], l_weights.at[0]).wait()
        arrived(wo_v.at[pl.ds(0, (DEV - 1) * (VH // NC)), :], r_wo)

        def rs_step(s, carry):
            ahead = HALF - 2 - s

            @pl.when(ahead >= 0)
            def _():
                ctx_row(wrap(z + ahead))

            @pl.when(ahead >= 1)
            def _():
                ctx_row(wrap(z - ahead))

            @pl.when(ahead == 0)
            def _():
                pl.semaphore_signal(go_sem, inc=1, device_id=idx(x, z, 0))
                wd_send()
            ra, rb = wrap(z + HALF - s), wrap(z - HALF + s)
            val_wait(ra)

            @pl.when(s >= 1)
            def _():
                val_wait(rb)
            rows2 = jnp.concatenate([val_v[ra], val_v[rb]], axis=0)
            chain(rows2, wo_v, rs_in, rs_out, s_rs, r_rs, s)
            return carry
        lax.fori_loop(0, HALF, rs_step, 0)

        val_wait(z)
        arrived(res_v.at[pl.ds(0, DEV - 1)], r_small.at[1])
        arrived(tab_v.at[pl.ds(0, DEV - 1)], r_small.at[0])
        resw_v[...] = res_v[...].reshape(DEV * MSG, 128).astype(F32)
        own_rows = val_v[z]
        sums = jnp.zeros((ROW, 1), F32)
        for i, (o, w) in enumerate(SUBS):
            part = nn(own_rows, wo_v[:, o:o + w]) + chain_end(rs_in, r_rs, o, w, i)
            res = []
            for j in range(o // 128, (o + w) // 128):
                res.append(jnp.concatenate(
                    [resw_v[pl.ds(t * JX + j, DEV, stride=MSG), :] for t in range(TOK)], axis=0))
            hidden = part + jnp.concatenate(res, axis=1)
            hid_v[:, pl.ds(o, w)] = hidden
            sums = sums + jnp.sum(hidden * hidden, axis=1, keepdims=True)
            gain = gain_ref[:, pl.ds(mo(x * DX + o, 128), w)].astype(F32)
            ag_v[z, :, pl.ds(o, w)] = (hidden * gain).astype(BF16)
        rout_copy.wait()
        logits = nt(ag_v[z, :, pl.ds(0, DX)], rout_v[...])
        lane = iota((ROW, 128), 1)
        high = logits.astype(BF16).astype(F32)
        sums_high = sums.astype(BF16).astype(F32)
        ext = high + pltpu.roll(logits - high, EXPERTS, 1)
        ext = jnp.where(lane == LANE_SUM, sums_high, ext)
        ext = jnp.where(lane == LANE_SUM + 1, sums - sums_high, ext)
        rows = iota((DEV, 128), 0)
        tabs = []
        for t in range(TOK):
            piece = jnp.zeros((DEV, 128), F32)
            for d in range(DEV):
                piece = jnp.where(rows == d, tab_v[d, pl.ds(t, 1), :], piece)
            tabs.append(piece)
        ext = ext + jnp.concatenate(tabs, axis=0)
        ag_v[z, :, pl.ds(DX, EXT)] = ext.astype(BF16)

        up, down = idx(x, wrap(z + 1), 1), idx(x, wrap(z - 1), 1)

        def ag_send(r, i, way):
            o, w = SUBS_AG[i]
            view = ag_v.at[r, :, pl.ds(o, w)]
            send(view, view, s_ag.at[way], r_ag.at[r, i], (up, down)[way])

        def ag_wait(r, i):
            o, w = SUBS_AG[i]
            arrived(ag_v.at[r, :, pl.ds(o, w)], r_ag.at[r, i])

        def dispatch(r):
            picked = nt(pick_lanes(), ag_v[r, :, pl.ds(DX, EXT)])
            jj, tok = iota((NX * SLOT, ROW), 0), iota((NX * SLOT, ROW), 1)
            wanted = (lax.rem(jj, SLOT) // DEV + 1).astype(F32)
            hit = (picked == wanted) & (lax.rem(jj, DEV) == lax.rem(tok, DEV))
            place = jnp.where(hit, 1.0, 0.0).astype(BF16)
            moved = nn(place, ag_v[r]).astype(BF16)
            dsp_v[r] = moved.reshape(NX, SLOT, DC)
            for i in range(NX):
                xx = xwrap(x + i + 1)
                send(dsp_v.at[r, xx], d_v.at[r, x], s_dsp, r_dsp.at[r], idx(xx, z, 0))

        for i in range(NS):
            ag_send(z, i, 0)
            ag_send(z, i, 1)
        dispatch(z)

        def ag_step(k, carry):
            ra, rb = wrap(z - k), wrap(z + k)
            for i in range(NS):
                ag_wait(ra, i)

                @pl.when(k < HALF)
                def _():
                    ag_send(ra, i, 0)
                    ag_wait(rb, i)

                @pl.when(k < HALF - 1)
                def _():
                    ag_send(rb, i, 1)
            dispatch(ra)

            @pl.when(k < HALF)
            def _():
                dispatch(rb)
            return carry
        lax.fori_loop(1, HALF + 1, ag_step, 0)

        pltpu.make_async_copy(
            wd_h.at[:, pl.ds(0, DX)], wd_v.at[pl.ds(wd_row, UNITS), :], l_weights.at[3]).wait()
        arrived(wd_v.at[pl.ds(0, (DEV - 1) * UNITS), :], r_wd)

        def act_rows(r):
            arrived(act_v.at[r], r_act.at[r])
            picked = nt(ag_v[r, :, pl.ds(DX, EXT)], pick_lanes())
            jj, tok = iota((ROW, NX * SLOT), 1), iota((ROW, NX * SLOT), 0)
            wanted = (lax.rem(jj, SLOT) // DEV + 1).astype(F32)
            hit = (picked == wanted) & (lax.rem(jj, DEV) == lax.rem(tok, DEV))
            place = jnp.where(hit, 1.0, 0.0).astype(BF16)
            return jnp.concatenate(
                [nn(place[:, i * SLOT:(i + 1) * SLOT], act_v[r, i]).astype(BF16) for i in range(NX)], axis=1)

        def rs2_step(s, carry):
            ra, rb = wrap(z + HALF - s), wrap(z - HALF + s)
            at_v[pl.ds(0, ROW), :] = act_rows(ra)

            @pl.when(s >= 1)
            def _():
                at_v[pl.ds(ROW, ROW), :] = act_rows(rb)
            chain(at_v[...], wd_v, rs2_in, rs2_out, s_rs2, r_rs2, s)
            return carry
        at_v[...] = jnp.zeros_like(at_v)
        lax.fori_loop(0, HALF, rs2_step, 0)

        rows_own = act_rows(z)
        for i, (o, w) in enumerate(SUBS):
            mixed = nn(rows_own, wd_v[:, o:o + w]) + chain_end(rs2_in, r_rs2, o, w, i) + hid_v[:, pl.ds(o, w)]
            for t in range(TOK):
                for j in range(o // 128, (o + w) // 128):
                    fin_v[pl.ds(t * JX + j, DEV, stride=MSG), :] = (
                        mixed[t * DEV:(t + 1) * DEV, j * 128 - o:j * 128 - o + 128])
        for t in range(TOK * JX, MSG):
            fin_v[pl.ds(t, DEV, stride=MSG), :] = jnp.zeros((DEV, 128), F32)
        fin_s[...] = fin_v[...].reshape(DEV, MSG, 128).astype(BF16)
        for i in range(DEV):
            to = lax.rem(dev + i + 1, DEV)

            if i < DEV - 1:
                send(fin_s.at[to], out_ref.at[x], s_out, r_out, idx(to // NC, z, lax.rem(to, NC)))
        out_ref[x] = fin_s[dev]
        arrived(out_ref.at[pl.ds(0, NX - 1)], r_out)

        arrived(ctx_v.at[pl.ds(0, NX * NZ - 1)], s_ctx)
        arrived(tab_v.at[pl.ds(0, NX - 1)], s_small.at[0])
        arrived(res_v.at[pl.ds(0, NX - 1)], s_small.at[1])
        arrived(wo_v.at[pl.ds(0, (NX - 1) * (VH // NC)), :], s_w.at[0])
        arrived(wgu_v.at[:, pl.ds(0, UNITS)], s_w.at[1])
        arrived(wgu_v.at[:, pl.ds(0, UNITS)], s_w.at[2])
        arrived(wd_v.at[pl.ds(0, (NX - 1) * UNITS), :], s_wd)
        arrived(val_v.at[:, :, pl.ds(0, (NX - 1) * VH)], s_val)
        for buf, sem in ((rs_out, s_rs), (rs2_out, s_rs2)):
            arrived(buf.at[0], sem.at[0])
            arrived(buf.at[1, pl.ds(1, HALF - 1)], sem.at[1])
        arrived(ag_v.at[pl.ds(0, HALF)], s_ag.at[0])
        arrived(ag_v.at[pl.ds(0, HALF - 1)], s_ag.at[1])
        arrived(dsp_v, s_dsp)
        arrived(fin_s.at[pl.ds(0, DEV - 1)], s_out)

    @pl.when(side)
    def _side():
        send(vu_h, vu_v.at[pl.ds(0, VH // NC), :], s_small.at[2], r_vu, idx(x, z, 1))
        own = [
            pltpu.make_async_copy(wg_h, wgu_v.at[:, gate_at], l_weights.at[1]),
            pltpu.make_async_copy(wu_h, wgu_v.at[:, up_at], l_weights.at[2]),
        ]
        for copy in own:
            copy.start()
        pl.semaphore_wait(go_sem, 1)
        wd_send()
        for copy in own:
            copy.wait()
        arrived(wgu_v.at[:, pl.ds(0, NC * UNITS)], r_gu)

        own_expert = x * QUAD + quad

        def experts(rows):
            for r in rows:
                arrived(d_v.at[r], r_dsp.at[r])
            both = jnp.zeros((SLOT * len(rows), 2 * NC * UNITS), F32)
            ext = jnp.zeros((SLOT * len(rows), EXT), F32)
            for xx in range(NX):
                both = both + nn(
                    jnp.concatenate([d_v[r, xx, :, pl.ds(0, DX)] for r in rows], axis=0),
                    wgu_v[xx * DX:(xx + 1) * DX, :])
                piece = jnp.concatenate([d_v[r, xx, :, pl.ds(DX, EXT)] for r in rows], axis=0).astype(F32)
                ext = ext + piece
            lane = iota(ext.shape, 1)
            squares = jnp.sum(
                jnp.where((lane == LANE_SUM) | (lane == LANE_SUM + 1), ext, 0.0), axis=1, keepdims=True)
            inv = lax.rsqrt(squares / D + norm_eps)
            logits = (ext + pltpu.roll(ext, EXT - EXPERTS, 1)) * inv
            named = (pltpu.roll(piece, EXT - LANE_TAB, 1) > 0.0) & (lane < EXPERTS)
            gates = jnp.where(named, 1.0 / (1.0 + jnp.exp(-logits)), 0.0)
            norm = jnp.sum(gates, axis=1, keepdims=True)
            mine = jnp.sum(jnp.where(lane == own_expert, gates, 0.0), axis=1, keepdims=True)
            share = jnp.where(norm > 0.0, route_scale * mine / norm, 0.0)
            gate = both[:, :NC * UNITS] * inv
            upward = both[:, NC * UNITS:] * inv
            act = (gate / (1.0 + jnp.exp(-gate)) * upward * share).astype(BF16)
            for i, r in enumerate(rows):
                act_s[r] = act[i * SLOT:(i + 1) * SLOT]
                for n in range(NX):
                    send(act_s.at[r], act_v.at[r, x], s_act, r_act.at[r], idx(xwrap(x + n), z, 1))

        experts([z])

        def step(k, carry):
            experts([wrap(z - k), wrap(z + k)])
            return carry
        lax.fori_loop(1, HALF, step, 0)
        experts([wrap(z + HALF)])

        arrived(out_ref, r_out)
        arrived(ctx_v, s_ctx)
        arrived(tab_v.at[pl.ds(0, NX)], s_small.at[0])
        arrived(res_v.at[pl.ds(0, NX)], s_small.at[1])
        arrived(vu_v.at[pl.ds(0, VH // NC), :], s_small.at[2])
        arrived(wo_v.at[pl.ds(0, NX * (VH // NC)), :], s_w.at[0])
        arrived(wd_v.at[pl.ds(0, NX * UNITS), :], s_wd)
        arrived(act_v, s_act)


def body(
    cache_kv, new_kv, queries, lengths, resid, value_up, out_proj, norm_gain, router, expert_ids, slots, w_gate, w_up,
    w_down,
):
    seqs, steps = resid.shape[:2]
    cache_len = cache_kv.shape[1]
    hbm = pl.BlockSpec(memory_space=pltpu.HBM)
    vmem = pl.BlockSpec(memory_space=pltpu.VMEM)
    smem = pl.BlockSpec(memory_space=pltpu.SMEM)
    dma = pltpu.SemaphoreType.DMA
    scratch = [
        pltpu.VMEM((seqs, KV, cache_len), BF16),
        pltpu.VMEM((seqs, steps * H, KV), BF16),
        pltpu.VMEM((steps * H, cache_len), F32),
        pltpu.VMEM((H * 16, 128), F32),
        pltpu.VMEM((H, 16, 128), BF16),
        pltpu.VMEM((NZ, DEV, 16, 128), BF16),
        pltpu.VMEM((DEV * 16, 128), F32),
        pltpu.VMEM((VH, LAT), BF16),
        pltpu.VMEM((NZ, ROW, NX * VH), BF16),
        pltpu.VMEM((NX * VH, DX), BF16),
        pltpu.VMEM((2, HALF + 1, ROW, DX), BF16),
        pltpu.VMEM((2, HALF, ROW, DX), BF16),
        pltpu.VMEM((ROW, DX), F32),
        pltpu.VMEM((8, 128), F32),
        pltpu.VMEM((DEV, 8, 128), F32),
        pltpu.VMEM((NX, MSG, 128), BF16),
        pltpu.VMEM((NX * MSG, 128), F32),
        pltpu.VMEM((DEV, MSG, 128), BF16),
        pltpu.VMEM((DEV * MSG, 128), F32),
        pltpu.VMEM((128, DX), BF16),
        pltpu.VMEM((NZ, ROW, DC), BF16),
        pltpu.VMEM((NZ, NX, SLOT, DC), BF16),
        pltpu.VMEM((NZ, NX, SLOT, DC), BF16),
        pltpu.VMEM((D, 2 * NC * UNITS), BF16),
        pltpu.VMEM((NZ, SLOT, NC * UNITS), BF16),
        pltpu.VMEM((NZ, NX, SLOT, NC * UNITS), BF16),
        pltpu.VMEM((NX * NC * UNITS, DX), BF16),
        pltpu.VMEM((2, HALF + 1, ROW, DX), BF16),
        pltpu.VMEM((2, HALF, ROW, DX), BF16),
        pltpu.VMEM((DEV * MSG, 128), F32),
        pltpu.VMEM((DEV, MSG, 128), BF16),
        pltpu.VMEM((2 * ROW, NX * NC * UNITS), BF16),
        dma((seqs,)), dma, dma((4,)),
        dma, dma((3,)), dma((3,)), dma, dma, dma((2,)), dma((2,)), dma, dma, dma((2,)), dma,
        dma((NZ,)), dma((2,)), dma, dma, dma, dma, dma((NZ,)), dma((2, HALF + 1, NS)), dma((NZ, NS)), dma((NZ,)),
        dma((NZ,)), dma((2, HALF + 1, NS)), dma,
        pltpu.SemaphoreType.REGULAR,
    ]
    out = pl.pallas_call(
        kernel,
        out_shape=jax.ShapeDtypeStruct((NX, MSG, 128), BF16),
        in_specs=[hbm, vmem, hbm, smem, vmem, hbm, hbm, vmem, hbm, smem, smem, hbm, hbm, hbm],
        out_specs=vmem,
        scratch_shapes=scratch,
        compiler_params=pltpu.CompilerParams(
            collective_id=0, has_side_effects=True, vmem_limit_bytes=(64 << 20) - (64 << 10)),
        name="layer",
    )(
        jnp.transpose(cache_kv, (0, 2, 1)), new_kv, queries.reshape(seqs, steps * H, KV), lengths, resid,
        value_up.T, out_proj, norm_gain.reshape(1, D), router.T, expert_ids, slots, w_gate, w_up, w_down,
    )
    out = out[:, :TOK * JX].reshape(NX, TOK, JX, 128).transpose(1, 0, 2, 3)
    return out.reshape(resid.shape)


def solution(mesh):
    return jax.shard_map(
        body,
        mesh=mesh,
        in_specs=(
            P(("rep", "ep"), None, None),
            P(("rep", "ep"), None, None),
            P(("rep", "ep"), None, None, None),
            P(("rep", "ep")),
            P(("rep", "ep"), None, None),
            P(None, "ep"),
            P("ep", None),
            P(),
            P(),
            P(("rep", "ep"), None, None),
            P(("rep", "ep"), None, None),
            P(None, "ep"),
            P(None, "ep"),
            P("ep", None),
        ),
        out_specs=P(("rep", "ep"), None, None),
        check_vma=False,
    )
```

```python
import functools
import math

import jax
import jax.numpy as jnp
from jax import lax
from jax.experimental import pallas as pl
from jax.experimental.pallas import tpu as pltpu
from jax.sharding import PartitionSpec as P

NX, NZ, NC = 4, 16, 2
DEV = NX * NC
HALF = NZ // 2

D = 7168
H = 64
LAT = 512
VH = 128
KV = 576
EXPERTS = 16
TOP = 8
CAP = 2
QK = 192
TOK = 4
UNITS = 128
ROW = DEV * TOK
SLOT = DEV * CAP
DX = D // NX
EXT = 128
DC = DX + EXT
JX = DX // 128
MSG = 64
LANE_SUM = 32
LANE_TAB = 64
QUAD = EXPERTS // NX
CHIPS_PER = NZ // QUAD

route_scale = 2.827
norm_eps = 1e-06

CUBE = 4

SUBS = tuple((256 * i, 256) for i in range(DX // 256))
SUBS_AG = SUBS[:-1] + ((SUBS[-1][0], SUBS[-1][1] + EXT),)
BLOCKS = ((0, 512), (512, 512), (1024, 768))
NS = len(SUBS)

F32 = jnp.float32
BF16 = jnp.bfloat16


def mo(value, by):
    return pl.multiple_of(value, by)


def nt(a, b):
    return lax.dot_general(a, b, (((1,), (1,)), ((), ())), preferred_element_type=F32)


def nn(a, b):
    return lax.dot_general(a, b, (((1,), (0,)), ((), ())), preferred_element_type=F32)


def iota(shape, axis):
    return lax.broadcasted_iota(jnp.int32, shape, axis)


def kernel(
    cache_h, new_ref, q_h, len_ref, resid_ref, vu_h, wo_h, gain_ref, router_h, ids_ref, slots_ref, wg_h, wu_h, wd_h,
    out_ref,
    cache_v, q_v, score_v, stage_v, ctx_v, arr_v, arrf_v, vu_v, val_v, wo_v, rs_in, rs_out, hid_v, tab_s, tab_v,
    ress_v, resf_v, res_v, resw_v, gain_v, rout_v, ag_v, dsp_v, d_v, wgu_v, act_s, act_v, wd_v, wdn_v, rs2_in, rs2_out,
    part_v, fin_v, fin_s,
    l_cache, l_misc, l_weights,
    s_ctx, s_tab, s_res, s_wo, s_core, s_wd, s_val, s_rs, s_ag, s_rs2, s_dsp, s_act, s_out,
    r_tab, r_res, r_wo, r_core, r_wd, r_row, r_ring, r_out,
    row_sem, all_sem,
):
    me = lax.axis_index("ep")
    c = lax.rem(me, NC)
    z = lax.rem(me // NC, NZ)
    x = me // (NC * NZ)
    dev = x * NC + c
    quad = z // CHIPS_PER

    def idx(xx, zz, cc):
        return {"ep": (xx * NZ + zz) * NC + cc}

    def wrap(zz):
        return lax.rem(zz + 2 * NZ, NZ)

    def xwrap(xx):
        return lax.rem(xx, NX)

    def send(src, dst, ssem, rsem, to):
        pltpu.make_async_remote_copy(src_ref=src, dst_ref=dst, send_sem=ssem, recv_sem=rsem, device_id=to).start()

    def arrived(ref, sem):
        pltpu.make_async_copy(ref, ref, sem).wait()

    main = c == 1
    side = c == 0

    loads = [pltpu.make_async_copy(q_h, q_v, l_misc)]
    loads += [pltpu.make_async_copy(cache_h.at[b], cache_v.at[b], l_cache.at[b]) for b in range(2)]
    for load in loads:
        load.start()

    bar = pltpu.get_barrier_semaphore()

    @pl.when(side)
    def _():
        def greet(o, carry):
            far = HALF - (o + 1) // 2
            zz = wrap(jnp.where(lax.rem(o, 2) == 1, z + far, z - far))
            for xx in range(NX):
                pl.semaphore_signal(bar, inc=1, device_id=idx(xx, zz, 1))
            return carry
        lax.fori_loop(0, NZ, greet, 0)

    @pl.when(main)
    def _():
        for xx in range(NX):
            pl.semaphore_signal(bar, inc=1, device_id=idx(xx, z, 0))
        for step in (1, -1):
            pl.semaphore_signal(bar, inc=1, device_id=idx(x, wrap(z + step), 1))

    wo_row = mo(x * VH + c * (VH // NC), VH // NC)
    gate_at = pl.ds(mo(c * UNITS, UNITS), UNITS)
    up_at = pl.ds(mo((NC + c) * UNITS, UNITS), UNITS)
    vu_at = pl.ds(mo(c * (VH // NC), VH // NC), VH // NC)
    router_copy = pltpu.make_async_copy(
        router_h.at[:, pl.ds(mo(x * DX, 128), DX)], rout_v.at[pl.ds(0, EXPERTS), :], l_weights.at[1])
    gate_copy = pltpu.make_async_copy(wg_h, wgu_v.at[:, gate_at], l_weights.at[1])
    up_copy = pltpu.make_async_copy(wu_h, wgu_v.at[:, up_at], l_weights.at[2])
    vu_copy = pltpu.make_async_copy(vu_h, vu_v.at[vu_at, :], l_weights.at[0])

    def row_start():
        @pl.when(side)
        def _():
            pl.semaphore_wait(bar, NX)
            pl.semaphore_signal(row_sem, inc=1, device_id=idx(x, z, 1))

        @pl.when(main)
        def _():
            pl.semaphore_wait(row_sem, 1)

        for xx in range(NX):
            other = jnp.logical_not(main & (x == xx))
            columns = pl.ds(xx * DX, DX)

            @pl.when(other)
            def _():
                send(wo_h.at[:, columns], wo_v.at[pl.ds(wo_row, VH // NC), :], s_wo, r_wo, idx(xx, z, 1))

            @pl.when(jnp.logical_not(other))
            def _():
                pltpu.make_async_copy(
                    wo_h.at[:, columns], wo_v.at[pl.ds(wo_row, VH // NC), :], l_weights.at[0]).start()

        @pl.when(main)
        def _():
            partner = idx(x, z, 0)
            send(vu_h, vu_v.at[vu_at, :], s_core.at[0], r_core.at[0], partner)
            send(wd_h, wdn_v, s_core.at[1], r_core.at[1], partner)
            send(wg_h, wgu_v.at[:, gate_at], s_core.at[2], r_core.at[2], partner)
            send(wu_h, wgu_v.at[:, up_at], s_core.at[3], r_core.at[3], partner)
            rout_v[...] = jnp.zeros_like(rout_v)
            router_copy.start()

        @pl.when(side)
        def _():
            vu_copy.start()
            gate_copy.start()
            up_copy.start()

    scale = 1.0 / math.sqrt(QK)
    blk = 512
    nblk = cache_v.shape[2] // blk
    loads[0].wait()
    for b in range(2):
        if b == 1:
            row_start()
        qb = q_v[b]
        qf = qb.astype(F32)
        step_of = iota((2 * H, 1), 0) // H
        new_rows = [new_ref[b, pl.ds(t, 1), :].astype(F32) for t in range(2)]
        s_new = [jnp.sum(qf * row, axis=1, keepdims=True) * scale for row in new_rows]
        s_new[1] = jnp.where(step_of >= 1, s_new[1], -jnp.inf)
        peak = jnp.maximum(s_new[0], s_new[1])
        loads[1 + b].wait()
        for p in range(nblk):
            sc = nn(qb, cache_v[b, :, pl.ds(p * blk, blk)]) * scale
            pos = iota((2 * H, blk), 1) + p * blk
            sc = jnp.where(pos < len_ref[b], sc, -jnp.inf)
            score_v[:, pl.ds(p * blk, blk)] = sc
            peak = jnp.maximum(peak, jnp.max(sc, axis=1, keepdims=True))
        p_new = [jnp.exp(s - peak) for s in s_new]
        total = p_new[0] + p_new[1]
        acc = p_new[0].astype(BF16).astype(F32) * new_rows[0][:, :LAT]
        acc = acc + p_new[1].astype(BF16).astype(F32) * new_rows[1][:, :LAT]
        for p in range(nblk):
            pr = jnp.exp(score_v[:, pl.ds(p * blk, blk)] - peak)
            total = total + jnp.sum(pr, axis=1, keepdims=True)
            acc = acc + nt(pr.astype(BF16), cache_v[b, pl.ds(0, LAT), pl.ds(p * blk, blk)])
        ctx = acc / total
        for s in range(2):
            for j in range(LAT // 128):
                stage_v[pl.ds(j * TOK + b * 2 + s, H, stride=16), :] = ctx[s * H:(s + 1) * H, j * 128:(j + 1) * 128]
    ctx_v[...] = stage_v[...].reshape(H, 16, 128).astype(BF16)

    @pl.when(main)
    def _():
        pl.semaphore_wait(bar, NX * NZ + 2)
        pl.semaphore_signal(all_sem, inc=1, device_id=idx(x, z, 0))

    @pl.when(side)
    def _():
        pl.semaphore_wait(all_sem, 1)

    def ctx_send(o, carry):
        far = HALF - (o + 1) // 2
        zz = wrap(jnp.where(lax.rem(o, 2) == 1, z + far, z - far))
        for i in range(NX):
            xx = xwrap(x + i + 1)
            own = side & (zz == z) & (xx == x)

            @pl.when(jnp.logical_not(own))
            def _():
                send(ctx_v.at[xx * NZ + zz], arr_v.at[z, dev], s_ctx, r_row.at[z], idx(xx, zz, 0))

            @pl.when(own)
            def _():
                arr_v[z, dev] = ctx_v[xx * NZ + zz]
        return carry
    lax.fori_loop(0, NZ, ctx_send, 0)

    rows8, lanes8 = iota((8, 128), 0), iota((8, 128), 1)
    table = jnp.zeros((8, 128), F32)
    for t in range(TOK):
        for k in range(TOP):
            hit = (rows8 == t) & (lanes8 == ids_ref[t // 2, t % 2, k] + LANE_TAB)
            table = jnp.where(hit, (slots_ref[t // 2, t % 2, k] + 1).astype(F32), table)
    tab_s[...] = table

    resf_v[...] = jnp.zeros_like(resf_v)
    for t in range(TOK):
        row = resid_ref[t // 2, pl.ds(t % 2, 1), :].astype(F32)
        for xx in range(NX):
            for j in range(JX):
                col = xx * DX + j * 128
                resf_v[pl.ds(xx * MSG + t * JX + j, 1), :] = row[:, col:col + 128]
    ress_v[...] = resf_v[...].reshape(NX, MSG, 128).astype(BF16)

    for xx in range(NX):
        other = jnp.logical_not(main & (x == xx))

        @pl.when(other)
        def _():
            send(tab_s, tab_v.at[dev], s_tab, r_tab, idx(xx, z, 1))
            send(ress_v.at[xx], res_v.at[dev], s_res, r_res, idx(xx, z, 1))

        @pl.when(jnp.logical_not(other))
        def _():
            tab_v[dev] = tab_s[...]
            res_v[dev] = ress_v[xx]

    def up_down(k):
        return wrap(z - k), wrap(z + k)

    @pl.when(side)
    def _side():
        vu_copy.wait()
        arrived(vu_v.at[pl.ds(0, VH // NC), :], r_core.at[0])
        own_lanes = pl.ds(mo(x * VH, VH), VH)

        def ctx_row(r):
            @pl.when(r == z)
            def _():
                arrived(arr_v.at[r, pl.ds(0, DEV - 1)], r_row.at[r])

            @pl.when(r != z)
            def _():
                arrived(arr_v.at[r], r_row.at[r])

            arrf_v[...] = arr_v[r].reshape(DEV * 16, 128).astype(F32)
            cols = []
            for j in range(LAT // 128):
                cols.append(jnp.concatenate(
                    [arrf_v[pl.ds(j * TOK + t, DEV, stride=16), :] for t in range(TOK)], axis=0))
            rows = jnp.concatenate(cols, axis=1).astype(BF16)
            val_v[r, :, own_lanes] = nt(rows, vu_v[...]).astype(BF16)
            view = val_v.at[r, :, own_lanes]
            for i in range(NX):
                send(view, view, s_val, r_row.at[r], idx(xwrap(x + i + 1), z, 1))

        def ctx_step(o, carry):
            far = HALF - (o + 1) // 2
            ctx_row(wrap(jnp.where(lax.rem(o, 2) == 1, z + far, z - far)))
            return carry
        lax.fori_loop(0, NZ, ctx_step, 0)

        arrived(wdn_v, r_core.at[1])
        for i in range(NX):
            xx = xwrap(x + i + 1)
            columns = pl.ds(mo(xx * DX, 128), DX)
            base = x * NC * UNITS
            send(wd_h.at[:, columns], wd_v.at[pl.ds(mo(base, UNITS), UNITS), :], s_wd, r_wd, idx(xx, z, 1))
            send(wdn_v.at[:, columns], wd_v.at[pl.ds(mo(base + UNITS, UNITS), UNITS), :], s_wd, r_wd, idx(xx, z, 1))

        gate_copy.wait()
        up_copy.wait()
        arrived(wgu_v.at[:, pl.ds(0, UNITS)], r_core.at[2])
        arrived(wgu_v.at[:, pl.ds(0, UNITS)], r_core.at[3])

        own_expert = x * QUAD + quad

        def experts(rows):
            for r in rows:
                arrived(d_v.at[r], r_row.at[r])
            both = jnp.zeros((SLOT * len(rows), 2 * NC * UNITS), F32)
            ext = jnp.zeros((SLOT * len(rows), EXT), F32)
            for xx in range(NX):
                both = both + nn(
                    jnp.concatenate([d_v[r, xx, :, pl.ds(0, DX)] for r in rows], axis=0),
                    wgu_v[xx * DX:(xx + 1) * DX, :])
                piece = jnp.concatenate([d_v[r, xx, :, pl.ds(DX, EXT)] for r in rows], axis=0).astype(F32)
                ext = ext + piece
            lane = iota(ext.shape, 1)
            squares = jnp.sum(
                jnp.where((lane == LANE_SUM) | (lane == LANE_SUM + 1), ext, 0.0), axis=1, keepdims=True)
            inv = lax.rsqrt(squares / D + norm_eps)
            logits = (ext + pltpu.roll(ext, EXT - EXPERTS, 1)) * inv
            named = (pltpu.roll(piece, EXT - LANE_TAB, 1) > 0.0) & (lane < EXPERTS)
            gates = jnp.where(named, 1.0 / (1.0 + jnp.exp(-logits)), 0.0)
            norm = jnp.sum(gates, axis=1, keepdims=True)
            mine = jnp.sum(jnp.where(lane == own_expert, gates, 0.0), axis=1, keepdims=True)
            share = jnp.where(norm > 0.0, route_scale * mine / norm, 0.0)
            gate = both[:, :NC * UNITS] * inv
            upward = both[:, NC * UNITS:] * inv
            act = (gate / (1.0 + jnp.exp(-gate)) * upward * share).astype(BF16)
            for i, r in enumerate(rows):
                act_s[r] = act[i * SLOT:(i + 1) * SLOT]
                for n in range(NX):
                    send(act_s.at[r], act_v.at[r, x], s_act, r_row.at[r], idx(xwrap(x + n + 1), z, 1))

        experts([z])

        def step(k, carry):
            experts(list(up_down(k)))
            return carry
        lax.fori_loop(1, HALF, step, 0)
        experts([wrap(z + HALF)])

        arrived(out_ref, r_out)
        arrived(ctx_v.at[pl.ds(0, NX * NZ - 1)], s_ctx)
        arrived(wo_v.at[pl.ds(0, NX * (VH // NC)), :], s_wo)
        arrived(tab_v.at[pl.ds(0, NX)], s_tab)
        arrived(res_v.at[pl.ds(0, NX)], s_res)
        arrived(wd_v, s_wd)
        arrived(val_v, s_val)
        arrived(act_v, s_act)

    @pl.when(main)
    def _main():
        up = idx(x, wrap(z + 1), 1)
        gain_v[...] = gain_ref[...].astype(F32)

        early = jnp.where(lax.rem(z, CUBE) == 0, 1, 0)

        def ways():
            for way in (early, 1 - early):
                yield way, idx(x, wrap(z + 1 - 2 * way), 1)

        def chain_step(in_ref, out_buf, ssem, s):
            for i, (o, w) in enumerate(SUBS):
                at = pl.ds(o, w)
                for way, to in ways():
                    r = wrap(z + (1 - 2 * way) * (HALF - s))

                    @pl.when((way == 0) | (s >= 2))
                    def _():
                        arrived(in_ref.at[way, s, :, at], r_ring.at[way, s, i])
                    total = part_v[r, :, at] + in_ref[way, s, :, at].astype(F32)
                    out_buf[way, s, :, at] = total.astype(BF16)
                    send(out_buf.at[way, s, :, at], in_ref.at[way, s + 1, :, at], ssem.at[way],
                         r_ring.at[way, s + 1, i], to)

        def chain_first(in_ref, out_buf, ssem, rows, weights):
            for o, w in BLOCKS:
                out_buf[0, 0, :, pl.ds(o, w)] = nn(rows, weights[:, o:o + w]).astype(BF16)
                for i in range(o // 256, (o + w) // 256):
                    at = pl.ds(*SUBS[i])
                    send(out_buf.at[0, 0, :, at], in_ref.at[0, 1, :, at], ssem.at[0], r_ring.at[0, 1, i], up)

        def chain_end(in_ref, o, w, i):
            at = pl.ds(o, w)
            for d in range(2):
                arrived(in_ref.at[d, HALF, :, at], r_ring.at[d, HALF, i])
            return part_v[z, :, at] + in_ref[0, HALF, :, at].astype(F32) + in_ref[1, HALF, :, at].astype(F32)

        rs_in[1, 1] = jnp.zeros((ROW, DX), BF16)
        rs2_in[1, 1] = jnp.zeros((ROW, DX), BF16)

        pltpu.make_async_copy(
            wo_h.at[:, pl.ds(0, DX)], wo_v.at[pl.ds(wo_row, VH // NC), :], l_weights.at[0]).wait()
        arrived(wo_v.at[pl.ds(0, (DEV - 1) * (VH // NC)), :], r_wo)

        def attended(rows):
            for r in rows:
                arrived(val_v.at[r], r_row.at[r])
            stacked = jnp.concatenate([val_v[r] for r in rows], axis=0)
            for o, w in BLOCKS:
                part = nn(stacked, wo_v[:, o:o + w])
                for i, r in enumerate(rows):
                    part_v[r, :, pl.ds(o, w)] = part[i * ROW:(i + 1) * ROW]

        first = wrap(z + HALF)
        arrived(val_v.at[first], r_row.at[first])
        chain_first(rs_in, rs_out, s_rs, val_v[first], wo_v)
        attended(list(up_down(HALF - 1)))

        def rs_step(s, carry):
            chain_step(rs_in, rs_out, s_rs, s)
            ahead = HALF - 1 - s

            @pl.when(ahead >= 1)
            def _():
                attended(list(up_down(ahead)))
            return carry
        lax.fori_loop(1, HALF, rs_step, 0)
        attended([z])

        arrived(res_v.at[pl.ds(0, DEV - 1)], r_res)
        arrived(tab_v.at[pl.ds(0, DEV - 1)], r_tab)
        resw_v[...] = res_v[...].reshape(DEV * MSG, 128).astype(F32)
        for j in range(JX):
            at = pl.ds(j * 128, 128)
            part_v[z, :, at] = part_v[z, :, at] + jnp.concatenate(
                [resw_v[pl.ds(t * JX + j, DEV, stride=MSG), :] for t in range(TOK)], axis=0)
        lane = iota((ROW, 128), 1)
        rows = iota((DEV, 128), 0)
        tabs = []
        for t in range(TOK):
            piece = jnp.zeros((DEV, 128), F32)
            for d in range(DEV):
                piece = jnp.where(rows == d, tab_v[d, pl.ds(t, 1), :], piece)
            tabs.append(piece)
        table_rows = jnp.concatenate(tabs, axis=0)
        router_copy.wait()

        def ag_send(r, i, way, slot):
            o, w = SUBS_AG[i]
            view = ag_v.at[r, :, pl.ds(o, w)]
            send(view, view, s_ag.at[way], r_ring.at[way, slot, i], idx(x, wrap(z + 1 - 2 * way), 1))

        def ag_wait(r, i, way, slot):
            o, w = SUBS_AG[i]
            arrived(ag_v.at[r, :, pl.ds(o, w)], r_ring.at[way, slot, i])

        sums = jnp.zeros((ROW, 1), F32)
        logits = jnp.zeros((ROW, 128), F32)
        for i, (o, w) in enumerate(SUBS):
            hidden = chain_end(rs_in, o, w, i)
            gain = jnp.concatenate(
                [gain_v[pl.ds(x * JX + j, 1), :] for j in range(o // 128, (o + w) // 128)], axis=1)
            ag_v[z, :, pl.ds(o, w)] = (hidden * gain).astype(BF16)
            if i < NS - 1:
                ag_send(z, i, 0, 1)
                ag_send(z, i, 1, 1)
            hid_v[:, pl.ds(o, w)] = hidden
            sums = sums + jnp.sum(hidden * hidden, axis=1, keepdims=True)
            logits = logits + nt(ag_v[z, :, pl.ds(o, w)], rout_v[:, pl.ds(o, w)])
        high = logits.astype(BF16).astype(F32)
        sums_high = sums.astype(BF16).astype(F32)
        ext = high + pltpu.roll(logits - high, EXPERTS, 1)
        ext = jnp.where(lane == LANE_SUM, sums_high, ext)
        ext = jnp.where(lane == LANE_SUM + 1, sums - sums_high, ext)
        ag_v[z, :, pl.ds(DX, EXT)] = (ext + table_rows).astype(BF16)
        ag_send(z, NS - 1, 0, 1)
        ag_send(z, NS - 1, 1, 1)

        def dispatch(rows):
            n = len(rows)
            size = n * NX * SLOT
            jj, lane = iota((size, 128), 0), iota((size, 128), 1)
            wanted_lane = LANE_TAB + lax.rem(jj // SLOT, NX) * QUAD + quad
            pick = jnp.where(lane == wanted_lane, 1.0, 0.0).astype(BF16)
            picked = nt(pick, jnp.concatenate([ag_v[r, :, pl.ds(DX, EXT)] for r in rows], axis=0))
            jj, tok = iota((size, n * ROW), 0), iota((size, n * ROW), 1)
            wanted = (lax.rem(jj, SLOT) // DEV + 1).astype(F32)
            hit = (picked == wanted) & (lax.rem(jj, DEV) == lax.rem(tok, DEV)) & (jj // (NX * SLOT) == tok // ROW)
            place = jnp.where(hit, 1.0, 0.0).astype(BF16)
            moved = nn(place, jnp.concatenate([ag_v[r] for r in rows], axis=0)).astype(BF16)
            for i, r in enumerate(rows):
                dsp_v[r] = moved[i * NX * SLOT:(i + 1) * NX * SLOT].reshape(NX, SLOT, DC)
            for r in rows:
                for i in range(NX):
                    xx = xwrap(x + i + 1)
                    send(dsp_v.at[r, xx], d_v.at[r, x], s_dsp, r_row.at[r], idx(xx, z, 0))

        def returned(rows):
            n = len(rows)
            for r in rows:
                arrived(act_v.at[r], r_row.at[r])
            size = n * NX * SLOT
            jj, lane = iota((size, 128), 0), iota((size, 128), 1)
            wanted_lane = LANE_TAB + jj // (n * SLOT) * QUAD + quad
            pick = jnp.where(lane == wanted_lane, 1.0, 0.0).astype(BF16)
            picked = nt(jnp.concatenate([ag_v[r, :, pl.ds(DX, EXT)] for r in rows], axis=0), pick)
            jj, tok = iota((n * ROW, size), 1), iota((n * ROW, size), 0)
            wanted = (lax.rem(jj, SLOT) // DEV + 1).astype(F32)
            hit = (picked == wanted) & (lax.rem(jj, DEV) == lax.rem(tok, DEV)) & (
                lax.rem(jj // SLOT, n) == tok // ROW)
            place = jnp.where(hit, 1.0, 0.0).astype(BF16)
            spread = []
            for i in range(NX):
                acts = jnp.concatenate([act_v[r, i] for r in rows], axis=0)
                spread.append(nn(place[:, i * n * SLOT:(i + 1) * n * SLOT], acts).astype(BF16))
            return jnp.concatenate(spread, axis=1)

        def down_part(rows):
            spread = returned(rows)
            for o, w in BLOCKS:
                part = nn(spread, wd_v[:, o:o + w])
                for i, r in enumerate(rows):
                    part_v[r, :, pl.ds(o, w)] = part[i * ROW:(i + 1) * ROW]

        dispatch([z])

        def ag_step(k, carry):
            for i in range(NS):
                for way, _ in ways():
                    r = wrap(z - (1 - 2 * way) * k)
                    ag_wait(r, i, way, k)

                    @pl.when((way == 0) | (k < HALF - 1))
                    def _():
                        ag_send(r, i, way, k + 1)
            dispatch(list(up_down(k)))
            return carry
        lax.fori_loop(1, HALF, ag_step, 0)
        last = wrap(z + HALF)
        for i in range(NS):
            ag_wait(last, i, 0, HALF)
        dispatch([last])

        arrived(wd_v, r_wd)
        down_part([z, *up_down(1)])

        def late(g, carry):
            down_part([*up_down(2 * g), *up_down(2 * g + 1)])
            return carry
        lax.fori_loop(1, HALF // 2, late, 0)

        spread = returned([last])
        chain_first(rs2_in, rs2_out, s_rs2, spread, wd_v)

        def rs2_step(s, carry):
            chain_step(rs2_in, rs2_out, s_rs2, s)
            return carry
        lax.fori_loop(1, HALF, rs2_step, 0)

        for t in range(TOK * JX, MSG):
            fin_v[pl.ds(t, DEV, stride=MSG), :] = jnp.zeros((DEV, 128), F32)
        for i, (o, w) in enumerate(SUBS):
            mixed = chain_end(rs2_in, o, w, i) + hid_v[:, pl.ds(o, w)]
            for t in range(TOK):
                for j in range(o // 128, (o + w) // 128):
                    fin_v[pl.ds(t * JX + j, DEV, stride=MSG), :] = (
                        mixed[t * DEV:(t + 1) * DEV, j * 128 - o:j * 128 - o + 128])
        fin_s[...] = fin_v[...].reshape(DEV, MSG, 128).astype(BF16)
        for i in range(DEV - 1):
            to = lax.rem(dev + i + 1, DEV)
            send(fin_s.at[to], out_ref.at[x], s_out, r_out, idx(to // NC, z, lax.rem(to, NC)))
        out_ref[x] = fin_s[dev]

        arrived(ctx_v, s_ctx)
        arrived(wo_v.at[pl.ds(0, (NX - 1) * (VH // NC)), :], s_wo)
        arrived(tab_v.at[pl.ds(0, NX - 1)], s_tab)
        arrived(res_v.at[pl.ds(0, NX - 1)], s_res)
        arrived(vu_v.at[pl.ds(0, VH // NC), :], s_core.at[0])
        arrived(wdn_v, s_core.at[1])
        arrived(wgu_v.at[:, pl.ds(0, UNITS)], s_core.at[2])
        arrived(wgu_v.at[:, pl.ds(0, UNITS)], s_core.at[3])
        for buf, sem in ((rs_out, s_rs), (rs2_out, s_rs2)):
            arrived(buf.at[0], sem.at[0])
            arrived(buf.at[1, pl.ds(1, HALF - 1)], sem.at[1])
        arrived(ag_v.at[pl.ds(0, HALF)], s_ag.at[0])
        arrived(ag_v.at[pl.ds(0, HALF - 1)], s_ag.at[1])
        arrived(dsp_v, s_dsp)
        arrived(fin_s.at[pl.ds(0, DEV - 1)], s_out)
        arrived(out_ref.at[pl.ds(0, NX - 1)], r_out)


def body(
    cache_kv, new_kv, queries, lengths, resid, value_up, out_proj, norm_gain, router, expert_ids, slots, w_gate, w_up,
    w_down,
):
    seqs, steps = resid.shape[:2]
    cache_len = cache_kv.shape[1]
    hbm = pl.BlockSpec(memory_space=pltpu.HBM)
    vmem = pl.BlockSpec(memory_space=pltpu.VMEM)
    smem = pl.BlockSpec(memory_space=pltpu.SMEM)
    dma = pltpu.SemaphoreType.DMA
    regular = pltpu.SemaphoreType.REGULAR
    scratch = [
        pltpu.VMEM((seqs, KV, cache_len), BF16),
        pltpu.VMEM((seqs, steps * H, KV), BF16),
        pltpu.VMEM((steps * H, cache_len), F32),
        pltpu.VMEM((H * 16, 128), F32),
        pltpu.VMEM((H, 16, 128), BF16),
        pltpu.VMEM((NZ, DEV, 16, 128), BF16),
        pltpu.VMEM((DEV * 16, 128), F32),
        pltpu.VMEM((VH, LAT), BF16),
        pltpu.VMEM((NZ, ROW, NX * VH), BF16),
        pltpu.VMEM((NX * VH, DX), BF16),
        pltpu.VMEM((2, HALF + 1, ROW, DX), BF16),
        pltpu.VMEM((2, HALF, ROW, DX), BF16),
        pltpu.VMEM((ROW, DX), F32),
        pltpu.VMEM((8, 128), F32),
        pltpu.VMEM((DEV, 8, 128), F32),
        pltpu.VMEM((NX, MSG, 128), BF16),
        pltpu.VMEM((NX * MSG, 128), F32),
        pltpu.VMEM((DEV, MSG, 128), BF16),
        pltpu.VMEM((DEV * MSG, 128), F32),
        pltpu.VMEM((D // 128, 128), F32),
        pltpu.VMEM((128, DX), BF16),
        pltpu.VMEM((NZ, ROW, DC), BF16),
        pltpu.VMEM((NZ, NX, SLOT, DC), BF16),
        pltpu.VMEM((NZ, NX, SLOT, DC), BF16),
        pltpu.VMEM((D, 2 * NC * UNITS), BF16),
        pltpu.VMEM((NZ, SLOT, NC * UNITS), BF16),
        pltpu.VMEM((NZ, NX, SLOT, NC * UNITS), BF16),
        pltpu.VMEM((NX * NC * UNITS, DX), BF16),
        pltpu.VMEM((UNITS, D), BF16),
        pltpu.VMEM((2, HALF + 1, ROW, DX), BF16),
        pltpu.VMEM((2, HALF, ROW, DX), BF16),
        pltpu.VMEM((NZ, ROW, DX), F32),
        pltpu.VMEM((DEV * MSG, 128), F32),
        pltpu.VMEM((DEV, MSG, 128), BF16),
        dma((seqs,)), dma, dma((3,)),
        dma, dma, dma, dma, dma((4,)), dma, dma, dma((2,)), dma((2,)), dma((2,)), dma, dma, dma,
        dma, dma, dma, dma((4,)), dma, dma((NZ,)), dma((2, HALF + 1, NS)), dma,
        regular, regular,
    ]
    out = pl.pallas_call(
        kernel,
        out_shape=jax.ShapeDtypeStruct((NX, MSG, 128), BF16),
        in_specs=[hbm, vmem, hbm, smem, vmem, hbm, hbm, vmem, hbm, smem, smem, hbm, hbm, hbm],
        out_specs=vmem,
        scratch_shapes=scratch,
        compiler_params=pltpu.CompilerParams(
            collective_id=0, has_side_effects=True, vmem_limit_bytes=(64 << 20) - (64 << 10)),
        name="layer",
    )(
        jnp.transpose(cache_kv, (0, 2, 1)), new_kv, queries.reshape(seqs, steps * H, KV), lengths, resid,
        value_up.T, out_proj, norm_gain.reshape(D // 128, 128), router.T, expert_ids, slots, w_gate, w_up, w_down,
    )
    out = out[:, :TOK * JX].reshape(NX, TOK, JX, 128).transpose(1, 0, 2, 3)
    return out.reshape(resid.shape)


def solution(mesh):
    return jax.shard_map(
        body,
        mesh=mesh,
        in_specs=(
            P(("rep", "ep"), None, None),
            P(("rep", "ep"), None, None),
            P(("rep", "ep"), None, None, None),
            P(("rep", "ep")),
            P(("rep", "ep"), None, None),
            P(None, "ep"),
            P("ep", None),
            P(),
            P(),
            P(("rep", "ep"), None, None),
            P(("rep", "ep"), None, None),
            P(None, "ep"),
            P(None, "ep"),
            P("ep", None),
        ),
        out_specs=P(("rep", "ep"), None, None),
        check_vma=False,
    )
```

```python
import functools
import math

import jax
import jax.numpy as jnp
from jax import lax
from jax.experimental import pallas as pl
from jax.experimental.pallas import tpu as pltpu
from jax.sharding import PartitionSpec as P

NX, NZ, NC = 4, 16, 2
DEV = NX * NC
HALF = NZ // 2

D = 7168
H = 64
LAT = 512
VH = 128
KV = 576
EXPERTS = 16
TOP = 8
CAP = 2
QK = 192
TOK = 4
UNITS = 128
ROW = DEV * TOK
SLOT = DEV * CAP
DX = D // NX
EXT = 128
JX = DX // 128
MSG = 64
LANE_SUM = 32
LANE_TAB = 64
QUAD = EXPERTS // NX
CHIPS_PER = NZ // QUAD

route_scale = 2.827
norm_eps = 1e-06

CUBE = 4

BX = 384
DA = DX - BX
DAE = DA + EXT
DG = DAE + NX * BX
PIECE = 384
SUBS = ((DA, BX),) + tuple((o, min(PIECE, DA - o)) for o in range(0, DA, PIECE))
NS = len(SUBS)
NP = DG // PIECE
NPA = DAE // PIECE
BLOCKS = ((0, 512), (512, 512), (1024, 768))

F32 = jnp.float32
BF16 = jnp.bfloat16


def mo(value, by):
    return pl.multiple_of(value, by)


def nt(a, b):
    return lax.dot_general(a, b, (((1,), (1,)), ((), ())), preferred_element_type=F32)


def nn(a, b):
    return lax.dot_general(a, b, (((1,), (0,)), ((), ())), preferred_element_type=F32)


def iota(shape, axis):
    return lax.broadcasted_iota(jnp.int32, shape, axis)


def kernel(
    cache_h, new_h, q_h, len_h, resid_h, vu_h, wo_h, gain_h, router_h, ids_h, slots_h, wg_h, wu_h, wd_h,
    out_ref,
    new_ref, len_ref, resid_ref, gain_ref, ids_ref, slots_ref,
    cache_v, q_v, score_v, stage_v, ctx_v, arr_v, arrf_v, vu_v, val_v, wo_v, rs_in, rs_out, hid_v, tab_s, tab_v,
    ress_v, resf_v, res_v, resw_v, gain_v, rout_v, ag_v, dsp_v, d_v, wgu_v, act_s, act_v, wd_v, wdn_v, rs2_in, rs2_out,
    part_v, fin_v, fin_s,
    l_cache, l_misc, l_weights, l_small,
    s_ctx, s_tab, s_res, s_wo, s_core, s_wd, s_val, s_rs, s_ag, s_rs2, s_dsp, s_act, s_out, s_bx,
    r_tab, r_res, r_wo, r_core, r_wd, r_row, r_ring, r_out, r_bx, r_twin,
    row_sem, all_sem,
):
    me = lax.axis_index("ep")
    c = lax.rem(me, NC)
    z = lax.rem(me // NC, NZ)
    x = me // (NC * NZ)
    dev = x * NC + c
    quad = z // CHIPS_PER
    group = lax.axis_index("rep")
    half = lax.rem(group, 2)
    twin = {"rep": group + 1 - 2 * half, "ep": me}

    def idx(xx, zz, cc):
        return {"ep": (xx * NZ + zz) * NC + cc}

    def wrap(zz):
        return lax.rem(zz + 2 * NZ, NZ)

    def xwrap(xx):
        return lax.rem(xx, NX)

    def send(src, dst, ssem, rsem, to):
        pltpu.make_async_remote_copy(src_ref=src, dst_ref=dst, send_sem=ssem, recv_sem=rsem, device_id=to).start()

    def arrived(ref, sem):
        pltpu.make_async_copy(ref, ref, sem).wait()

    main = c == 1
    side = c == 0

    loads = [pltpu.make_async_copy(q_h, q_v, l_misc)]
    loads += [pltpu.make_async_copy(cache_h.at[b], cache_v.at[b], l_cache.at[b]) for b in range(2)]
    small = [
        pltpu.make_async_copy(src, dst, l_small.at[i]) for i, (src, dst) in enumerate((
            (new_h, new_ref), (len_h, len_ref), (resid_h, resid_ref), (gain_h, gain_ref), (ids_h, ids_ref),
            (slots_h, slots_ref)))
    ]
    for load in loads[:2] + small[:2] + loads[2:] + small[2:]:
        load.start()

    bar = pltpu.get_barrier_semaphore()

    @pl.when(side)
    def _():
        def greet(o, carry):
            far = HALF - (o + 1) // 2
            zz = wrap(jnp.where(lax.rem(o, 2) == 1, z + far, z - far))
            for xx in range(NX):
                pl.semaphore_signal(bar, inc=1, device_id=idx(xx, zz, 1))
            return carry
        lax.fori_loop(0, NZ, greet, 0)

    @pl.when(main)
    def _():
        for xx in range(NX):
            pl.semaphore_signal(bar, inc=1, device_id=idx(xx, z, 0))
        for step in (1, -1):
            pl.semaphore_signal(bar, inc=1, device_id=idx(x, wrap(z + step), 1))
        pl.semaphore_signal(bar, inc=1, device_id=twin)

    gate_at = pl.ds(mo(c * UNITS, UNITS), UNITS)
    up_at = pl.ds(mo((NC + c) * UNITS, UNITS), UNITS)
    vu_at = pl.ds(mo(c * (VH // NC), VH // NC), VH // NC)
    router_copy = pltpu.make_async_copy(
        router_h.at[:, pl.ds(mo(x * DX, 128), DX)], rout_v.at[pl.ds(0, EXPERTS), :], l_weights.at[1])
    gate_copy = pltpu.make_async_copy(wg_h, wgu_v.at[:, gate_at], l_weights.at[1])
    up_copy = pltpu.make_async_copy(wu_h, wgu_v.at[:, up_at], l_weights.at[2])
    vu_copy = pltpu.make_async_copy(vu_h, vu_v.at[vu_at, :], l_weights.at[0])

    wo_row = pl.ds(mo(x * VH + c * (VH // NC), VH // NC), VH // NC)

    def own_columns(xx):
        return pl.ds(mo(xx * DX, 128), DX)

    wo_copy = pltpu.make_async_copy(wo_h.at[:, own_columns(x)], wo_v.at[wo_row, :], l_weights.at[0])

    def wo_send(xx):
        send(wo_h.at[:, own_columns(xx)], wo_v.at[wo_row, :], s_wo, r_wo, idx(xx, z, 1))

    def wd_rows(xx, cc):
        return pl.ds(mo((xx * NC + cc) * UNITS, UNITS), UNITS)

    def row_start():
        @pl.when(side)
        def _():
            pl.semaphore_wait(bar, NX)
            pl.semaphore_signal(row_sem, inc=1, device_id=idx(x, z, 1))

        @pl.when(main)
        def _():
            pl.semaphore_wait(row_sem, 1)

        for i in range(NX - 1):
            wo_send(xwrap(x + i + 1))

        @pl.when(main)
        def _():
            wo_copy.start()
            send(vu_h, vu_v.at[vu_at, :], s_core.at[0], r_core.at[0], idx(x, z, 0))
            rout_v[...] = jnp.zeros_like(rout_v)
            router_copy.start()

        @pl.when(side)
        def _():
            wo_send(x)
            vu_copy.start()

    scale = 1.0 / math.sqrt(QK)
    blk = 512
    nblk = cache_v.shape[2] // blk
    loads[0].wait()
    small[0].wait()
    small[1].wait()
    for b in range(2):
        if b == 1:
            row_start()
        qb = q_v[b]
        qf = qb.astype(F32)
        step_of = iota((2 * H, 1), 0) // H
        new_rows = [new_ref[b, pl.ds(t, 1), :].astype(F32) for t in range(2)]
        s_new = [jnp.sum(qf * row, axis=1, keepdims=True) * scale for row in new_rows]
        s_new[1] = jnp.where(step_of >= 1, s_new[1], -jnp.inf)
        peak = jnp.maximum(s_new[0], s_new[1])
        loads[1 + b].wait()
        for p in range(nblk):
            sc = nn(qb, cache_v[b, :, pl.ds(p * blk, blk)]) * scale
            pos = iota((2 * H, blk), 1) + p * blk
            sc = jnp.where(pos < len_ref[b], sc, -jnp.inf)
            score_v[:, pl.ds(p * blk, blk)] = sc
            peak = jnp.maximum(peak, jnp.max(sc, axis=1, keepdims=True))
        p_new = [jnp.exp(s - peak) for s in s_new]
        total = p_new[0] + p_new[1]
        acc = p_new[0].astype(BF16).astype(F32) * new_rows[0][:, :LAT]
        acc = acc + p_new[1].astype(BF16).astype(F32) * new_rows[1][:, :LAT]
        for p in range(nblk):
            pr = jnp.exp(score_v[:, pl.ds(p * blk, blk)] - peak)
            total = total + jnp.sum(pr, axis=1, keepdims=True)
            acc = acc + nt(pr.astype(BF16), cache_v[b, pl.ds(0, LAT), pl.ds(p * blk, blk)])
        ctx = acc / total
        for s in range(2):
            for j in range(LAT // 128):
                stage_v[pl.ds(j * TOK + b * 2 + s, H, stride=16), :] = ctx[s * H:(s + 1) * H, j * 128:(j + 1) * 128]
    ctx_v[...] = stage_v[...].reshape(H, 16, 128).astype(BF16)

    @pl.when(main)
    def _():
        pl.semaphore_wait(bar, NX * NZ + 3)
        pl.semaphore_signal(all_sem, inc=1, device_id=idx(x, z, 0))

    @pl.when(side)
    def _():
        pl.semaphore_wait(all_sem, 1)

    def ctx_send(o, carry):
        far = HALF - (o + 1) // 2
        zz = wrap(jnp.where(lax.rem(o, 2) == 1, z + far, z - far))
        for i in range(NX):
            xx = xwrap(x + i + 1)
            own = side & (zz == z) & (xx == x)

            @pl.when(jnp.logical_not(own))
            def _():
                send(ctx_v.at[xx * NZ + zz], arr_v.at[z, dev], s_ctx, r_row.at[z], idx(xx, zz, 0))

            @pl.when(own)
            def _():
                arr_v[z, dev] = ctx_v[xx * NZ + zz]
        return carry
    lax.fori_loop(0, NZ, ctx_send, 0)

    @pl.when(main)
    def _():
        @pl.when(half == 1)
        def _():
            send(wd_h, wdn_v, s_core.at[1], r_core.at[1], idx(x, z, 0))
        send(wg_h, wgu_v.at[:, gate_at], s_core.at[2], r_core.at[2], idx(x, z, 0))
        send(wu_h, wgu_v.at[:, up_at], s_core.at[3], r_core.at[3], idx(x, z, 0))

    @pl.when(side)
    def _():
        gate_copy.start()
        up_copy.start()

    for load in small[2:]:
        load.wait()

    rows8, lanes8 = iota((8, 128), 0), iota((8, 128), 1)
    table = jnp.zeros((8, 128), F32)
    for t in range(TOK):
        for k in range(TOP):
            hit = (rows8 == t) & (lanes8 == ids_ref[t // 2, t % 2, k] + LANE_TAB)
            table = jnp.where(hit, (slots_ref[t // 2, t % 2, k] + 1).astype(F32), table)
    tab_s[...] = table

    resf_v[...] = jnp.zeros_like(resf_v)
    for t in range(TOK):
        row = resid_ref[t // 2, pl.ds(t % 2, 1), :].astype(F32)
        for xx in range(NX):
            for j in range(JX):
                col = xx * DX + j * 128
                resf_v[pl.ds(xx * MSG + t * JX + j, 1), :] = row[:, col:col + 128]
    ress_v[...] = resf_v[...].reshape(NX, MSG, 128).astype(BF16)

    for xx in range(NX):
        other = jnp.logical_not(main & (x == xx))

        @pl.when(other)
        def _():
            send(tab_s, tab_v.at[dev], s_tab, r_tab, idx(xx, z, 1))
            send(ress_v.at[xx], res_v.at[dev], s_res, r_res, idx(xx, z, 1))

        @pl.when(jnp.logical_not(other))
        def _():
            tab_v[dev] = tab_s[...]
            res_v[dev] = ress_v[xx]

    def up_down(k):
        return wrap(z - k), wrap(z + k)

    @pl.when(side)
    def _side():
        vu_copy.wait()
        arrived(vu_v.at[pl.ds(0, VH // NC), :], r_core.at[0])
        own_lanes = pl.ds(mo(x * VH, VH), VH)

        def wd_send(source):
            for i in range(NX):
                xx = xwrap(x + i + 1)
                send(source.at[:, own_columns(xx)], wd_v.at[wd_rows(x, half), :], s_wd, r_wd, idx(xx, z, 1))

        def ctx_row(r):
            @pl.when(r == z)
            def _():
                arrived(arr_v.at[r, pl.ds(0, DEV - 1)], r_row.at[r])

            @pl.when(r != z)
            def _():
                arrived(arr_v.at[r], r_row.at[r])

            arrf_v[...] = arr_v[r].reshape(DEV * 16, 128).astype(F32)
            cols = []
            for j in range(LAT // 128):
                cols.append(jnp.concatenate(
                    [arrf_v[pl.ds(j * TOK + t, DEV, stride=16), :] for t in range(TOK)], axis=0))
            rows = jnp.concatenate(cols, axis=1).astype(BF16)
            val_v[r, :, own_lanes] = nt(rows, vu_v[...]).astype(BF16)
            view = val_v.at[r, :, own_lanes]
            for i in range(NX):
                send(view, view, s_val, r_row.at[r], idx(xwrap(x + i + 1), z, 1))

        def ctx_step(o, carry):
            far = HALF - (o + 1) // 2
            ctx_row(wrap(jnp.where(lax.rem(o, 2) == 1, z + far, z - far)))
            return carry
        lax.fori_loop(0, NZ, ctx_step, 0)

        @pl.when(half == 0)
        def _():
            wd_send(wd_h)

        @pl.when(half == 1)
        def _():
            arrived(wdn_v, r_core.at[1])
            wd_send(wdn_v)

        gate_copy.wait()
        up_copy.wait()
        arrived(wgu_v.at[:, pl.ds(0, UNITS)], r_core.at[2])
        arrived(wgu_v.at[:, pl.ds(0, UNITS)], r_core.at[3])

        own_expert = x * QUAD + quad

        def experts(rows):
            for r in rows:
                arrived(d_v.at[r], r_row.at[r])
            both = jnp.zeros((SLOT * len(rows), 2 * NC * UNITS), F32)
            ext = jnp.zeros((SLOT * len(rows), EXT), F32)
            shared = jnp.concatenate([d_v[r, NX] for r in rows], axis=0)
            for xx in range(NX):
                both = both + nn(
                    jnp.concatenate([d_v[r, xx, :, pl.ds(0, DA)] for r in rows], axis=0),
                    wgu_v[xx * DX:xx * DX + DA, :])
                both = both + nn(shared[:, xx * BX:(xx + 1) * BX], wgu_v[xx * DX + DA:(xx + 1) * DX, :])
                piece = jnp.concatenate([d_v[r, xx, :, pl.ds(DA, EXT)] for r in rows], axis=0).astype(F32)
                ext = ext + piece
            lane = iota(ext.shape, 1)
            squares = jnp.sum(
                jnp.where((lane == LANE_SUM) | (lane == LANE_SUM + 1), ext, 0.0), axis=1, keepdims=True)
            inv = lax.rsqrt(squares / D + norm_eps)
            logits = (ext + pltpu.roll(ext, EXT - EXPERTS, 1)) * inv
            named = (pltpu.roll(piece, EXT - LANE_TAB, 1) > 0.0) & (lane < EXPERTS)
            gates = jnp.where(named, 1.0 / (1.0 + jnp.exp(-logits)), 0.0)
            norm = jnp.sum(gates, axis=1, keepdims=True)
            mine = jnp.sum(jnp.where(lane == own_expert, gates, 0.0), axis=1, keepdims=True)
            share = jnp.where(norm > 0.0, route_scale * mine / norm, 0.0)
            gate = both[:, :NC * UNITS] * inv
            upward = both[:, NC * UNITS:] * inv
            act = (gate / (1.0 + jnp.exp(-gate)) * upward * share).astype(BF16)
            for i, r in enumerate(rows):
                act_s[r] = act[i * SLOT:(i + 1) * SLOT]
                for n in range(NX):
                    send(act_s.at[r], act_v.at[r, x], s_act, r_row.at[r], idx(xwrap(x + n + 1), z, 1))

        experts([z])

        def step(k, carry):
            experts(list(up_down(k)))
            return carry
        lax.fori_loop(1, HALF, step, 0)
        experts([wrap(z + HALF)])

        arrived(out_ref, r_out)
        arrived(ctx_v.at[pl.ds(0, NX * NZ - 1)], s_ctx)
        arrived(wo_v.at[pl.ds(0, NX * (VH // NC)), :], s_wo)
        arrived(tab_v.at[pl.ds(0, NX)], s_tab)
        arrived(res_v.at[pl.ds(0, NX)], s_res)
        arrived(wd_v.at[pl.ds(0, NX * UNITS), :], s_wd)
        arrived(val_v, s_val)
        arrived(act_v, s_act)

    @pl.when(main)
    def _main():
        up = idx(x, wrap(z + 1), 1)
        gain_v[...] = gain_ref[...].astype(F32)

        early = jnp.where(lax.rem(z, CUBE) < CUBE // 2, 1, 0)

        def ways(pieces):
            for i in range(pieces + 1):
                if i < pieces:
                    yield i, early, idx(x, wrap(z + 1 - 2 * early), 1)
                if i > 0:
                    yield i - 1, 1 - early, idx(x, wrap(z - 1 + 2 * early), 1)

        def slot_a(s):
            return lax.rem(s, 3)

        def slot_g(k):
            return lax.rem(k + 2, 3)

        def slot_b(s):
            return jnp.where(s <= 3, s + 2, lax.rem(s, 3))

        def chain_step(in_ref, out_buf, ssem, slot, s):
            for i, way, to in ways(NS):
                at = pl.ds(*SUBS[i])
                r = wrap(z + (1 - 2 * way) * (HALF - s))

                @pl.when((way == 0) | (s >= 2))
                def _():
                    arrived(in_ref.at[way, s, :, at], r_ring.at[way, slot(s), i])
                total = part_v[r, :, at] + in_ref[way, s, :, at].astype(F32)
                out_buf[way, s, :, at] = total.astype(BF16)
                send(out_buf.at[way, s, :, at], in_ref.at[way, s + 1, :, at], ssem.at[way],
                     r_ring.at[way, slot(s + 1), i], to)

        def chain_first(in_ref, out_buf, ssem, slot, rows, weights):
            for i, (o, w) in enumerate(SUBS):
                at = pl.ds(o, w)
                out_buf[0, 0, :, at] = nn(rows, weights[:, o:o + w]).astype(BF16)
                send(out_buf.at[0, 0, :, at], in_ref.at[0, 1, :, at], ssem.at[0], r_ring.at[0, slot(1), i], up)

        def chain_end(in_ref, slot, o, w, i):
            at = pl.ds(o, w)
            for d in range(2):
                arrived(in_ref.at[d, HALF, :, at], r_ring.at[d, slot(HALF), i])
            return part_v[z, :, at] + in_ref[0, HALF, :, at].astype(F32) + in_ref[1, HALF, :, at].astype(F32)

        rs_in[1, 1] = jnp.zeros((ROW, DX), BF16)
        rs2_in[1, 1] = jnp.zeros((ROW, DX), BF16)

        wo_copy.wait()
        arrived(wo_v.at[pl.ds(0, (DEV - 1) * (VH // NC)), :], r_wo)

        def attended(rows):
            for r in rows:
                arrived(val_v.at[r], r_row.at[r])
            stacked = jnp.concatenate([val_v[r] for r in rows], axis=0)
            for o, w in BLOCKS:
                part = nn(stacked, wo_v[:, o:o + w])
                for i, r in enumerate(rows):
                    part_v[r, :, pl.ds(o, w)] = part[i * ROW:(i + 1) * ROW]

        first = wrap(z + HALF)
        arrived(val_v.at[first], r_row.at[first])
        chain_first(rs_in, rs_out, s_rs, slot_a, val_v[first], wo_v)
        attended(list(up_down(HALF - 1)))

        def rs_step(s, carry):
            chain_step(rs_in, rs_out, s_rs, slot_a, s)
            ahead = HALF - 1 - s

            @pl.when(ahead >= 1)
            def _():
                attended(list(up_down(ahead)))
            return carry
        lax.fori_loop(1, HALF, rs_step, 0)
        attended([z])

        arrived(res_v.at[pl.ds(0, DEV - 1)], r_res)
        arrived(tab_v.at[pl.ds(0, DEV - 1)], r_tab)
        resw_v[...] = res_v[...].reshape(DEV * MSG, 128).astype(F32)
        for j in range(JX):
            at = pl.ds(j * 128, 128)
            part_v[z, :, at] = part_v[z, :, at] + jnp.concatenate(
                [resw_v[pl.ds(t * JX + j, DEV, stride=MSG), :] for t in range(TOK)], axis=0)
        lane = iota((ROW, 128), 1)
        rows = iota((DEV, 128), 0)
        tabs = []
        for t in range(TOK):
            piece = jnp.zeros((DEV, 128), F32)
            for d in range(DEV):
                piece = jnp.where(rows == d, tab_v[d, pl.ds(t, 1), :], piece)
            tabs.append(piece)
        table_rows = jnp.concatenate(tabs, axis=0)
        router_copy.wait()

        def ag_send(r, i, way, k):
            view = ag_v.at[r, :, pl.ds(i * PIECE, PIECE)]
            send(view, view, s_ag.at[way], r_ring.at[way, slot_g(k), i], idx(x, wrap(z + 1 - 2 * way), 1))

        def ag_wait(r, i, way, k):
            arrived(ag_v.at[r, :, pl.ds(i * PIECE, PIECE)], r_ring.at[way, slot_g(k), i])

        sums = jnp.zeros((ROW, 1), F32)
        logits = jnp.zeros((ROW, 128), F32)
        bx_at = pl.ds(mo(DAE + x * BX, 128), BX)
        for i, (o, w) in enumerate(SUBS):
            hidden = chain_end(rs_in, slot_a, o, w, i)
            gain = jnp.concatenate(
                [gain_v[pl.ds(x * JX + j, 1), :] for j in range(o // 128, (o + w) // 128)], axis=1)
            scaled = (hidden * gain).astype(BF16)
            if i == 0:
                ag_v[z, :, bx_at] = scaled
                view = ag_v.at[z, :, bx_at]
                for j in range(NX - 1):
                    send(view, view, s_bx, r_bx, idx(xwrap(x + j + 1), z, 1))
            else:
                ag_v[z, :, pl.ds(o, w)] = scaled
                if i < NS - 1:
                    ag_send(z, i - 1, 0, 1)
                    ag_send(z, i - 1, 1, 1)
            hid_v[:, pl.ds(o, w)] = hidden
            sums = sums + jnp.sum(hidden * hidden, axis=1, keepdims=True)
            logits = logits + nt(scaled, rout_v[:, pl.ds(o, w)])
        high = logits.astype(BF16).astype(F32)
        sums_high = sums.astype(BF16).astype(F32)
        ext = high + pltpu.roll(logits - high, EXPERTS, 1)
        ext = jnp.where(lane == LANE_SUM, sums_high, ext)
        ext = jnp.where(lane == LANE_SUM + 1, sums - sums_high, ext)
        ag_v[z, :, pl.ds(DA, EXT)] = (ext + table_rows).astype(BF16)
        ag_send(z, NPA - 1, 0, 1)
        ag_send(z, NPA - 1, 1, 1)
        arrived(wd_v.at[pl.ds(0, NX * UNITS), :], r_wd)
        for xx in range(NX):
            view = wd_v.at[wd_rows(xx, half), :]
            send(view, view, s_wd, r_twin, twin)
        arrived(ag_v.at[z, :, pl.ds(DAE, (NX - 1) * BX)], r_bx)
        for i in range(NPA, NP):
            ag_send(z, i, 0, 1)
            ag_send(z, i, 1, 1)

        def dispatch(rows):
            n = len(rows)
            size = n * NX * SLOT
            jj, lane = iota((size, 128), 0), iota((size, 128), 1)
            wanted_lane = LANE_TAB + lax.rem(x + lax.rem(jj // SLOT, NX), NX) * QUAD + quad
            pick = jnp.where(lane == wanted_lane, 1.0, 0.0).astype(BF16)
            picked = nt(pick, jnp.concatenate([ag_v[r, :, pl.ds(DA, EXT)] for r in rows], axis=0))
            jj, tok = iota((size, n * ROW), 0), iota((size, n * ROW), 1)
            wanted = (lax.rem(jj, SLOT) // DEV + 1).astype(F32)
            hit = (picked == wanted) & (lax.rem(jj, DEV) == lax.rem(tok, DEV)) & (jj // (NX * SLOT) == tok // ROW)
            place = jnp.where(hit, 1.0, 0.0).astype(BF16)
            moved = nn(place, jnp.concatenate([ag_v[r, :, pl.ds(0, DAE)] for r in rows], axis=0)).astype(BF16)
            own = jnp.concatenate([place[i * NX * SLOT:i * NX * SLOT + SLOT] for i in range(n)], axis=0)
            shared = nn(own, jnp.concatenate([ag_v[r, :, pl.ds(DAE, NX * BX)] for r in rows], axis=0)).astype(BF16)
            for i, r in enumerate(rows):
                dsp_v[r, pl.ds(0, NX)] = moved[i * NX * SLOT:(i + 1) * NX * SLOT].reshape(NX, SLOT, DAE)
                dsp_v[r, NX] = shared[i * SLOT:(i + 1) * SLOT]
            for r in rows:
                for i in range(1, NX):
                    send(dsp_v.at[r, i], d_v.at[r, x], s_dsp, r_row.at[r], idx(xwrap(x + i), z, 0))
                send(dsp_v.at[r, 0], d_v.at[r, x], s_dsp, r_row.at[r], idx(x, z, 0))
                send(dsp_v.at[r, NX], d_v.at[r, NX], s_dsp, r_row.at[r], idx(x, z, 0))

        def returned(rows):
            n = len(rows)
            for r in rows:
                arrived(act_v.at[r], r_row.at[r])
            size = n * NX * SLOT
            jj, lane = iota((size, 128), 0), iota((size, 128), 1)
            wanted_lane = LANE_TAB + jj // (n * SLOT) * QUAD + quad
            pick = jnp.where(lane == wanted_lane, 1.0, 0.0).astype(BF16)
            picked = nt(jnp.concatenate([ag_v[r, :, pl.ds(DA, EXT)] for r in rows], axis=0), pick)
            jj, tok = iota((n * ROW, size), 1), iota((n * ROW, size), 0)
            wanted = (lax.rem(jj, SLOT) // DEV + 1).astype(F32)
            hit = (picked == wanted) & (lax.rem(jj, DEV) == lax.rem(tok, DEV)) & (
                lax.rem(jj // SLOT, n) == tok // ROW)
            place = jnp.where(hit, 1.0, 0.0).astype(BF16)
            spread = []
            for i in range(NX):
                acts = jnp.concatenate([act_v[r, i] for r in rows], axis=0)
                spread.append(nn(place[:, i * n * SLOT:(i + 1) * n * SLOT], acts).astype(BF16))
            return jnp.concatenate(spread, axis=1)

        def down_part(rows):
            spread = returned(rows)
            for o, w in BLOCKS:
                part = nn(spread, wd_v[:, o:o + w])
                for i, r in enumerate(rows):
                    part_v[r, :, pl.ds(o, w)] = part[i * ROW:(i + 1) * ROW]

        dispatch([z])

        def ag_step(k, carry):
            for i, way, _ in ways(NP):
                r = wrap(z - (1 - 2 * way) * k)
                ag_wait(r, i, way, k)

                @pl.when((way == 0) | (k < HALF - 1))
                def _():
                    ag_send(r, i, way, k + 1)
            dispatch(list(up_down(k)))
            return carry
        lax.fori_loop(1, HALF, ag_step, 0)
        last = wrap(z + HALF)
        for i in range(NP):
            ag_wait(last, i, 0, HALF)
        dispatch([last])

        arrived(wd_v.at[pl.ds(0, NX * UNITS), :], r_twin)
        down_part([z, *up_down(1)])

        def late(g, carry):
            down_part([*up_down(2 * g), *up_down(2 * g + 1)])
            return carry
        lax.fori_loop(1, HALF // 2, late, 0)

        spread = returned([last])
        chain_first(rs2_in, rs2_out, s_rs2, slot_b, spread, wd_v)

        def rs2_step(s, carry):
            chain_step(rs2_in, rs2_out, s_rs2, slot_b, s)
            return carry
        lax.fori_loop(1, HALF, rs2_step, 0)

        for t in range(TOK * JX, MSG):
            fin_v[pl.ds(t, DEV, stride=MSG), :] = jnp.zeros((DEV, 128), F32)
        for i, (o, w) in enumerate(SUBS):
            mixed = chain_end(rs2_in, slot_b, o, w, i) + hid_v[:, pl.ds(o, w)]
            for t in range(TOK):
                for j in range(o // 128, (o + w) // 128):
                    fin_v[pl.ds(t * JX + j, DEV, stride=MSG), :] = (
                        mixed[t * DEV:(t + 1) * DEV, j * 128 - o:j * 128 - o + 128])
        fin_s[...] = fin_v[...].reshape(DEV, MSG, 128).astype(BF16)
        for i in range(DEV - 1):
            to = lax.rem(dev + i + 1, DEV)
            send(fin_s.at[to], out_ref.at[x], s_out, r_out, idx(to // NC, z, lax.rem(to, NC)))
        out_copy = pltpu.make_async_copy(fin_s.at[dev], out_ref.at[x], l_misc)
        out_copy.start()

        arrived(ctx_v, s_ctx)
        arrived(wo_v.at[pl.ds(0, (NX - 1) * (VH // NC)), :], s_wo)
        arrived(tab_v.at[pl.ds(0, NX - 1)], s_tab)
        arrived(res_v.at[pl.ds(0, NX - 1)], s_res)
        arrived(vu_v.at[pl.ds(0, VH // NC), :], s_core.at[0])
        @pl.when(half == 1)
        def _():
            arrived(wdn_v, s_core.at[1])
        arrived(wd_v.at[pl.ds(0, NX * UNITS), :], s_wd)
        arrived(wgu_v.at[:, pl.ds(0, UNITS)], s_core.at[2])
        arrived(wgu_v.at[:, pl.ds(0, UNITS)], s_core.at[3])
        for buf, sem in ((rs_out, s_rs), (rs2_out, s_rs2)):
            arrived(buf.at[0], sem.at[0])
            arrived(buf.at[1, pl.ds(1, HALF - 1)], sem.at[1])
        arrived(ag_v.at[pl.ds(0, HALF)], s_ag.at[0])
        arrived(ag_v.at[pl.ds(0, HALF - 1)], s_ag.at[1])
        arrived(dsp_v, s_dsp)
        arrived(fin_s.at[pl.ds(0, DEV - 1)], s_out)
        arrived(ag_v.at[z, :, pl.ds(DAE, (NX - 1) * BX)], s_bx)
        out_copy.wait()
        arrived(out_ref.at[pl.ds(0, NX - 1)], r_out)


def body(
    cache_kv, new_kv, queries, lengths, resid, value_up, out_proj, norm_gain, router, expert_ids, slots, w_gate, w_up,
    w_down,
):
    seqs, steps = resid.shape[:2]
    cache_len = cache_kv.shape[1]
    hbm = pl.BlockSpec(memory_space=pltpu.HBM)
    dma = pltpu.SemaphoreType.DMA
    regular = pltpu.SemaphoreType.REGULAR
    scratch = [
        pltpu.VMEM(new_kv.shape, BF16),
        pltpu.SMEM(lengths.shape, jnp.int32),
        pltpu.VMEM(resid.shape, BF16),
        pltpu.VMEM((D // 128, 128), BF16),
        pltpu.SMEM(expert_ids.shape, jnp.int32),
        pltpu.SMEM(slots.shape, jnp.int32),
        pltpu.VMEM((seqs, KV, cache_len), BF16),
        pltpu.VMEM((seqs, steps * H, KV), BF16),
        pltpu.VMEM((steps * H, cache_len), F32),
        pltpu.VMEM((H * 16, 128), F32),
        pltpu.VMEM((H, 16, 128), BF16),
        pltpu.VMEM((NZ, DEV, 16, 128), BF16),
        pltpu.VMEM((DEV * 16, 128), F32),
        pltpu.VMEM((VH, LAT), BF16),
        pltpu.VMEM((NZ, ROW, NX * VH), BF16),
        pltpu.VMEM((NX * VH, DX), BF16),
        pltpu.VMEM((2, HALF + 1, ROW, DX), BF16),
        pltpu.VMEM((2, HALF, ROW, DX), BF16),
        pltpu.VMEM((ROW, DX), F32),
        pltpu.VMEM((8, 128), F32),
        pltpu.VMEM((DEV, 8, 128), F32),
        pltpu.VMEM((NX, MSG, 128), BF16),
        pltpu.VMEM((NX * MSG, 128), F32),
        pltpu.VMEM((DEV, MSG, 128), BF16),
        pltpu.VMEM((DEV * MSG, 128), F32),
        pltpu.VMEM((D // 128, 128), F32),
        pltpu.VMEM((128, DX), BF16),
        pltpu.VMEM((NZ, ROW, DG), BF16),
        pltpu.VMEM((NZ, NX + 1, SLOT, DAE), BF16),
        pltpu.VMEM((NZ, NX + 1, SLOT, DAE), BF16),
        pltpu.VMEM((D, 2 * NC * UNITS), BF16),
        pltpu.VMEM((NZ, SLOT, NC * UNITS), BF16),
        pltpu.VMEM((NZ, NX, SLOT, NC * UNITS), BF16),
        pltpu.VMEM((NX * NC * UNITS, DX), BF16),
        pltpu.VMEM((UNITS, D), BF16),
        pltpu.VMEM((2, HALF + 1, ROW, DX), BF16),
        pltpu.VMEM((2, HALF, ROW, DX), BF16),
        pltpu.VMEM((NZ, ROW, DX), F32),
        pltpu.VMEM((DEV * MSG, 128), F32),
        pltpu.VMEM((DEV, MSG, 128), BF16),
        dma((seqs,)), dma, dma((3,)), dma((6,)),
        dma, dma, dma, dma, dma((4,)), dma, dma, dma((2,)), dma((2,)), dma((2,)), dma, dma, dma, dma,
        dma, dma, dma, dma((4,)), dma, dma((NZ,)), dma((2, 6, NP)), dma, dma, dma,
        regular, regular,
    ]
    out = pl.pallas_call(
        kernel,
        out_shape=jax.ShapeDtypeStruct((NX, MSG, 128), BF16),
        in_specs=[hbm] * 14,
        out_specs=hbm,
        scratch_shapes=scratch,
        compiler_params=pltpu.CompilerParams(
            collective_id=0, has_side_effects=True, vmem_limit_bytes=(64 << 20) - (64 << 10)),
        name="layer",
    )(
        jnp.transpose(cache_kv, (0, 2, 1)), new_kv, queries.reshape(seqs, steps * H, KV), lengths, resid,
        value_up.T, out_proj, norm_gain.reshape(D // 128, 128), router.T, expert_ids, slots, w_gate, w_up, w_down,
    )
    out = out[:, :TOK * JX].reshape(NX, TOK, JX, 128).transpose(1, 0, 2, 3)
    return out.reshape(resid.shape)


def solution(mesh):
    return jax.shard_map(
        body,
        mesh=mesh,
        in_specs=(
            P(("rep", "ep"), None, None),
            P(("rep", "ep"), None, None),
            P(("rep", "ep"), None, None, None),
            P(("rep", "ep")),
            P(("rep", "ep"), None, None),
            P(None, "ep"),
            P("ep", None),
            P(),
            P(),
            P(("rep", "ep"), None, None),
            P(("rep", "ep"), None, None),
            P(None, "ep"),
            P(None, "ep"),
            P("ep", None),
        ),
        out_specs=P(("rep", "ep"), None, None),
        check_vma=False,
    )
```

```python
import functools
import math

import jax
import jax.numpy as jnp
from jax import lax
from jax.experimental import pallas as pl
from jax.experimental.pallas import tpu as pltpu
from jax.sharding import PartitionSpec as P

NX, NZ, NC = 4, 16, 2
DEV = NX * NC
HALF = NZ // 2

D = 7168
H = 64
LAT = 512
VH = 128
KV = 576
EXPERTS = 16
TOP = 8
CAP = 2
QK = 192
TOK = 4
UNITS = 128
ROW = DEV * TOK
SLOT = DEV * CAP
DX = D // NX
EXT = 128
JX = DX // 128
MSG = 64
LANE_SUM = 32
LANE_TAB = 64
QUAD = EXPERTS // NX
CHIPS_PER = NZ // QUAD

route_scale = 2.827
norm_eps = 1e-06

CUBE = 4

BX = 384
DA = DX - BX
DAE = DA + EXT
DG = DAE + NX * BX
PIECE = 768
SUBS = ((DA, BX), (0, 512), (512, 512), (1024, 384))
NS = len(SUBS)
NP = DG // PIECE
NPA = DAE // PIECE
BLOCKS = ((0, 512), (512, 512), (1024, 768))
DOWN = 4

F32 = jnp.float32
BF16 = jnp.bfloat16


def mo(value, by):
    return pl.multiple_of(value, by)


def nt(a, b):
    return lax.dot_general(a, b, (((1,), (1,)), ((), ())), preferred_element_type=F32)


def nn(a, b):
    return lax.dot_general(a, b, (((1,), (0,)), ((), ())), preferred_element_type=F32)


def iota(shape, axis):
    return lax.broadcasted_iota(jnp.int32, shape, axis)


def kernel(
    cache_h, new_h, q_h, len_h, resid_h, vu_h, wo_h, gain_h, router_h, ids_h, slots_h, wg_h, wu_h, wd_h,
    out_ref,
    new_ref, len_ref, resid_ref, gain_ref, ids_ref, slots_ref,
    cache_v, q_v, score_v, stage_v, ctx_v, arr_v, arrf_v, vu_v, val_v, wo_v, ctxn_v, won_v, at_v, rs_in, rs_out, att_v, tab_s, tab_v,
    ress_v, resf_v, res_v, resw_v, gain_v, rout_v, ag_v, dsp_v, d_v, wgu_v, act_s, act_v, wd_v, wdn_v, rs2_in, rs2_out,
    part_v, fin_v, fin_s, sum_v,
    l_cache, l_misc, l_weights, l_small,
    s_ctx, s_tab, s_res, s_wo, s_core, s_wd, s_val, s_rs, s_ag, s_rs2, s_dsp, s_act, s_out, s_bx,
    r_tab, r_res, r_wo, r_wox, r_woy, r_core, r_wd, r_row, r_ring, r_out, r_bx, r_twin,
    row_sem, all_sem,
):
    me = lax.axis_index("ep")
    c = lax.rem(me, NC)
    z = lax.rem(me // NC, NZ)
    x = me // (NC * NZ)
    dev = x * NC + c
    quad = z // CHIPS_PER
    group = lax.axis_index("rep")
    half = lax.rem(group, 2)
    twin = {"rep": group + 1 - 2 * half, "ep": me}

    def idx(xx, zz, cc):
        return {"ep": (xx * NZ + zz) * NC + cc}

    def wrap(zz):
        return lax.rem(zz + 2 * NZ, NZ)

    def xwrap(xx):
        return lax.rem(xx, NX)

    def send(src, dst, ssem, rsem, to):
        pltpu.make_async_remote_copy(src_ref=src, dst_ref=dst, send_sem=ssem, recv_sem=rsem, device_id=to).start()

    def arrived(ref, sem):
        pltpu.make_async_copy(ref, ref, sem).wait()

    main = c == 1
    side = c == 0

    loads = [pltpu.make_async_copy(q_h, q_v, l_misc)]
    loads += [pltpu.make_async_copy(cache_h.at[b], cache_v.at[b], l_cache.at[b]) for b in range(2)]
    small = [
        pltpu.make_async_copy(src, dst, l_small.at[i]) for i, (src, dst) in enumerate((
            (new_h, new_ref), (len_h, len_ref), (resid_h, resid_ref), (gain_h, gain_ref), (ids_h, ids_ref),
            (slots_h, slots_ref)))
    ]
    for load in loads[:2] + small[:2] + loads[2:] + small[2:]:
        load.start()

    bar = pltpu.get_barrier_semaphore()

    @pl.when(side)
    def _():
        def greet(o, carry):
            far = HALF - (o + 1) // 2
            zz = wrap(jnp.where(lax.rem(o, 2) == 1, z + far, z - far))
            for xx in range(NX):
                pl.semaphore_signal(bar, inc=1, device_id=idx(xx, zz, 1))
            return carry
        lax.fori_loop(0, NZ, greet, 0)

    @pl.when(main)
    def _():
        for xx in range(NX):
            pl.semaphore_signal(bar, inc=1, device_id=idx(xx, z, 0))
            pl.semaphore_signal(bar, inc=1, device_id=idx(xx, wrap(z + HALF), 1))
        for step in (1, -1):
            pl.semaphore_signal(bar, inc=1, device_id=idx(x, wrap(z + step), 1))
        pl.semaphore_signal(bar, inc=1, device_id=twin)

    gate_at = pl.ds(mo(c * UNITS, UNITS), UNITS)
    up_at = pl.ds(mo((NC + c) * UNITS, UNITS), UNITS)
    vu_at = pl.ds(mo(c * (VH // NC), VH // NC), VH // NC)
    router_copy = pltpu.make_async_copy(
        router_h.at[:, pl.ds(mo(x * DX, 128), DX)], rout_v.at[pl.ds(0, EXPERTS), :], l_weights.at[1])
    gate_copy = pltpu.make_async_copy(wg_h, wgu_v.at[:, gate_at], l_weights.at[1])
    up_copy = pltpu.make_async_copy(wu_h, wgu_v.at[:, up_at], l_weights.at[2])
    vu_copy = pltpu.make_async_copy(vu_h, vu_v.at[vu_at, :], l_weights.at[0])

    def wo_rows(xx, cc):
        return pl.ds(mo(xx * VH + cc * (VH // NC), VH // NC), VH // NC)

    def own_columns(xx):
        return pl.ds(mo(xx * DX, 128), DX)

    def wd_rows(xx, cc):
        return pl.ds(mo((xx * NC + cc) * UNITS, UNITS), UNITS)

    wo_copy = pltpu.make_async_copy(wo_h.at[:, own_columns(x)], wo_v.at[wo_rows(x, 1), :], l_weights.at[0])
    wd_copy = pltpu.make_async_copy(wd_h.at[:, own_columns(x)], wd_v.at[wd_rows(x, half), :], l_weights.at[2])

    def wo_send(source):
        for i in range(NX - 1):
            xx = xwrap(x + i + 1)
            send(source.at[:, own_columns(xx)], wo_v.at[wo_rows(x, half), :], s_wo, r_wox.at[i], idx(xx, z, 1))

    def row_next():
        @pl.when(main & (half == 0))
        def _():
            arrived(won_v.at[:, pl.ds(0, (NX - 1) * DX)], r_core.at[2])
            wo_send(won_v)

    def row_start():
        @pl.when(side)
        def _():
            pl.semaphore_wait(bar, NX)
            pl.semaphore_signal(row_sem, inc=1, device_id=idx(x, z, 1))

        @pl.when(main)
        def _():
            pl.semaphore_wait(row_sem, 1)

        @pl.when(main)
        def _():
            @pl.when(half == 1)
            def _():
                wo_send(wo_h)
            wo_copy.start()
            send(vu_h, vu_v.at[vu_at, :], s_core.at[0], r_core.at[0], idx(x, z, 0))
            rout_v[...] = jnp.zeros_like(rout_v)
            router_copy.start()

        @pl.when(side)
        def _():
            vu_copy.start()
            @pl.when(half == 0)
            def _():
                for i in range(NX - 1):
                    columns = own_columns(xwrap(x + i + 1))
                    send(wo_h.at[:, columns], won_v.at[:, columns], s_core.at[0], r_core.at[2], idx(x, z, 1))
            send(wo_h.at[:, own_columns(x)], wo_v.at[wo_rows(x, 0), :], s_wo, r_wo, idx(x, z, 1))

    scale = 1.0 / math.sqrt(QK)
    blk = 512
    nblk = cache_v.shape[2] // blk
    loads[0].wait()
    small[0].wait()
    small[1].wait()
    for b in range(2):
        qb = q_v[b]
        qf = qb.astype(F32)
        step_of = iota((2 * H, 1), 0) // H
        new_rows = [new_ref[b, pl.ds(t, 1), :].astype(F32) for t in range(2)]
        s_new = [jnp.sum(qf * row, axis=1, keepdims=True) * scale for row in new_rows]
        s_new[1] = jnp.where(step_of >= 1, s_new[1], -jnp.inf)
        peak = jnp.maximum(s_new[0], s_new[1])
        loads[1 + b].wait()
        for p in range(nblk):
            sc = nn(qb, cache_v[b, :, pl.ds(p * blk, blk)]) * scale
            pos = iota((2 * H, blk), 1) + p * blk
            sc = jnp.where(pos < len_ref[b], sc, -jnp.inf)
            score_v[:, pl.ds(p * blk, blk)] = sc
            peak = jnp.maximum(peak, jnp.max(sc, axis=1, keepdims=True))
        if b == 0:
            row_start()
        else:
            row_next()
        p_new = [jnp.exp(s - peak) for s in s_new]
        total = p_new[0] + p_new[1]
        acc = p_new[0].astype(BF16).astype(F32) * new_rows[0][:, :LAT]
        acc = acc + p_new[1].astype(BF16).astype(F32) * new_rows[1][:, :LAT]
        for p in range(nblk):
            pr = jnp.exp(score_v[:, pl.ds(p * blk, blk)] - peak)
            total = total + jnp.sum(pr, axis=1, keepdims=True)
            acc = acc + nt(pr.astype(BF16), cache_v[b, pl.ds(0, LAT), pl.ds(p * blk, blk)])
        ctx = acc / total
        for s in range(2):
            for j in range(LAT // 128):
                stage_v[pl.ds(j * TOK + b * 2 + s, H, stride=16), :] = ctx[s * H:(s + 1) * H, j * 128:(j + 1) * 128]
    ctx_v[...] = stage_v[...].reshape(H, 16, 128).astype(BF16)

    @pl.when(main)
    def _():
        send(ctx_v, ctxn_v, s_ctx.at[0], r_core.at[1], idx(x, z, 0))
        pl.semaphore_wait(bar, NX * NZ + NX + 3)
        pl.semaphore_signal(all_sem, inc=1, device_id=idx(x, z, 0))

    @pl.when(side)
    def _():
        arrived(ctxn_v, r_core.at[1])
        pl.semaphore_wait(all_sem, 1)

    def near(o):
        return wrap(jnp.where(lax.rem(o, 2) == 1, z - (o + 1) // 2, z + o // 2))

    def ctx_send(o, carry):
        zz = near(o)
        for i in range(NX):
            xx = xwrap(x + i + 1)
            own = (zz == z) & (xx == x)
            for core, tiles in ((0, ctx_v), (1, ctxn_v)):
                @pl.when(jnp.logical_not(own))
                def _():
                    send(tiles.at[xx * NZ + zz], arr_v.at[z, x * NC + core], s_ctx.at[core], r_row.at[z],
                         idx(xx, zz, 0))

                @pl.when(own)
                def _():
                    arr_v[z, x * NC + core] = tiles[xx * NZ + zz]
        return carry

    @pl.when(side)
    def _():
        lax.fori_loop(0, NZ, ctx_send, 0)

        @pl.when(half == 0)
        def _():
            for i in range(NX - 1):
                columns = own_columns(xwrap(x + i + 1))
                send(wd_h.at[:, columns], wdn_v.at[:, columns], s_wd.at[0], r_core.at[0], idx(x, z, 1))
            send(wd_h.at[:, own_columns(x)], wd_v.at[wd_rows(x, half), :], s_wd.at[1], r_wd.at[0], idx(x, z, 1))

    @pl.when(main)
    def _():
        for i in range(NX - 1):
            xx = xwrap(x + NX - i - 1)
            view = wo_v.at[wo_rows(xx, half), :]
            arrived(view, r_wox.at[i])
            send(view, view, s_wo, r_woy, twin)

        def wd_send(source):
            for i in range(NX - 1):
                xx = xwrap(x + i + 1)
                send(source.at[:, own_columns(xx)], wd_v.at[wd_rows(x, half), :], s_wd.at[0], r_wd.at[1], idx(xx, z, 1))

        @pl.when(half == 0)
        def _():
            arrived(wdn_v.at[:, pl.ds(0, (NX - 1) * DX)], r_core.at[0])
            wd_send(wdn_v)

        @pl.when(half == 1)
        def _():
            wd_copy.start()
            wd_send(wd_h)
        send(wg_h, wgu_v.at[:, gate_at], s_core.at[1], r_core.at[2], idx(x, z, 0))
        send(wu_h, wgu_v.at[:, up_at], s_core.at[2], r_core.at[3], idx(x, z, 0))

    @pl.when(side)
    def _():
        gate_copy.start()
        up_copy.start()

    for load in small[2:]:
        load.wait()

    rows8, lanes8 = iota((8, 128), 0), iota((8, 128), 1)
    table = jnp.zeros((8, 128), F32)
    for t in range(TOK):
        for k in range(TOP):
            hit = (rows8 == t) & (lanes8 == ids_ref[t // 2, t % 2, k] + LANE_TAB)
            table = jnp.where(hit, (slots_ref[t // 2, t % 2, k] + 1).astype(F32), table)
    tab_s[...] = table

    resf_v[...] = jnp.zeros_like(resf_v)
    for t in range(TOK):
        row = resid_ref[t // 2, pl.ds(t % 2, 1), :].astype(F32)
        for xx in range(NX):
            for j in range(JX):
                col = xx * DX + j * 128
                resf_v[pl.ds(xx * MSG + t * JX + j, 1), :] = row[:, col:col + 128]
    ress_v[...] = resf_v[...].reshape(NX, MSG, 128).astype(BF16)

    def to_home():
        for i in range(NX):
            xx = xwrap(x + i)
            send(tab_s, tab_v.at[dev], s_tab, r_tab, idx(xx, wrap(z + HALF), 1))
            send(ress_v.at[xx], res_v.at[dev], s_res, r_res, idx(xx, wrap(z + HALF), 1))

    def up_down(k):
        return wrap(z - k), wrap(z + k)

    early = jnp.where(lax.rem(z, CUBE) < CUBE // 2, 1, 0)
    last = wrap(z + HALF)

    def along(way):
        return idx(x, wrap(z + 1 - 2 * way), c)

    def ways(pieces):
        for i in range(pieces + 1):
            if i < pieces:
                yield i, early
            if i > 0:
                yield i - 1, 1 - early

    def slot_r(s):
        return lax.rem(s, 3)

    def slot_l(s):
        return 3 + lax.rem(s, 3)

    def slot_g(k):
        return lax.rem(k + 2, 3)

    def chain_send(in_ref, out_buf, ssem, slot, way, s, i, total):
        at = pl.ds(*SUBS[i])
        out_buf[way, s, :, at] = total.astype(BF16)
        send(out_buf.at[way, s, :, at], in_ref.at[way, s + 1, :, at], ssem.at[way], r_ring.at[way, slot(s + 1), i],
             along(way))

    def chain_piece(in_ref, out_buf, ssem, slot, s, i, way):
        at = pl.ds(*SUBS[i])
        r = wrap(z - (1 - 2 * way) * s)

        @pl.when((way == 0) | (s >= 2))
        def _():
            arrived(in_ref.at[way, s, :, at], r_ring.at[way, slot(s), i])
        chain_send(in_ref, out_buf, ssem, slot, way, s, i, part_v[r, :, at] + in_ref[way, s, :, at].astype(F32))

    def chain_step(in_ref, out_buf, ssem, slot, s):
        for i, way in ways(NS):
            chain_piece(in_ref, out_buf, ssem, slot, s, i, way)

    def chain_end(in_ref, slot, i):
        at = pl.ds(*SUBS[i])
        for way in range(2):
            arrived(in_ref.at[way, HALF, :, at], r_ring.at[way, slot(HALF), i])
        return part_v[last, :, at] + in_ref[0, HALF, :, at].astype(F32) + in_ref[1, HALF, :, at].astype(F32)

    @pl.when(side)
    def _side():
        vu_copy.wait()
        arrived(vu_v.at[pl.ds(0, VH // NC), :], r_core.at[0])
        own_lanes = pl.ds(mo(x * VH, VH), VH)

        def ctx_row(r):
            @pl.when(r == z)
            def _():
                arrived(arr_v.at[r, pl.ds(0, DEV - NC)], r_row.at[r])

            @pl.when(r != z)
            def _():
                arrived(arr_v.at[r], r_row.at[r])

            arrf_v[...] = arr_v[r].reshape(DEV * 16, 128).astype(F32)
            cols = []
            for j in range(LAT // 128):
                cols.append(jnp.concatenate(
                    [arrf_v[pl.ds(j * TOK + t, DEV, stride=16), :] for t in range(TOK)], axis=0))
            rows = jnp.concatenate(cols, axis=1).astype(BF16)
            val_v[r, :, own_lanes] = nt(rows, vu_v[...]).astype(BF16)
            view = val_v.at[r, :, own_lanes]
            for i in range(NX):
                send(view, view, s_val, r_row.at[r], idx(xwrap(x + i + 1), z, 1))

        def ctx_step(o, carry):
            ctx_row(near(o))
            return carry
        lax.fori_loop(0, NZ, ctx_step, 0)
        to_home()

        gate_copy.wait()
        up_copy.wait()
        arrived(wgu_v.at[:, pl.ds(0, UNITS)], r_core.at[2])
        arrived(wgu_v.at[:, pl.ds(0, UNITS)], r_core.at[3])

        own_expert = x * QUAD + quad

        def experts(rows):
            for r in rows:
                arrived(d_v.at[r], r_row.at[r])
            both = jnp.zeros((SLOT * len(rows), 2 * NC * UNITS), F32)
            ext = jnp.zeros((SLOT * len(rows), EXT), F32)
            shared = jnp.concatenate([d_v[r, NX] for r in rows], axis=0)
            for xx in range(NX):
                both = both + nn(
                    jnp.concatenate([d_v[r, xx, :, pl.ds(0, DA)] for r in rows], axis=0),
                    wgu_v[xx * DX:xx * DX + DA, :])
                both = both + nn(shared[:, xx * BX:(xx + 1) * BX], wgu_v[xx * DX + DA:(xx + 1) * DX, :])
                piece = jnp.concatenate([d_v[r, xx, :, pl.ds(DA, EXT)] for r in rows], axis=0).astype(F32)
                ext = ext + piece
            lane = iota(ext.shape, 1)
            squares = jnp.sum(
                jnp.where((lane == LANE_SUM) | (lane == LANE_SUM + 1), ext, 0.0), axis=1, keepdims=True)
            inv = lax.rsqrt(squares / D + norm_eps)
            logits = (ext + pltpu.roll(ext, EXT - EXPERTS, 1)) * inv
            named = (pltpu.roll(piece, EXT - LANE_TAB, 1) > 0.0) & (lane < EXPERTS)
            gates = jnp.where(named, 1.0 / (1.0 + jnp.exp(-logits)), 0.0)
            norm = jnp.sum(gates, axis=1, keepdims=True)
            mine = jnp.sum(jnp.where(lane == own_expert, gates, 0.0), axis=1, keepdims=True)
            share = jnp.where(norm > 0.0, route_scale * mine / norm, 0.0)
            gate = both[:, :NC * UNITS] * inv
            upward = both[:, NC * UNITS:] * inv
            act = (gate / (1.0 + jnp.exp(-gate)) * upward * share).astype(BF16)
            for i, r in enumerate(rows):
                act_s[r] = act[i * SLOT:(i + 1) * SLOT]
                for n in range(NX):
                    send(act_s.at[r], act_v.at[r, x], s_act, r_row.at[r], idx(xwrap(x + n + 1), z, 1))

        experts([z])

        def step(k, carry):
            experts(list(up_down(k)))
            return carry
        lax.fori_loop(1, HALF, step, 0)
        experts([last])

        arrived(ctx_v.at[pl.ds(0, NX * NZ - 1)], s_ctx.at[0])
        arrived(ctx_v.at[pl.ds(0, NX * NZ - 1)], s_ctx.at[1])
        @pl.when(half == 0)
        def _():
            arrived(won_v.at[:, pl.ds(0, (NX - 1) * DX)], s_core.at[0])
        arrived(wo_v.at[pl.ds(0, VH // NC), :], s_wo)
        arrived(tab_v.at[pl.ds(0, NX)], s_tab)
        arrived(res_v.at[pl.ds(0, NX)], s_res)

        @pl.when(half == 0)
        def _():
            arrived(wdn_v.at[:, pl.ds(0, (NX - 1) * DX)], s_wd.at[0])
            arrived(wdn_v.at[:, pl.ds(0, DX)], s_wd.at[1])
        arrived(val_v, s_val)
        arrived(act_v, s_act)
        arrived(sum_v, r_out)

    @pl.when(main)
    def _main():
        gain_v[...] = gain_ref[...].astype(F32)
        rs_in[1, 1] = jnp.zeros((ROW, DX), BF16)
        rs2_in[1, 1] = jnp.zeros((ROW, DX), BF16)

        def twin_send(xx):
            view = wd_v.at[wd_rows(xx, half), :]
            send(view, view, s_wd.at[1], r_twin, twin)

        @pl.when(half == 0)
        def _():
            arrived(wd_v.at[wd_rows(x, half), :], r_wd.at[0])

        @pl.when(half == 1)
        def _():
            wd_copy.wait()
        twin_send(x)

        wo_copy.wait()
        arrived(wo_v.at[wo_rows(x, 0), :], r_wo)
        arrived(wo_v.at[pl.ds(0, (NX - 1) * (VH // NC)), :], r_woy)
        to_home()

        def attended(rows):
            for r in rows:
                arrived(val_v.at[r], r_row.at[r])
            stacked = jnp.concatenate([val_v[r] for r in rows], axis=0)
            for o, w in BLOCKS:
                part = nn(stacked, wo_v[:, o:o + w])
                for i, r in enumerate(rows):
                    part_v[r, :, pl.ds(o, w)] = part[i * ROW:(i + 1) * ROW]

        arrived(val_v.at[z], r_row.at[z])
        for i, (o, w) in enumerate(SUBS):
            chain_send(rs_in, rs_out, s_rs, slot_r, 0, 0, i, nn(val_v[z], wo_v[:, o:o + w]))
        attended(list(up_down(1)))

        def rs_step(s, carry):
            chain_step(rs_in, rs_out, s_rs, slot_r, s)

            @pl.when(s < HALF - 1)
            def _():
                attended(list(up_down(s + 1)))

            @pl.when(s == HALF // 2)
            def _():
                arrived(wd_v.at[pl.ds(0, (NX - 1) * UNITS), :], r_wd.at[1])
                for i in range(NX - 1):
                    twin_send(xwrap(x + i + 1))
            return carry
        lax.fori_loop(1, HALF, rs_step, 0)
        attended([last])

        arrived(res_v, r_res)
        arrived(tab_v, r_tab)
        resw_v[...] = res_v[...].reshape(DEV * MSG, 128).astype(F32)
        lane = iota((ROW, 128), 1)
        rows = iota((DEV, 128), 0)
        tabs = []
        for t in range(TOK):
            piece = jnp.zeros((DEV, 128), F32)
            for d in range(DEV):
                piece = jnp.where(rows == d, tab_v[d, pl.ds(t, 1), :], piece)
            tabs.append(piece)
        table_rows = jnp.concatenate(tabs, axis=0)
        router_copy.wait()

        def ag_send(r, i, way, k):
            view = ag_v.at[r, :, pl.ds(i * PIECE, PIECE)]
            send(view, view, s_ag.at[way], r_ring.at[way, slot_g(k), i], along(way))

        def ag_wait(r, i, way, k):
            arrived(ag_v.at[r, :, pl.ds(i * PIECE, PIECE)], r_ring.at[way, slot_g(k), i])

        sums = jnp.zeros((ROW, 1), F32)
        logits = jnp.zeros((ROW, 128), F32)
        bx_at = pl.ds(mo(DAE + x * BX, 128), BX)
        for i, (o, w) in enumerate(SUBS):
            attn = chain_end(rs_in, slot_r, i)
            att_v[:, pl.ds(o, w)] = attn
            hidden = attn + jnp.concatenate([
                jnp.concatenate([resw_v[pl.ds(t * JX + j, DEV, stride=MSG), :] for t in range(TOK)], axis=0)
                for j in range(o // 128, (o + w) // 128)], axis=1)
            gain = jnp.concatenate(
                [gain_v[pl.ds(x * JX + j, 1), :] for j in range(o // 128, (o + w) // 128)], axis=1)
            scaled = (hidden * gain).astype(BF16)
            if i == 0:
                ag_v[z, :, bx_at] = scaled
                view = ag_v.at[z, :, bx_at]
                for j in range(NX - 1):
                    send(view, view, s_bx, r_bx, idx(xwrap(x + j + 1), z, 1))
            else:
                ag_v[z, :, pl.ds(o, w)] = scaled
                if o + w >= PIECE > o:
                    ag_send(z, 0, 0, 1)
                    ag_send(z, 0, 1, 1)
            sums = sums + jnp.sum(hidden * hidden, axis=1, keepdims=True)
            logits = logits + nt(scaled, rout_v[:, pl.ds(o, w)])
        high = logits.astype(BF16).astype(F32)
        sums_high = sums.astype(BF16).astype(F32)
        ext = high + pltpu.roll(logits - high, EXPERTS, 1)
        ext = jnp.where(lane == LANE_SUM, sums_high, ext)
        ext = jnp.where(lane == LANE_SUM + 1, sums - sums_high, ext)
        ag_v[z, :, pl.ds(DA, EXT)] = (ext + table_rows).astype(BF16)
        ag_send(z, NPA - 1, 0, 1)
        ag_send(z, NPA - 1, 1, 1)
        arrived(ag_v.at[z, :, pl.ds(DAE, (NX - 1) * BX)], r_bx)
        for i in range(NPA, NP):
            ag_send(z, i, 0, 1)
            ag_send(z, i, 1, 1)

        def dispatch(rows):
            n = len(rows)
            size = n * NX * SLOT
            jj, lane = iota((size, 128), 0), iota((size, 128), 1)
            wanted_lane = LANE_TAB + lax.rem(x + lax.rem(jj // SLOT, NX), NX) * QUAD + quad
            pick = jnp.where(lane == wanted_lane, 1.0, 0.0).astype(BF16)
            picked = nt(pick, jnp.concatenate([ag_v[r, :, pl.ds(DA, EXT)] for r in rows], axis=0))
            jj, tok = iota((size, n * ROW), 0), iota((size, n * ROW), 1)
            wanted = (lax.rem(jj, SLOT) // DEV + 1).astype(F32)
            hit = (picked == wanted) & (lax.rem(jj, DEV) == lax.rem(tok, DEV)) & (jj // (NX * SLOT) == tok // ROW)
            place = jnp.where(hit, 1.0, 0.0).astype(BF16)
            moved = nn(place, jnp.concatenate([ag_v[r, :, pl.ds(0, DAE)] for r in rows], axis=0)).astype(BF16)
            own = jnp.concatenate([place[i * NX * SLOT:i * NX * SLOT + SLOT] for i in range(n)], axis=0)
            shared = nn(own, jnp.concatenate([ag_v[r, :, pl.ds(DAE, NX * BX)] for r in rows], axis=0)).astype(BF16)
            for i, r in enumerate(rows):
                dsp_v[r, pl.ds(0, NX)] = moved[i * NX * SLOT:(i + 1) * NX * SLOT].reshape(NX, SLOT, DAE)
                dsp_v[r, NX] = shared[i * SLOT:(i + 1) * SLOT]
            for r in rows:
                for i in (2, 1, 3):
                    send(dsp_v.at[r, i], d_v.at[r, x], s_dsp, r_row.at[r], idx(xwrap(x + i), z, 0))
                send(dsp_v.at[r, 0], d_v.at[r, x], s_dsp, r_row.at[r], idx(x, z, 0))
                send(dsp_v.at[r, NX], d_v.at[r, NX], s_dsp, r_row.at[r], idx(x, z, 0))

        def returned(rows):
            n = len(rows)
            for r in rows:
                arrived(act_v.at[r], r_row.at[r])
            size = n * NX * SLOT
            jj, lane = iota((size, 128), 0), iota((size, 128), 1)
            wanted_lane = LANE_TAB + jj // (n * SLOT) * QUAD + quad
            pick = jnp.where(lane == wanted_lane, 1.0, 0.0).astype(BF16)
            picked = nt(jnp.concatenate([ag_v[r, :, pl.ds(DA, EXT)] for r in rows], axis=0), pick)
            jj, tok = iota((n * ROW, size), 1), iota((n * ROW, size), 0)
            wanted = (lax.rem(jj, SLOT) // DEV + 1).astype(F32)
            hit = (picked == wanted) & (lax.rem(jj, DEV) == lax.rem(tok, DEV)) & (
                lax.rem(jj // SLOT, n) == tok // ROW)
            place = jnp.where(hit, 1.0, 0.0).astype(BF16)
            spread = []
            for i in range(NX):
                acts = jnp.concatenate([act_v[r, i] for r in rows], axis=0)
                spread.append(nn(place[:, i * n * SLOT:(i + 1) * n * SLOT], acts).astype(BF16))
            return jnp.concatenate(spread, axis=1)

        def down_blocks(rows, blocks):
            for o, w in blocks:
                at = pl.ds(o, w)
                part = nn(at_v[...], wd_v[:, o:o + w])
                for i, r in enumerate(rows):
                    part_v[r, :, at] = part[i * ROW:(i + 1) * ROW]

        def down_part(rows):
            at_v[pl.ds(0, len(rows) * ROW), :] = returned(rows)
            down_blocks(rows, BLOCKS)

        def down_first():
            spread = returned([z])
            for o, w in BLOCKS:
                at = pl.ds(o, w)
                part_v[z, :, at] = nn(spread, wd_v[:, o:o + w]) + att_v[:, at]
        at_v[...] = jnp.zeros_like(at_v)
        dispatch([z])

        def ag_step(k, carry):
            behind = list(up_down(k - 1))
            done = list(up_down(k - DOWN - 1))

            def pieces(i):
                for way in (early, 1 - early):
                    r = wrap(z - (1 - 2 * way) * k)
                    ag_wait(r, i, way, k)

                    @pl.when((way == 0) | (k < HALF - 1))
                    def _():
                        ag_send(r, i, way, k + 1)
            def follow(i):
                @pl.when(k > DOWN + 1)
                def _():
                    for way in (early, 1 - early):
                        chain_piece(rs2_in, rs2_out, s_rs2, slot_l, k - DOWN - 1, i, way)
            pieces(0)

            @pl.when(k >= 2)
            def _():
                dispatch(behind)
            pieces(1)

            @pl.when(k == DOWN)
            def _():
                arrived(wd_v.at[pl.ds(0, NX * UNITS), :], r_twin)
                down_first()

            @pl.when(k > DOWN + 1)
            def _():
                at_v[...] = returned(done)
                down_blocks(done, BLOCKS[:1])
            pieces(2)

            @pl.when(k == DOWN + 1)
            def _():
                for i, (o, w) in enumerate(SUBS):
                    chain_send(rs2_in, rs2_out, s_rs2, slot_l, 0, 0, i, part_v[z, :, pl.ds(o, w)])

            @pl.when(k > DOWN + 1)
            def _():
                down_blocks(done, BLOCKS[1:])
            pieces(3)
            for i in range(NS):
                follow(i)
            return carry
        lax.fori_loop(1, HALF, ag_step, 0)
        dispatch(list(up_down(HALF - 1)))
        for i in range(NP):
            ag_wait(last, i, 0, HALF)
        dispatch([last])

        down_part(list(up_down(HALF - DOWN - 1)))

        def late(k, carry):
            chain_step(rs2_in, rs2_out, s_rs2, slot_l, k - 1)
            down_part(list(up_down(k)))
            return carry
        lax.fori_loop(HALF - DOWN, HALF, late, 0)
        chain_step(rs2_in, rs2_out, s_rs2, slot_l, HALF - 1)
        down_part([last])

        for t in range(TOK * JX, MSG):
            fin_v[pl.ds(t, DEV, stride=MSG), :] = jnp.zeros((DEV, 128), F32)
        for i, (o, w) in enumerate(SUBS):
            mixed = chain_end(rs2_in, slot_l, i)
            for t in range(TOK):
                for j in range(o // 128, (o + w) // 128):
                    fin_v[pl.ds(t * JX + j, DEV, stride=MSG), :] = (
                        mixed[t * DEV:(t + 1) * DEV, j * 128 - o:j * 128 - o + 128])
        fin_s[...] = fin_v[...].reshape(DEV, MSG, 128).astype(BF16)
        for i in range(DEV - 1):
            to = lax.rem(dev + i + 1, DEV)
            send(fin_s.at[to], sum_v.at[x], s_out, r_out, idx(to // NC, z, lax.rem(to, NC)))
        sum_v[x] = fin_s[dev]

        arrived(ctx_v, s_ctx.at[0])
        arrived(wo_v.at[pl.ds(0, 2 * (NX - 1) * (VH // NC)), :], s_wo)
        arrived(tab_v.at[pl.ds(0, NX)], s_tab)
        arrived(res_v.at[pl.ds(0, NX)], s_res)
        arrived(vu_v.at[pl.ds(0, VH // NC), :], s_core.at[0])
        arrived(wgu_v.at[:, pl.ds(0, UNITS)], s_core.at[1])
        arrived(wgu_v.at[:, pl.ds(0, UNITS)], s_core.at[2])
        arrived(wd_v.at[pl.ds(0, (NX - 1) * UNITS), :], s_wd.at[0])
        arrived(wd_v.at[pl.ds(0, NX * UNITS), :], s_wd.at[1])
        for way in range(2):
            arrived(rs_out.at[way, pl.ds(way, HALF - way)], s_rs.at[way])
            arrived(rs2_out.at[way, pl.ds(way, HALF - way)], s_rs2.at[way])
            arrived(ag_v.at[pl.ds(0, HALF - way)], s_ag.at[way])
        arrived(ag_v.at[z, :, pl.ds(DAE, (NX - 1) * BX)], s_bx)
        arrived(dsp_v, s_dsp)
        arrived(fin_s.at[pl.ds(0, DEV - 1)], s_out)
        arrived(sum_v.at[pl.ds(0, NX - 1)], r_out)

    total = sum_v[...].reshape(NX * MSG, 128).astype(F32) + resf_v[...]
    ress_v[...] = total.reshape(NX, MSG, 128).astype(BF16)
    out_copy = pltpu.make_async_copy(ress_v, out_ref, l_misc)
    out_copy.start()
    out_copy.wait()


def body(
    cache_kv, new_kv, queries, lengths, resid, value_up, out_proj, norm_gain, router, expert_ids, slots, w_gate, w_up,
    w_down,
):
    seqs, steps = resid.shape[:2]
    cache_len = cache_kv.shape[1]
    hbm = pl.BlockSpec(memory_space=pltpu.HBM)
    dma = pltpu.SemaphoreType.DMA
    regular = pltpu.SemaphoreType.REGULAR
    scratch = [
        pltpu.VMEM(new_kv.shape, BF16),
        pltpu.SMEM(lengths.shape, jnp.int32),
        pltpu.VMEM(resid.shape, BF16),
        pltpu.VMEM((D // 128, 128), BF16),
        pltpu.SMEM(expert_ids.shape, jnp.int32),
        pltpu.SMEM(slots.shape, jnp.int32),
        pltpu.VMEM((seqs, KV, cache_len), BF16),
        pltpu.VMEM((seqs, steps * H, KV), BF16),
        pltpu.VMEM((steps * H, cache_len), F32),
        pltpu.VMEM((H * 16, 128), F32),
        pltpu.VMEM((H, 16, 128), BF16),
        pltpu.VMEM((NZ, DEV, 16, 128), BF16),
        pltpu.VMEM((DEV * 16, 128), F32),
        pltpu.VMEM((VH, LAT), BF16),
        pltpu.VMEM((NZ, ROW, NX * VH), BF16),
        pltpu.VMEM((NX * VH, DX), BF16),
        pltpu.VMEM((H, 16, 128), BF16),
        pltpu.VMEM((VH // NC, D), BF16),
        pltpu.VMEM((2 * ROW, NX * NC * UNITS), BF16),
        pltpu.VMEM((2, HALF + 1, ROW, DX), BF16),
        pltpu.VMEM((2, HALF, ROW, DX), BF16),
        pltpu.VMEM((ROW, DX), F32),
        pltpu.VMEM((8, 128), F32),
        pltpu.VMEM((DEV, 8, 128), F32),
        pltpu.VMEM((NX, MSG, 128), BF16),
        pltpu.VMEM((NX * MSG, 128), F32),
        pltpu.VMEM((DEV, MSG, 128), BF16),
        pltpu.VMEM((DEV * MSG, 128), F32),
        pltpu.VMEM((D // 128, 128), F32),
        pltpu.VMEM((128, DX), BF16),
        pltpu.VMEM((NZ, ROW, DG), BF16),
        pltpu.VMEM((NZ, NX + 1, SLOT, DAE), BF16),
        pltpu.VMEM((NZ, NX + 1, SLOT, DAE), BF16),
        pltpu.VMEM((D, 2 * NC * UNITS), BF16),
        pltpu.VMEM((NZ, SLOT, NC * UNITS), BF16),
        pltpu.VMEM((NZ, NX, SLOT, NC * UNITS), BF16),
        pltpu.VMEM((NX * NC * UNITS, DX), BF16),
        pltpu.VMEM((UNITS, D), BF16),
        pltpu.VMEM((2, HALF + 1, ROW, DX), BF16),
        pltpu.VMEM((2, HALF, ROW, DX), BF16),
        pltpu.VMEM((NZ, ROW, DX), F32),
        pltpu.VMEM((DEV * MSG, 128), F32),
        pltpu.VMEM((DEV, MSG, 128), BF16),
        pltpu.VMEM((NX, MSG, 128), BF16),
        dma((seqs,)), dma, dma((3,)), dma((6,)),
        dma((2,)), dma, dma, dma, dma((3,)), dma((2,)), dma, dma((2,)), dma((2,)), dma((2,)), dma, dma, dma, dma,
        dma, dma, dma, dma((3,)), dma, dma((4,)), dma((2,)), dma((NZ,)), dma((2, 6, NP)), dma, dma, dma,
        regular, regular,
    ]
    out = pl.pallas_call(
        kernel,
        out_shape=jax.ShapeDtypeStruct((NX, MSG, 128), BF16),
        in_specs=[hbm] * 14,
        out_specs=hbm,
        scratch_shapes=scratch,
        compiler_params=pltpu.CompilerParams(
            collective_id=0, has_side_effects=True, vmem_limit_bytes=(64 << 20) - (64 << 10)),
        name="layer",
    )(
        jnp.transpose(cache_kv, (0, 2, 1)), new_kv, queries.reshape(seqs, steps * H, KV), lengths, resid,
        value_up.T, out_proj, norm_gain.reshape(D // 128, 128), router.T, expert_ids, slots, w_gate, w_up, w_down,
    )
    out = out[:, :TOK * JX].reshape(NX, TOK, JX, 128).transpose(1, 0, 2, 3)
    return out.reshape(resid.shape)


def solution(mesh):
    return jax.shard_map(
        body,
        mesh=mesh,
        in_specs=(
            P(("rep", "ep"), None, None),
            P(("rep", "ep"), None, None),
            P(("rep", "ep"), None, None, None),
            P(("rep", "ep")),
            P(("rep", "ep"), None, None),
            P(None, "ep"),
            P("ep", None),
            P(),
            P(),
            P(("rep", "ep"), None, None),
            P(("rep", "ep"), None, None),
            P(None, "ep"),
            P(None, "ep"),
            P("ep", None),
        ),
        out_specs=P(("rep", "ep"), None, None),
        check_vma=False,
    )
```

```python
import functools
import math

import jax
import jax.numpy as jnp
from jax import lax
from jax.experimental import pallas as pl
from jax.experimental.pallas import tpu as pltpu
from jax.sharding import PartitionSpec as P

NX, NZ, NC = 4, 16, 2
DEV = NX * NC
HALF = NZ // 2

D = 7168
H = 64
LAT = 512
VH = 128
KV = 576
EXPERTS = 16
TOP = 8
CAP = 2
QK = 192
TOK = 4
UNITS = 128
ROW = DEV * TOK
SLOT = DEV * CAP
DX = D // NX
EXT = 128
JX = DX // 128
MSG = 64
LANE_SUM = 32
LANE_TOK = 48
LANE_TAB = 64
QUAD = EXPERTS // NX
CHIPS_PER = NZ // QUAD

route_scale = 2.827
norm_eps = 1e-06

CUBE = 4

BX = 384
DA = DX - BX
DAE = DA + EXT
DG = DAE + NX * BX
PIECE = 768
SUBS = ((DA, BX), (0, 512), (512, 512), (1024, 384))
NS = len(SUBS)
NP = DG // PIECE
NPA = DAE // PIECE
BLOCKS = ((0, 512), (512, 512), (1024, 768))
DOWN = 4

F32 = jnp.float32
BF16 = jnp.bfloat16


def mo(value, by):
    return pl.multiple_of(value, by)


def nt(a, b):
    return lax.dot_general(a, b, (((1,), (1,)), ((), ())), preferred_element_type=F32)


def nn(a, b):
    return lax.dot_general(a, b, (((1,), (0,)), ((), ())), preferred_element_type=F32)


def iota(shape, axis):
    return lax.broadcasted_iota(jnp.int32, shape, axis)


def kernel(
    cache_h, new_h, q_h, len_h, resid_h, vu_h, wo_h, gain_h, router_h, ids_h, slots_h, wg_h, wu_h, wd_h,
    out_ref,
    new_ref, len_ref, resid_ref, gain_ref, ids_ref, slots_ref,
    cache_v, q_v, score_v, stage_v, ctx_v, arr_v, arrf_v, vu_v, val_v, wo_v, ctxn_v, won_v, rs_in, rs_out, att_v,
    ress_v, resf_v, res_v, resw_v, gain_v, rout_v, ag_v, dsp_v, d_v, wgu_v, act_s, act_v, wd_v, wdn_v, rs2_in, rs2_out,
    part_v, fin_v, fin_s, sum_v, outv_v,
    l_cache, l_misc, l_weights, l_small,
    s_ctx, s_res, s_wo, s_core, s_wd, s_val, s_rs, s_ag, s_rs2, s_dsp, s_act, s_out, s_bx,
    r_res, r_wo, r_wox, r_woy, r_core, r_wd, r_row, r_ring, r_out, r_bx, r_twin,
    row_sem, all_sem,
):
    me = lax.axis_index("ep")
    c = lax.rem(me, NC)
    z = lax.rem(me // NC, NZ)
    x = me // (NC * NZ)
    dev = x * NC + c
    quad = z // CHIPS_PER
    group = lax.axis_index("rep")
    half = lax.rem(group, 2)
    twin = {"rep": group + 1 - 2 * half, "ep": me}

    def idx(xx, zz, cc):
        return {"ep": (xx * NZ + zz) * NC + cc}

    def wrap(zz):
        return lax.rem(zz + 2 * NZ, NZ)

    def xwrap(xx):
        return lax.rem(xx, NX)

    def send(src, dst, ssem, rsem, to):
        pltpu.make_async_remote_copy(src_ref=src, dst_ref=dst, send_sem=ssem, recv_sem=rsem, device_id=to).start()

    def arrived(ref, sem):
        pltpu.make_async_copy(ref, ref, sem).wait()

    main = c == 1
    side = c == 0

    loads = [pltpu.make_async_copy(q_h, q_v, l_misc)]
    loads += [pltpu.make_async_copy(cache_h.at[b], cache_v.at[b], l_cache.at[b]) for b in range(2)]
    small = [
        pltpu.make_async_copy(src, dst, l_small.at[i]) for i, (src, dst) in enumerate((
            (new_h, new_ref), (len_h, len_ref), (resid_h, resid_ref), (gain_h, gain_ref), (ids_h, ids_ref),
            (slots_h, slots_ref)))
    ]
    for load in loads[:2] + small[:2] + loads[2:] + small[2:]:
        load.start()

    bar = pltpu.get_barrier_semaphore()

    @pl.when(side)
    def _():
        def greet(o, carry):
            far = HALF - (o + 1) // 2
            zz = wrap(jnp.where(lax.rem(o, 2) == 1, z + far, z - far))
            for xx in range(NX):
                pl.semaphore_signal(bar, inc=1, device_id=idx(xx, zz, 1))
            return carry
        lax.fori_loop(0, NZ, greet, 0)

    @pl.when(main)
    def _():
        for xx in range(NX):
            pl.semaphore_signal(bar, inc=1, device_id=idx(xx, z, 0))
            pl.semaphore_signal(bar, inc=1, device_id=idx(xx, wrap(z + HALF), 1))
        for step in (1, -1):
            pl.semaphore_signal(bar, inc=1, device_id=idx(x, wrap(z + step), 1))
        pl.semaphore_signal(bar, inc=1, device_id=twin)

    gate_at = pl.ds(mo(c * UNITS, UNITS), UNITS)
    up_at = pl.ds(mo((NC + c) * UNITS, UNITS), UNITS)
    vu_at = pl.ds(mo(c * (VH // NC), VH // NC), VH // NC)
    router_copy = pltpu.make_async_copy(
        router_h.at[:, pl.ds(mo(x * DX, 128), DX)], rout_v.at[pl.ds(0, EXPERTS), :], l_weights.at[1])
    gate_copy = pltpu.make_async_copy(wg_h, wgu_v.at[:, gate_at], l_weights.at[1])
    up_copy = pltpu.make_async_copy(wu_h, wgu_v.at[:, up_at], l_weights.at[2])
    vu_copy = pltpu.make_async_copy(vu_h, vu_v.at[vu_at, :], l_weights.at[0])

    def wo_rows(xx, cc):
        return pl.ds(mo(xx * VH + cc * (VH // NC), VH // NC), VH // NC)

    def own_columns(xx):
        return pl.ds(mo(xx * DX, 128), DX)

    def wd_rows(xx, cc):
        return pl.ds(mo((xx * NC + cc) * UNITS, UNITS), UNITS)

    wo_copy = pltpu.make_async_copy(wo_h.at[:, own_columns(x)], wo_v.at[wo_rows(x, 1), :], l_weights.at[0])
    wd_copy = pltpu.make_async_copy(wd_h.at[:, own_columns(x)], wd_v.at[wd_rows(x, half), :], l_weights.at[2])

    def wo_half(xx, h):
        return pl.ds(mo(xx * DX + h * (DX // 2), 128), DX // 2)

    def wo_send(source):
        for h in range(2):
            for i in range(NX - 1):
                xx = xwrap(x + i + 1)
                send(source.at[:, wo_half(xx, h)], wo_v.at[wo_rows(x, half), wo_half(0, h)], s_wo, r_wox.at[x, h],
                     idx(xx, z, 1))

    def row_next():
        @pl.when(main & (half == 0))
        def _():
            arrived(won_v.at[:, pl.ds(0, (NX - 1) * DX)], r_core.at[2])
            wo_send(won_v)

    def row_start():
        @pl.when(side)
        def _():
            pl.semaphore_wait(bar, NX)
            pl.semaphore_signal(row_sem, inc=1, device_id=idx(x, z, 1))

        @pl.when(main)
        def _():
            pl.semaphore_wait(row_sem, 1)

        @pl.when(main)
        def _():
            @pl.when(half == 1)
            def _():
                wo_send(wo_h)
            wo_copy.start()
            send(vu_h, vu_v.at[vu_at, :], s_core.at[0], r_core.at[0], idx(x, z, 0))
            rout_v[...] = jnp.zeros_like(rout_v)
            router_copy.start()

        @pl.when(side)
        def _():
            vu_copy.start()
            @pl.when(half == 0)
            def _():
                for i in range(NX - 1):
                    columns = own_columns(xwrap(x + i + 1))
                    send(wo_h.at[:, columns], won_v.at[:, columns], s_core.at[0], r_core.at[2], idx(x, z, 1))
            send(wo_h.at[:, own_columns(x)], wo_v.at[wo_rows(x, 0), :], s_wo, r_wo, idx(x, z, 1))

    scale = 1.0 / math.sqrt(QK)
    blk = 512
    nblk = cache_v.shape[2] // blk
    loads[0].wait()
    small[0].wait()
    small[1].wait()
    for b in range(2):
        qb = q_v[b]
        qf = qb.astype(F32)
        step_of = iota((2 * H, 1), 0) // H
        new_rows = [new_ref[b, pl.ds(t, 1), :].astype(F32) for t in range(2)]
        s_new = [jnp.sum(qf * row, axis=1, keepdims=True) * scale for row in new_rows]
        s_new[1] = jnp.where(step_of >= 1, s_new[1], -jnp.inf)
        peak = jnp.maximum(s_new[0], s_new[1])
        loads[1 + b].wait()
        for p in range(nblk):
            sc = nn(qb, cache_v[b, :, pl.ds(p * blk, blk)]) * scale
            pos = iota((2 * H, blk), 1) + p * blk
            sc = jnp.where(pos < len_ref[b], sc, -jnp.inf)
            score_v[:, pl.ds(p * blk, blk)] = sc
            peak = jnp.maximum(peak, jnp.max(sc, axis=1, keepdims=True))
        if b == 0:
            row_start()
        else:
            row_next()
        p_new = [jnp.exp(s - peak) for s in s_new]
        total = p_new[0] + p_new[1]
        acc = p_new[0].astype(BF16).astype(F32) * new_rows[0][:, :LAT]
        acc = acc + p_new[1].astype(BF16).astype(F32) * new_rows[1][:, :LAT]
        for p in range(nblk):
            pr = jnp.exp(score_v[:, pl.ds(p * blk, blk)] - peak)
            total = total + jnp.sum(pr, axis=1, keepdims=True)
            acc = acc + nt(pr.astype(BF16), cache_v[b, pl.ds(0, LAT), pl.ds(p * blk, blk)])
        ctx = acc / total
        for s in range(2):
            for j in range(LAT // 128):
                stage_v[pl.ds(j * TOK + b * 2 + s, H, stride=16), :] = ctx[s * H:(s + 1) * H, j * 128:(j + 1) * 128]
    ctx_v[...] = stage_v[...].reshape(H, 16, 128).astype(BF16)

    @pl.when(main)
    def _():
        send(ctx_v, ctxn_v, s_ctx.at[0], r_core.at[1], idx(x, z, 0))
        pl.semaphore_wait(bar, NX * NZ + NX + 3)
        pl.semaphore_signal(all_sem, inc=1, device_id=idx(x, z, 0))

    @pl.when(side)
    def _():
        arrived(ctxn_v, r_core.at[1])
        pl.semaphore_wait(all_sem, 1)

    def near(o):
        return wrap(jnp.where(lax.rem(o, 2) == 1, z - (o + 1) // 2, z + o // 2))

    def ctx_send(o, carry):
        zz = near(o)
        for i in range(NX):
            xx = xwrap(x + i + 1)
            own = (zz == z) & (xx == x)
            for core, tiles in ((0, ctx_v), (1, ctxn_v)):
                @pl.when(jnp.logical_not(own))
                def _():
                    send(tiles.at[xx * NZ + zz], arr_v.at[z, x * NC + core], s_ctx.at[core], r_row.at[z],
                         idx(xx, zz, 0))

                @pl.when(own)
                def _():
                    arr_v[z, x * NC + core] = tiles[xx * NZ + zz]
        return carry

    @pl.when(side)
    def _():
        lax.fori_loop(0, NZ, ctx_send, 0)

        @pl.when(half == 0)
        def _():
            for i in range(NX - 1):
                columns = own_columns(xwrap(x + i + 1))
                send(wd_h.at[:, columns], wdn_v.at[:, columns], s_wd.at[0], r_core.at[0], idx(x, z, 1))
            send(wd_h.at[:, own_columns(x)], wd_v.at[wd_rows(x, half), :], s_wd.at[1], r_wd.at[0], idx(x, z, 1))

    @pl.when(main)
    def _():
        for h in range(2):
            for i in range(NX - 1):
                xx = i + jnp.where(x <= i, 1, 0)
                view = wo_v.at[wo_rows(xx, half), wo_half(0, h)]
                arrived(view, r_wox.at[xx, h])
                send(view, view, s_wo, r_woy, twin)

        def wd_send(source):
            for i in range(NX - 1):
                xx = xwrap(x + i + 1)
                send(source.at[:, own_columns(xx)], wd_v.at[wd_rows(x, half), :], s_wd.at[0], r_wd.at[1], idx(xx, z, 1))

        @pl.when(half == 0)
        def _():
            arrived(wdn_v.at[:, pl.ds(0, (NX - 1) * DX)], r_core.at[0])
            wd_send(wdn_v)

        @pl.when(half == 1)
        def _():
            wd_copy.start()
            wd_send(wd_h)
        send(wg_h, wgu_v.at[:, gate_at], s_core.at[1], r_core.at[2], idx(x, z, 0))
        send(wu_h, wgu_v.at[:, up_at], s_core.at[2], r_core.at[3], idx(x, z, 0))

    @pl.when(side)
    def _():
        gate_copy.start()
        up_copy.start()

    for load in small[2:]:
        load.wait()

    rows8, lanes8 = iota((8, 128), 0), iota((8, 128), 1)
    table = jnp.where(lanes8 == LANE_TOK, (rows8 + 1).astype(F32), 0.0)
    for t in range(TOK):
        for k in range(TOP):
            hit = (rows8 == t) & (lanes8 == ids_ref[t // 2, t % 2, k] + LANE_TAB)
            table = jnp.where(hit, (slots_ref[t // 2, t % 2, k] + 1).astype(F32), table)
    resf_v[...] = jnp.zeros_like(resf_v)
    for t in range(TOK):
        row = resid_ref[t // 2, pl.ds(t % 2, 1), :].astype(F32)
        for xx in range(NX):
            for j in range(JX):
                col = xx * DX + j * 128
                resf_v[pl.ds(xx * MSG + t * JX + j, 1), :] = row[:, col:col + 128]
    for xx in range(NX):
        resf_v[pl.ds(xx * MSG + TOK * JX, 8), :] = table
    ress_v[...] = resf_v[...].reshape(NX, MSG, 128).astype(BF16)

    def to_home():
        for i in range(NX):
            xx = xwrap(x + i)
            send(ress_v.at[xx], res_v.at[dev], s_res, r_res, idx(xx, wrap(z + HALF), 1))

    def up_down(k):
        return wrap(z - k), wrap(z + k)

    early = jnp.where(lax.rem(z, CUBE) < CUBE // 2, 1, 0)
    last = wrap(z + HALF)

    def along(way):
        return idx(x, wrap(z + 1 - 2 * way), c)

    def ways(pieces):
        for i in range(pieces + 1):
            if i < pieces:
                yield i, early
            if i > 0:
                yield i - 1, 1 - early

    def slot_r(s):
        return lax.rem(s, 3)

    def slot_l(s):
        return 3 + lax.rem(s, 3)

    def slot_g(k):
        return lax.rem(k + 2, 3)

    def chain_send(in_ref, out_buf, ssem, slot, way, s, i, total):
        at = pl.ds(*SUBS[i])
        out_buf[way, s, :, at] = total.astype(BF16)
        send(out_buf.at[way, s, :, at], in_ref.at[way, s + 1, :, at], ssem.at[way], r_ring.at[way, slot(s + 1), i],
             along(way))

    def chain_piece(in_ref, out_buf, ssem, slot, s, i, way):
        at = pl.ds(*SUBS[i])
        r = wrap(z - (1 - 2 * way) * s)

        @pl.when((way == 0) | (s >= 2))
        def _():
            arrived(in_ref.at[way, s, :, at], r_ring.at[way, slot(s), i])
        chain_send(in_ref, out_buf, ssem, slot, way, s, i, part_v[r, :, at] + in_ref[way, s, :, at].astype(F32))

    def chain_step(in_ref, out_buf, ssem, slot, s):
        for i, way in ways(NS):
            chain_piece(in_ref, out_buf, ssem, slot, s, i, way)

    def chain_end(in_ref, slot, i):
        at = pl.ds(*SUBS[i])
        for way in range(2):
            arrived(in_ref.at[way, HALF, :, at], r_ring.at[way, slot(HALF), i])
        return part_v[last, :, at] + in_ref[0, HALF, :, at].astype(F32) + in_ref[1, HALF, :, at].astype(F32)

    @pl.when(side)
    def _side():
        vu_copy.wait()
        arrived(vu_v.at[pl.ds(0, VH // NC), :], r_core.at[0])
        own_lanes = pl.ds(mo(x * VH, VH), VH)

        def ctx_row(r):
            @pl.when(r == z)
            def _():
                arrived(arr_v.at[r, pl.ds(0, DEV - NC)], r_row.at[r])

            @pl.when(r != z)
            def _():
                arrived(arr_v.at[r], r_row.at[r])

            arrf_v[...] = arr_v[r].reshape(DEV * 16, 128).astype(F32)
            cols = []
            for j in range(LAT // 128):
                cols.append(jnp.concatenate(
                    [arrf_v[pl.ds(j * TOK + t, DEV, stride=16), :] for t in range(TOK)], axis=0))
            rows = jnp.concatenate(cols, axis=1).astype(BF16)
            val_v[r, :, own_lanes] = nt(rows, vu_v[...]).astype(BF16)
            view = val_v.at[r, :, own_lanes]
            for i in range(NX):
                send(view, view, s_val, r_row.at[r], idx(xwrap(x + i + 1), z, 1))

        def ctx_step(o, carry):
            ctx_row(near(o))

            return carry
        lax.fori_loop(0, NZ, ctx_step, 0)
        to_home()

        gate_copy.wait()
        up_copy.wait()
        arrived(wgu_v.at[:, pl.ds(0, UNITS)], r_core.at[2])
        arrived(wgu_v.at[:, pl.ds(0, UNITS)], r_core.at[3])

        own_expert = x * QUAD + quad
        act_at = pl.ds(mo(x * NC * UNITS, 128), NC * UNITS)

        def experts(rows):
            for r in rows:
                arrived(d_v.at[r], r_row.at[r])
            both = jnp.zeros((SLOT * len(rows), 2 * NC * UNITS), F32)
            ext = jnp.zeros((SLOT * len(rows), EXT), F32)
            shared = jnp.concatenate([d_v[r, NX] for r in rows], axis=0)
            for xx in range(NX):
                both = both + nn(
                    jnp.concatenate([d_v[r, xx, :, pl.ds(0, DA)] for r in rows], axis=0),
                    wgu_v[xx * DX:xx * DX + DA, :])
                both = both + nn(shared[:, xx * BX:(xx + 1) * BX], wgu_v[xx * DX + DA:(xx + 1) * DX, :])
                piece = jnp.concatenate([d_v[r, xx, :, pl.ds(DA, EXT)] for r in rows], axis=0)
                ext = ext + piece.astype(F32)
            n = len(rows)
            token = nt(jnp.where(iota((n * ROW, 128), 1) == LANE_TOK, 1.0, 0.0).astype(BF16), piece)
            piece = piece.astype(F32)
            jj, tok = iota(token.shape, 1), iota(token.shape, 0)
            wanted = (lax.rem(tok, ROW) // DEV + 1).astype(F32)
            hit = (token == wanted) & (lax.rem(jj, DEV) == lax.rem(tok, DEV)) & (jj // SLOT == tok // ROW)
            place = jnp.where(hit, 1.0, 0.0).astype(BF16)
            lane = iota(ext.shape, 1)
            squares = jnp.sum(
                jnp.where((lane == LANE_SUM) | (lane == LANE_SUM + 1), ext, 0.0), axis=1, keepdims=True)
            inv = lax.rsqrt(squares / D + norm_eps)
            logits = (ext + pltpu.roll(ext, EXT - EXPERTS, 1)) * inv
            named = (pltpu.roll(piece, EXT - LANE_TAB, 1) > 0.0) & (lane < EXPERTS)
            gates = jnp.where(named, 1.0 / (1.0 + jnp.exp(-logits)), 0.0)
            norm = jnp.sum(gates, axis=1, keepdims=True)
            mine = jnp.sum(jnp.where(lane == own_expert, gates, 0.0), axis=1, keepdims=True)
            share = jnp.where(norm > 0.0, route_scale * mine / norm, 0.0)
            gate = both[:, :NC * UNITS] * inv
            upward = both[:, NC * UNITS:] * inv
            act = (gate / (1.0 + jnp.exp(-gate)) * upward * share).astype(BF16)
            spread = nn(place, act).astype(BF16)
            for i, r in enumerate(rows):
                act_s[r] = spread[i * ROW:(i + 1) * ROW]
                for m in range(NX):
                    send(act_s.at[r], act_v.at[r, :, act_at], s_act, r_row.at[r], idx(xwrap(x + m + 1), z, 1))

        experts([z])

        def step(k, carry):
            experts(list(up_down(k)))
            return carry
        lax.fori_loop(1, HALF, step, 0)
        experts([last])

        arrived(ctx_v.at[pl.ds(0, NX * NZ - 1)], s_ctx.at[0])
        arrived(ctx_v.at[pl.ds(0, NX * NZ - 1)], s_ctx.at[1])
        @pl.when(half == 0)
        def _():
            arrived(won_v.at[:, pl.ds(0, (NX - 1) * DX)], s_core.at[0])
        arrived(wo_v.at[pl.ds(0, VH // NC), :], s_wo)
        arrived(res_v.at[pl.ds(0, NX)], s_res)

        @pl.when(half == 0)
        def _():
            arrived(wdn_v.at[:, pl.ds(0, (NX - 1) * DX)], s_wd.at[0])
            arrived(wdn_v.at[:, pl.ds(0, DX)], s_wd.at[1])
        arrived(val_v, s_val)
        arrived(act_v, s_act)
        arrived(sum_v, r_out)

    @pl.when(main)
    def _main():
        gain_v[...] = gain_ref[...].astype(F32)
        rs_in[1, 1] = jnp.zeros((ROW, DX), BF16)
        rs2_in[1, 1] = jnp.zeros((ROW, DX), BF16)

        def twin_send(xx):
            view = wd_v.at[wd_rows(xx, half), :]
            send(view, view, s_wd.at[1], r_twin, twin)

        @pl.when(half == 0)
        def _():
            arrived(wd_v.at[wd_rows(x, half), :], r_wd.at[0])

        @pl.when(half == 1)
        def _():
            wd_copy.wait()
        twin_send(x)

        wo_copy.wait()
        arrived(wo_v.at[wo_rows(x, 0), :], r_wo)
        arrived(wo_v.at[pl.ds(0, (NX - 1) * (VH // NC)), :], r_woy)
        to_home()

        def attended(rows):
            for r in rows:
                arrived(val_v.at[r], r_row.at[r])
            stacked = jnp.concatenate([val_v[r] for r in rows], axis=0)
            for o, w in BLOCKS:
                part = nn(stacked, wo_v[:, o:o + w])
                for i, r in enumerate(rows):
                    part_v[r, :, pl.ds(o, w)] = part[i * ROW:(i + 1) * ROW]

        arrived(val_v.at[z], r_row.at[z])
        for i, (o, w) in enumerate(SUBS):
            chain_send(rs_in, rs_out, s_rs, slot_r, 0, 0, i, nn(val_v[z], wo_v[:, o:o + w]))
        attended(list(up_down(1)))

        def rs_step(s, carry):
            chain_step(rs_in, rs_out, s_rs, slot_r, s)

            @pl.when(s < HALF - 1)
            def _():
                attended(list(up_down(s + 1)))

            @pl.when(s == HALF // 2)
            def _():
                arrived(wd_v.at[pl.ds(0, (NX - 1) * UNITS), :], r_wd.at[1])
                for i in range(NX - 1):
                    twin_send(xwrap(x + i + 1))
            return carry
        lax.fori_loop(1, HALF, rs_step, 0)
        attended([last])

        arrived(res_v, r_res)
        resw_v[...] = res_v[...].reshape(DEV * MSG, 128).astype(F32)
        lane = iota((ROW, 128), 1)
        tabs = [resw_v[pl.ds(TOK * JX + t, DEV, stride=MSG), :] for t in range(TOK)]
        table_rows = jnp.concatenate(tabs, axis=0)
        router_copy.wait()

        def ag_send(r, i, way, k):
            view = ag_v.at[r, :, pl.ds(i * PIECE, PIECE)]
            send(view, view, s_ag.at[way], r_ring.at[way, slot_g(k), i], along(way))

        def ag_wait(r, i, way, k):
            arrived(ag_v.at[r, :, pl.ds(i * PIECE, PIECE)], r_ring.at[way, slot_g(k), i])

        bx_at = pl.ds(mo(DAE + x * BX, 128), BX)
        sums = jnp.zeros((ROW, 1), F32)
        logits = jnp.zeros((ROW, 128), F32)
        for i, (o, w) in enumerate(SUBS):
            attn = chain_end(rs_in, slot_r, i)
            att_v[:, pl.ds(o, w)] = attn
            hidden = attn + jnp.concatenate([
                jnp.concatenate([resw_v[pl.ds(t * JX + j, DEV, stride=MSG), :] for t in range(TOK)], axis=0)
                for j in range(o // 128, (o + w) // 128)], axis=1)
            gain = jnp.concatenate(
                [gain_v[pl.ds(x * JX + j, 1), :] for j in range(o // 128, (o + w) // 128)], axis=1)
            scaled = (hidden * gain).astype(BF16)
            if i == 0:
                ag_v[z, :, bx_at] = scaled
                view = ag_v.at[z, :, bx_at]
                for j in (1, 0, 2):
                    send(view, view, s_bx, r_bx, idx(xwrap(x + j + 1), z, 1))
            else:
                ag_v[z, :, pl.ds(o, w)] = scaled
                if o + w >= PIECE > o:
                    ag_send(z, 0, 0, 1)
                    ag_send(z, 0, 1, 1)
            sums = sums + jnp.sum(hidden * hidden, axis=1, keepdims=True)
            logits = logits + nt(scaled, rout_v[:, pl.ds(o, w)])
        high = logits.astype(BF16).astype(F32)
        sums_high = sums.astype(BF16).astype(F32)
        ext = high + pltpu.roll(logits - high, EXPERTS, 1)
        ext = jnp.where(lane == LANE_SUM, sums_high, ext)
        ext = jnp.where(lane == LANE_SUM + 1, sums - sums_high, ext)
        ag_v[z, :, pl.ds(DA, EXT)] = (ext + table_rows).astype(BF16)
        ag_send(z, NPA - 1, 0, 1)
        ag_send(z, NPA - 1, 1, 1)
        arrived(ag_v.at[z, :, pl.ds(DAE, (NX - 1) * BX)], r_bx)
        for i in range(NPA, NP):
            ag_send(z, i, 0, 1)
            ag_send(z, i, 1, 1)

        def dispatch(rows):
            n = len(rows)
            size = n * NX * SLOT
            jj, lane = iota((size, 128), 0), iota((size, 128), 1)
            wanted_lane = LANE_TAB + lax.rem(x + lax.rem(jj // SLOT, NX), NX) * QUAD + quad
            pick = jnp.where(lane == wanted_lane, 1.0, 0.0).astype(BF16)
            picked = nt(pick, jnp.concatenate([ag_v[r, :, pl.ds(DA, EXT)] for r in rows], axis=0))
            jj, tok = iota((size, n * ROW), 0), iota((size, n * ROW), 1)
            wanted = (lax.rem(jj, SLOT) // DEV + 1).astype(F32)
            hit = (picked == wanted) & (lax.rem(jj, DEV) == lax.rem(tok, DEV)) & (jj // (NX * SLOT) == tok // ROW)
            place = jnp.where(hit, 1.0, 0.0).astype(BF16)
            moved = nn(place, jnp.concatenate([ag_v[r, :, pl.ds(0, DAE)] for r in rows], axis=0)).astype(BF16)
            own = jnp.concatenate([place[i * NX * SLOT:i * NX * SLOT + SLOT] for i in range(n)], axis=0)
            shared = nn(own, jnp.concatenate([ag_v[r, :, pl.ds(DAE, NX * BX)] for r in rows], axis=0)).astype(BF16)
            for i, r in enumerate(rows):
                dsp_v[r, pl.ds(0, NX)] = moved[i * NX * SLOT:(i + 1) * NX * SLOT].reshape(NX, SLOT, DAE)
                dsp_v[r, NX] = shared[i * SLOT:(i + 1) * SLOT]
            for r in rows:
                for i in (2, 1, 3, 0):
                    send(dsp_v.at[r, i], d_v.at[r, x], s_dsp, r_row.at[r], idx(xwrap(x + i), z, 0))
                send(dsp_v.at[r, NX], d_v.at[r, NX], s_dsp, r_row.at[r], idx(x, z, 0))

        def returned(rows):
            for r in rows:
                arrived(act_v.at[r], r_row.at[r])
            return jnp.concatenate([act_v[r] for r in rows], axis=0)

        def down_blocks(rows, blocks):
            for o, w in blocks:
                at = pl.ds(o, w)
                part = nn(jnp.concatenate([act_v[r] for r in rows], axis=0), wd_v[:, o:o + w])
                for i, r in enumerate(rows):
                    part_v[r, :, at] = part[i * ROW:(i + 1) * ROW]

        def down_part(rows):
            returned(rows)
            down_blocks(rows, BLOCKS)

        def down_first():
            spread = returned([z])
            for o, w in BLOCKS:
                at = pl.ds(o, w)
                part_v[z, :, at] = nn(spread, wd_v[:, o:o + w]) + att_v[:, at]
        dispatch([z])

        def ag_step(k, carry):
            behind = list(up_down(k - 1))
            done = list(up_down(k - DOWN - 1))

            def pieces(i):
                for way in (early, 1 - early):
                    r = wrap(z - (1 - 2 * way) * k)
                    ag_wait(r, i, way, k)

                    @pl.when((way == 0) | (k < HALF - 1))
                    def _():
                        ag_send(r, i, way, k + 1)
            def follow(i):
                @pl.when(k > DOWN + 1)
                def _():
                    for way in (early, 1 - early):
                        chain_piece(rs2_in, rs2_out, s_rs2, slot_l, k - DOWN - 1, i, way)
            pieces(0)

            @pl.when(k >= 2)
            def _():
                dispatch(behind)
            pieces(1)

            @pl.when(k == DOWN)
            def _():
                arrived(wd_v.at[pl.ds(0, NX * UNITS), :], r_twin)
                down_first()

            @pl.when(k == DOWN + 1)
            def _():
                for i, (o, w) in enumerate(SUBS):
                    chain_send(rs2_in, rs2_out, s_rs2, slot_l, 0, 0, i, part_v[z, :, pl.ds(o, w)])

            @pl.when(k > DOWN + 1)
            def _():
                returned(done)
                down_blocks(done, BLOCKS[:1])
            pieces(2)

            @pl.when(k > DOWN + 1)
            def _():
                down_blocks(done, BLOCKS[1:])
            pieces(3)
            for i in range(NS):
                follow(i)
            return carry
        lax.fori_loop(1, HALF, ag_step, 0)
        dispatch(list(up_down(HALF - 1)))
        for i in range(NP):
            ag_wait(last, i, 0, HALF)
        dispatch([last])

        down_part(list(up_down(HALF - DOWN - 1)))

        def late(k, carry):
            chain_step(rs2_in, rs2_out, s_rs2, slot_l, k - 1)
            down_part(list(up_down(k)))
            return carry
        lax.fori_loop(HALF - DOWN, HALF, late, 0)
        chain_step(rs2_in, rs2_out, s_rs2, slot_l, HALF - 1)
        down_part([last])

        for t in range(TOK * JX, MSG):
            fin_v[pl.ds(t, DEV, stride=MSG), :] = jnp.zeros((DEV, 128), F32)
        for i, (o, w) in enumerate(SUBS):
            mixed = chain_end(rs2_in, slot_l, i)
            for t in range(TOK):
                for j in range(o // 128, (o + w) // 128):
                    fin_v[pl.ds(t * JX + j, DEV, stride=MSG), :] = (
                        mixed[t * DEV:(t + 1) * DEV, j * 128 - o:j * 128 - o + 128])
        fin_s[...] = fin_v[...].reshape(DEV, MSG, 128).astype(BF16)
        for i in range(DEV - 1):
            to = lax.rem(dev + i + 1, DEV)
            send(fin_s.at[to], sum_v.at[x], s_out, r_out, idx(to // NC, z, lax.rem(to, NC)))
        sum_v[x] = fin_s[dev]

        arrived(ctx_v, s_ctx.at[0])
        arrived(wo_v.at[pl.ds(0, 2 * (NX - 1) * (VH // NC)), :], s_wo)
        arrived(res_v.at[pl.ds(0, NX)], s_res)
        arrived(vu_v.at[pl.ds(0, VH // NC), :], s_core.at[0])
        arrived(wgu_v.at[:, pl.ds(0, UNITS)], s_core.at[1])
        arrived(wgu_v.at[:, pl.ds(0, UNITS)], s_core.at[2])
        arrived(wd_v.at[pl.ds(0, (NX - 1) * UNITS), :], s_wd.at[0])
        arrived(wd_v.at[pl.ds(0, NX * UNITS), :], s_wd.at[1])
        for way in range(2):
            arrived(rs_out.at[way, pl.ds(way, HALF - way)], s_rs.at[way])
            arrived(rs2_out.at[way, pl.ds(way, HALF - way)], s_rs2.at[way])
            arrived(ag_v.at[pl.ds(0, HALF - way)], s_ag.at[way])
        arrived(ag_v.at[z, :, pl.ds(DAE, (NX - 1) * BX)], s_bx)
        arrived(dsp_v, s_dsp)
        arrived(fin_s.at[pl.ds(0, DEV - 1)], s_out)
        arrived(sum_v.at[pl.ds(0, NX - 1)], r_out)

    resf_v[...] = sum_v[...].reshape(NX * MSG, 128).astype(F32) + resf_v[...]
    for t in range(TOK):
        rows = [resf_v[pl.ds(xx * MSG + t * JX, JX), :] for xx in range(NX)]
        outv_v[t] = jnp.concatenate(rows, axis=0).astype(BF16)
    out_copy = pltpu.make_async_copy(outv_v, out_ref, l_misc)
    out_copy.start()
    out_copy.wait()


def body(
    cache_kv, new_kv, queries, lengths, resid, value_up, out_proj, norm_gain, router, expert_ids, slots, w_gate, w_up,
    w_down,
):
    seqs, steps = resid.shape[:2]
    cache_len = cache_kv.shape[1]
    hbm = pl.BlockSpec(memory_space=pltpu.HBM)
    dma = pltpu.SemaphoreType.DMA
    regular = pltpu.SemaphoreType.REGULAR
    scratch = [
        pltpu.VMEM(new_kv.shape, BF16),
        pltpu.SMEM(lengths.shape, jnp.int32),
        pltpu.VMEM(resid.shape, BF16),
        pltpu.VMEM((D // 128, 128), BF16),
        pltpu.SMEM(expert_ids.shape, jnp.int32),
        pltpu.SMEM(slots.shape, jnp.int32),
        pltpu.VMEM((seqs, KV, cache_len), BF16),
        pltpu.VMEM((seqs, steps * H, KV), BF16),
        pltpu.VMEM((steps * H, cache_len), F32),
        pltpu.VMEM((H * 16, 128), F32),
        pltpu.VMEM((H, 16, 128), BF16),
        pltpu.VMEM((NZ, DEV, 16, 128), BF16),
        pltpu.VMEM((DEV * 16, 128), F32),
        pltpu.VMEM((VH, LAT), BF16),
        pltpu.VMEM((NZ, ROW, NX * VH), BF16),
        pltpu.VMEM((NX * VH, DX), BF16),
        pltpu.VMEM((H, 16, 128), BF16),
        pltpu.VMEM((VH // NC, D), BF16),
        pltpu.VMEM((2, HALF + 1, ROW, DX), BF16),
        pltpu.VMEM((2, HALF, ROW, DX), BF16),
        pltpu.VMEM((ROW, DX), F32),
        pltpu.VMEM((NX, MSG, 128), BF16),
        pltpu.VMEM((NX * MSG, 128), F32),
        pltpu.VMEM((DEV, MSG, 128), BF16),
        pltpu.VMEM((DEV * MSG, 128), F32),
        pltpu.VMEM((D // 128, 128), F32),
        pltpu.VMEM((128, DX), BF16),
        pltpu.VMEM((NZ, ROW, DG), BF16),
        pltpu.VMEM((NZ, NX + 1, SLOT, DAE), BF16),
        pltpu.VMEM((NZ, NX + 1, SLOT, DAE), BF16),
        pltpu.VMEM((D, 2 * NC * UNITS), BF16),
        pltpu.VMEM((NZ, ROW, NC * UNITS), BF16),
        pltpu.VMEM((NZ, ROW, NX * NC * UNITS), BF16),
        pltpu.VMEM((NX * NC * UNITS, DX), BF16),
        pltpu.VMEM((UNITS, D), BF16),
        pltpu.VMEM((2, HALF + 1, ROW, DX), BF16),
        pltpu.VMEM((2, HALF, ROW, DX), BF16),
        pltpu.VMEM((NZ, ROW, DX), F32),
        pltpu.VMEM((DEV * MSG, 128), F32),
        pltpu.VMEM((DEV, MSG, 128), BF16),
        pltpu.VMEM((NX, MSG, 128), BF16),
        pltpu.VMEM((TOK, NX * JX, 128), BF16),
        dma((seqs,)), dma, dma((3,)), dma((6,)),
        dma((2,)), dma, dma, dma((3,)), dma((2,)), dma, dma((2,)), dma((2,)), dma((2,)), dma, dma, dma, dma,
        dma, dma, dma((NX, 2)), dma, dma((4,)), dma((2,)), dma((NZ,)), dma((2, 6, NP)), dma, dma, dma,
        regular, regular,
    ]
    out = pl.pallas_call(
        kernel,
        out_shape=jax.ShapeDtypeStruct((TOK, NX * JX, 128), BF16),
        in_specs=[hbm] * 14,
        out_specs=hbm,
        scratch_shapes=scratch,
        compiler_params=pltpu.CompilerParams(
            collective_id=0, has_side_effects=True, vmem_limit_bytes=(64 << 20) - (64 << 10)),
        name="layer",
    )(
        jnp.transpose(cache_kv, (0, 2, 1)), new_kv, queries.reshape(seqs, steps * H, KV), lengths, resid,
        value_up.T, out_proj, norm_gain.reshape(D // 128, 128), router.T, expert_ids, slots, w_gate, w_up, w_down,
    )
    return out.reshape(resid.shape)


def solution(mesh):
    return jax.shard_map(
        body,
        mesh=mesh,
        in_specs=(
            P(("rep", "ep"), None, None),
            P(("rep", "ep"), None, None),
            P(("rep", "ep"), None, None, None),
            P(("rep", "ep")),
            P(("rep", "ep"), None, None),
            P(None, "ep"),
            P("ep", None),
            P(),
            P(),
            P(("rep", "ep"), None, None),
            P(("rep", "ep"), None, None),
            P(None, "ep"),
            P(None, "ep"),
            P("ep", None),
        ),
        out_specs=P(("rep", "ep"), None, None),
        check_vma=False,
    )
```

```python
import functools
import math

import jax
import jax.numpy as jnp
from jax import lax
from jax.experimental import pallas as pl
from jax.experimental.pallas import tpu as pltpu
from jax.sharding import PartitionSpec as P

NX, NZ, NC = 4, 16, 2
DEV = NX * NC
HALF = NZ // 2

D = 7168
H = 64
LAT = 512
VH = 128
KV = 576
EXPERTS = 16
TOP = 8
CAP = 2
QK = 192
TOK = 4
UNITS = 128
ROW = DEV * TOK
SLOT = DEV * CAP
DX = D // NX
EXT = 128
JX = DX // 128
MSG = 64
LANE_SUM = 32
LANE_TOK = 48
LANE_TAB = 64
QUAD = EXPERTS // NX
CHIPS_PER = NZ // QUAD

route_scale = 2.827
norm_eps = 1e-06

CUBE = 4

BX = 384
DA = DX - BX
DAE = DA + EXT
DG = DAE + NX * BX
PIECE = 768
SUBS = ((DA, BX), (0, 256), (256, 256), (512, 256), (768, 256), (1024, 384))
NS = len(SUBS)
NP = DG // PIECE
NPA = DAE // PIECE
BLOCKS = ((0, 512), (512, 512), (1024, 768))
DOWN = 4

F32 = jnp.float32
BF16 = jnp.bfloat16


def mo(value, by):
    return pl.multiple_of(value, by)


def nt(a, b):
    return lax.dot_general(a, b, (((1,), (1,)), ((), ())), preferred_element_type=F32)


def nn(a, b):
    return lax.dot_general(a, b, (((1,), (0,)), ((), ())), preferred_element_type=F32)


def iota(shape, axis):
    return lax.broadcasted_iota(jnp.int32, shape, axis)


def kernel(
    cache_h, new_h, q_h, len_h, resid_h, vu_h, wo_h, gain_h, router_h, ids_h, slots_h, wg_h, wu_h, wd_h,
    out_ref,
    new_ref, len_ref, resid_ref, gain_ref, ids_ref, slots_ref,
    cache_v, q_v, score_v, stage_v, ctx_v, arr_v, arrf_v, vu_v, val_v, wo_v, ctxn_v, won_v, rs_in, rs_out, att_v,
    ress_v, resf_v, res_v, resw_v, gain_v, rout_v, ag_v, dsp_v, d_v, wgu_v, act_s, act_v, wd_v, wdn_v, rs2_in, rs2_out,
    part_v, fin_v, fin_s, sum_v, outv_v,
    l_cache, l_misc, l_weights, l_small,
    s_ctx, s_res, s_wo, s_core, s_wd, s_val, s_rs, s_ag, s_rs2, s_dsp, s_act, s_out, s_bx,
    r_res, r_wo, r_wox, r_woy, r_core, r_wd, r_row, r_ring, r_out, r_bx, r_twin,
    row_sem, all_sem,
):
    me = lax.axis_index("ep")
    c = lax.rem(me, NC)
    z = lax.rem(me // NC, NZ)
    x = me // (NC * NZ)
    dev = x * NC + c
    quad = z // CHIPS_PER
    group = lax.axis_index("rep")
    half = lax.rem(group, 2)
    twin = {"rep": group + 1 - 2 * half, "ep": me}

    def idx(xx, zz, cc):
        return {"ep": (xx * NZ + zz) * NC + cc}

    def wrap(zz):
        return lax.rem(zz + 2 * NZ, NZ)

    def xwrap(xx):
        return lax.rem(xx, NX)

    def send(src, dst, ssem, rsem, to):
        pltpu.make_async_remote_copy(src_ref=src, dst_ref=dst, send_sem=ssem, recv_sem=rsem, device_id=to).start()

    def arrived(ref, sem):
        pltpu.make_async_copy(ref, ref, sem).wait()

    main = c == 1
    side = c == 0

    loads = [pltpu.make_async_copy(q_h, q_v, l_misc)]
    loads += [pltpu.make_async_copy(cache_h.at[b], cache_v.at[b], l_cache.at[b]) for b in range(2)]
    small = [
        pltpu.make_async_copy(src, dst, l_small.at[i]) for i, (src, dst) in enumerate((
            (new_h, new_ref), (len_h, len_ref), (resid_h, resid_ref), (gain_h, gain_ref), (ids_h, ids_ref),
            (slots_h, slots_ref)))
    ]
    for load in loads[:2] + small[:2] + loads[2:] + small[2:]:
        load.start()

    bar = pltpu.get_barrier_semaphore()

    @pl.when(side)
    def _():
        def greet(o, carry):
            far = HALF - (o + 1) // 2
            zz = wrap(jnp.where(lax.rem(o, 2) == 1, z + far, z - far))
            for xx in range(NX):
                pl.semaphore_signal(bar, inc=1, device_id=idx(xx, zz, 1))
            return carry
        lax.fori_loop(0, NZ, greet, 0)

    @pl.when(main)
    def _():
        for xx in range(NX):
            pl.semaphore_signal(bar, inc=1, device_id=idx(xx, z, 0))
            pl.semaphore_signal(bar, inc=1, device_id=idx(xx, wrap(z + HALF), 1))
        for step in (1, -1):
            pl.semaphore_signal(bar, inc=1, device_id=idx(x, wrap(z + step), 1))
        pl.semaphore_signal(bar, inc=1, device_id=twin)

    gate_at = pl.ds(mo(c * UNITS, UNITS), UNITS)
    up_at = pl.ds(mo((NC + c) * UNITS, UNITS), UNITS)
    vu_at = pl.ds(mo(c * (VH // NC), VH // NC), VH // NC)
    router_copy = pltpu.make_async_copy(
        router_h.at[:, pl.ds(mo(x * DX, 128), DX)], rout_v.at[pl.ds(0, EXPERTS), :], l_weights.at[1])
    gate_copy = pltpu.make_async_copy(wg_h, wgu_v.at[:, gate_at], l_weights.at[1])
    up_copy = pltpu.make_async_copy(wu_h, wgu_v.at[:, up_at], l_weights.at[2])
    vu_copy = pltpu.make_async_copy(vu_h, vu_v.at[vu_at, :], l_weights.at[0])

    def wo_rows(xx, cc):
        return pl.ds(mo(xx * VH + cc * (VH // NC), VH // NC), VH // NC)

    def own_columns(xx):
        return pl.ds(mo(xx * DX, 128), DX)

    def wd_rows(xx, cc):
        return pl.ds(mo((xx * NC + cc) * UNITS, UNITS), UNITS)

    wo_copy = pltpu.make_async_copy(wo_h.at[:, own_columns(x)], wo_v.at[wo_rows(x, 1), :], l_weights.at[0])
    wd_copy = pltpu.make_async_copy(wd_h.at[:, own_columns(x)], wd_v.at[wd_rows(x, half), :], l_weights.at[2])

    def wo_half(xx, h):
        return pl.ds(mo(xx * DX + h * (DX // 2), 128), DX // 2)

    def wo_send(source):
        for h in range(2):
            for i in range(NX - 1):
                xx = xwrap(x + i + 1)
                send(source.at[:, wo_half(xx, h)], wo_v.at[wo_rows(x, half), wo_half(0, h)], s_wo, r_wox.at[x, h],
                     idx(xx, z, 1))

    def row_next():
        @pl.when(main & (half == 0))
        def _():
            arrived(won_v.at[:, pl.ds(0, (NX - 1) * DX)], r_core.at[2])
            wo_send(won_v)

    def row_start():
        @pl.when(side)
        def _():
            pl.semaphore_wait(bar, NX)
            pl.semaphore_signal(row_sem, inc=1, device_id=idx(x, z, 1))

        @pl.when(main)
        def _():
            pl.semaphore_wait(row_sem, 1)

        @pl.when(main)
        def _():
            @pl.when(half == 1)
            def _():
                wo_send(wo_h)
            wo_copy.start()
            send(vu_h, vu_v.at[vu_at, :], s_core.at[0], r_core.at[0], idx(x, z, 0))
            rout_v[...] = jnp.zeros_like(rout_v)
            router_copy.start()

        @pl.when(side)
        def _():
            vu_copy.start()
            @pl.when(half == 0)
            def _():
                for i in range(NX - 1):
                    columns = own_columns(xwrap(x + i + 1))
                    send(wo_h.at[:, columns], won_v.at[:, columns], s_core.at[0], r_core.at[2], idx(x, z, 1))
            send(wo_h.at[:, own_columns(x)], wo_v.at[wo_rows(x, 0), :], s_wo, r_wo, idx(x, z, 1))

    scale = 1.0 / math.sqrt(QK)
    blk = 512
    nblk = cache_v.shape[2] // blk
    loads[0].wait()
    small[0].wait()
    small[1].wait()
    for b in range(2):
        qb = q_v[b]
        qf = qb.astype(F32)
        step_of = iota((2 * H, 1), 0) // H
        new_rows = [new_ref[b, pl.ds(t, 1), :].astype(F32) for t in range(2)]
        s_new = [jnp.sum(qf * row, axis=1, keepdims=True) * scale for row in new_rows]
        s_new[1] = jnp.where(step_of >= 1, s_new[1], -jnp.inf)
        peak = jnp.maximum(s_new[0], s_new[1])
        loads[1 + b].wait()
        for p in range(nblk):
            sc = nn(qb, cache_v[b, :, pl.ds(p * blk, blk)]) * scale
            pos = iota((2 * H, blk), 1) + p * blk
            sc = jnp.where(pos < len_ref[b], sc, -jnp.inf)
            score_v[:, pl.ds(p * blk, blk)] = sc
            peak = jnp.maximum(peak, jnp.max(sc, axis=1, keepdims=True))
        if b == 0:
            row_start()
        else:
            row_next()
        p_new = [jnp.exp(s - peak) for s in s_new]
        total = p_new[0] + p_new[1]
        acc = p_new[0].astype(BF16).astype(F32) * new_rows[0][:, :LAT]
        acc = acc + p_new[1].astype(BF16).astype(F32) * new_rows[1][:, :LAT]
        for p in range(nblk):
            pr = jnp.exp(score_v[:, pl.ds(p * blk, blk)] - peak)
            total = total + jnp.sum(pr, axis=1, keepdims=True)
            acc = acc + nt(pr.astype(BF16), cache_v[b, pl.ds(0, LAT), pl.ds(p * blk, blk)])
        ctx = acc / total
        for s in range(2):
            for j in range(LAT // 128):
                stage_v[pl.ds(j * TOK + b * 2 + s, H, stride=16), :] = ctx[s * H:(s + 1) * H, j * 128:(j + 1) * 128]
    ctx_v[...] = stage_v[...].reshape(H, 16, 128).astype(BF16)

    @pl.when(main)
    def _():
        send(ctx_v, ctxn_v, s_ctx.at[0], r_core.at[1], idx(x, z, 0))
        pl.semaphore_wait(bar, NX * NZ + NX + 3)
        pl.semaphore_signal(all_sem, inc=1, device_id=idx(x, z, 0))

    @pl.when(side)
    def _():
        arrived(ctxn_v, r_core.at[1])
        pl.semaphore_wait(all_sem, 1)

    def near(o):
        return wrap(jnp.where(lax.rem(o, 2) == 1, z - (o + 1) // 2, z + o // 2))

    def ctx_send(o, carry):
        zz = near(o)
        for i in range(NX):
            xx = xwrap(x + i + 1)
            own = (zz == z) & (xx == x)
            for core, tiles in ((0, ctx_v), (1, ctxn_v)):
                @pl.when(jnp.logical_not(own))
                def _():
                    send(tiles.at[xx * NZ + zz], arr_v.at[z, x * NC + core], s_ctx.at[core], r_row.at[z],
                         idx(xx, zz, 0))

                @pl.when(own)
                def _():
                    arr_v[z, x * NC + core] = tiles[xx * NZ + zz]
        return carry

    @pl.when(side)
    def _():
        lax.fori_loop(0, NZ, ctx_send, 0)

        @pl.when(half == 0)
        def _():
            for i in range(NX - 1):
                columns = own_columns(xwrap(x + i + 1))
                send(wd_h.at[:, columns], wdn_v.at[:, columns], s_wd.at[0], r_core.at[0], idx(x, z, 1))
            send(wd_h.at[:, own_columns(x)], wd_v.at[wd_rows(x, half), :], s_wd.at[1], r_wd.at[0], idx(x, z, 1))

    @pl.when(main)
    def _():
        for h in range(2):
            for i in range(NX - 1):
                xx = i + jnp.where(x <= i, 1, 0)
                view = wo_v.at[wo_rows(xx, half), wo_half(0, h)]
                arrived(view, r_wox.at[xx, h])
                send(view, view, s_wo, r_woy, twin)

        def wd_send(source):
            for i in range(NX - 1):
                xx = xwrap(x + i + 1)
                send(source.at[:, own_columns(xx)], wd_v.at[wd_rows(x, half), :], s_wd.at[0], r_wd.at[1], idx(xx, z, 1))

        @pl.when(half == 0)
        def _():
            arrived(wdn_v.at[:, pl.ds(0, (NX - 1) * DX)], r_core.at[0])
            wd_send(wdn_v)

        @pl.when(half == 1)
        def _():
            wd_copy.start()
            wd_send(wd_h)
        send(wg_h, wgu_v.at[:, gate_at], s_core.at[1], r_core.at[2], idx(x, z, 0))
        send(wu_h, wgu_v.at[:, up_at], s_core.at[2], r_core.at[3], idx(x, z, 0))

    @pl.when(side)
    def _():
        gate_copy.start()
        up_copy.start()

    for load in small[2:]:
        load.wait()

    rows8, lanes8 = iota((8, 128), 0), iota((8, 128), 1)
    table = jnp.where(lanes8 == LANE_TOK, (rows8 + 1).astype(F32), 0.0)
    for t in range(TOK):
        for k in range(TOP):
            hit = (rows8 == t) & (lanes8 == ids_ref[t // 2, t % 2, k] + LANE_TAB)
            table = jnp.where(hit, (slots_ref[t // 2, t % 2, k] + 1).astype(F32), table)
    resf_v[...] = jnp.zeros_like(resf_v)
    for t in range(TOK):
        row = resid_ref[t // 2, pl.ds(t % 2, 1), :].astype(F32)
        for xx in range(NX):
            for j in range(JX):
                col = xx * DX + j * 128
                resf_v[pl.ds(xx * MSG + t * JX + j, 1), :] = row[:, col:col + 128]
    for xx in range(NX):
        resf_v[pl.ds(xx * MSG + TOK * JX, 8), :] = table
    ress_v[...] = resf_v[...].reshape(NX, MSG, 128).astype(BF16)

    def to_home():
        for i in range(NX):
            xx = xwrap(x + i)
            send(ress_v.at[xx], res_v.at[dev], s_res, r_res, idx(xx, wrap(z + HALF), 1))

    def up_down(k):
        return wrap(z - k), wrap(z + k)

    early = jnp.where(lax.rem(z, CUBE) < CUBE // 2, 1, 0)
    last = wrap(z + HALF)

    def along(way):
        return idx(x, wrap(z + 1 - 2 * way), c)

    def ways(pieces):
        for i in range(pieces + 1):
            if i < pieces:
                yield i, early
            if i > 0:
                yield i - 1, 1 - early

    def slot_r(s):
        return lax.rem(s, 3)

    def slot_l(s):
        return 3 + lax.rem(s, 3)

    def slot_g(k):
        return lax.rem(k + 2, 3)

    def chain_send(in_ref, out_buf, ssem, slot, way, s, i, total):
        at = pl.ds(*SUBS[i])
        out_buf[way, s, :, at] = total.astype(BF16)
        send(out_buf.at[way, s, :, at], in_ref.at[way, s + 1, :, at], ssem.at[way], r_ring.at[way, slot(s + 1), i],
             along(way))

    def chain_piece(in_ref, out_buf, ssem, slot, s, i, way):
        at = pl.ds(*SUBS[i])
        r = wrap(z - (1 - 2 * way) * s)

        @pl.when((way == 0) | (s >= 2))
        def _():
            arrived(in_ref.at[way, s, :, at], r_ring.at[way, slot(s), i])
        chain_send(in_ref, out_buf, ssem, slot, way, s, i, part_v[r, :, at] + in_ref[way, s, :, at].astype(F32))

    def chain_step(in_ref, out_buf, ssem, slot, s):
        for i, way in ways(NS):
            chain_piece(in_ref, out_buf, ssem, slot, s, i, way)

    def chain_end(in_ref, slot, i):
        at = pl.ds(*SUBS[i])
        for way in range(2):
            arrived(in_ref.at[way, HALF, :, at], r_ring.at[way, slot(HALF), i])
        return part_v[last, :, at] + in_ref[0, HALF, :, at].astype(F32) + in_ref[1, HALF, :, at].astype(F32)

    @pl.when(side)
    def _side():
        vu_copy.wait()
        arrived(vu_v.at[pl.ds(0, VH // NC), :], r_core.at[0])
        own_lanes = pl.ds(mo(x * VH, VH), VH)

        def ctx_row(r):
            @pl.when(r == z)
            def _():
                arrived(arr_v.at[r, pl.ds(0, DEV - NC)], r_row.at[r])

            @pl.when(r != z)
            def _():
                arrived(arr_v.at[r], r_row.at[r])

            arrf_v[...] = arr_v[r].reshape(DEV * 16, 128).astype(F32)
            cols = []
            for j in range(LAT // 128):
                cols.append(jnp.concatenate(
                    [arrf_v[pl.ds(j * TOK + t, DEV, stride=16), :] for t in range(TOK)], axis=0))
            rows = jnp.concatenate(cols, axis=1).astype(BF16)
            val_v[r, :, own_lanes] = nt(rows, vu_v[...]).astype(BF16)
            view = val_v.at[r, :, own_lanes]
            for i in range(NX):
                send(view, view, s_val, r_row.at[r], idx(xwrap(x + i + 1), z, 1))

        def ctx_step(o, carry):
            ctx_row(near(o))

            return carry
        lax.fori_loop(0, NZ, ctx_step, 0)
        to_home()

        gate_copy.wait()
        up_copy.wait()
        arrived(wgu_v.at[:, pl.ds(0, UNITS)], r_core.at[2])
        arrived(wgu_v.at[:, pl.ds(0, UNITS)], r_core.at[3])

        own_expert = x * QUAD + quad
        act_at = pl.ds(mo(x * NC * UNITS, 128), NC * UNITS)

        def experts(rows):
            for r in rows:
                arrived(d_v.at[r], r_row.at[r])
            both = jnp.zeros((SLOT * len(rows), 2 * NC * UNITS), F32)
            ext = jnp.zeros((SLOT * len(rows), EXT), F32)
            shared = jnp.concatenate([d_v[r, NX] for r in rows], axis=0)
            for xx in range(NX):
                both = both + nn(
                    jnp.concatenate([d_v[r, xx, :, pl.ds(0, DA)] for r in rows], axis=0),
                    wgu_v[xx * DX:xx * DX + DA, :])
                both = both + nn(shared[:, xx * BX:(xx + 1) * BX], wgu_v[xx * DX + DA:(xx + 1) * DX, :])
                piece = jnp.concatenate([d_v[r, xx, :, pl.ds(DA, EXT)] for r in rows], axis=0)
                ext = ext + piece.astype(F32)
            n = len(rows)
            token = nt(jnp.where(iota((n * ROW, 128), 1) == LANE_TOK, 1.0, 0.0).astype(BF16), piece)
            piece = piece.astype(F32)
            jj, tok = iota(token.shape, 1), iota(token.shape, 0)
            wanted = (lax.rem(tok, ROW) // DEV + 1).astype(F32)
            hit = (token == wanted) & (lax.rem(jj, DEV) == lax.rem(tok, DEV)) & (jj // SLOT == tok // ROW)
            place = jnp.where(hit, 1.0, 0.0).astype(BF16)
            lane = iota(ext.shape, 1)
            squares = jnp.sum(
                jnp.where((lane == LANE_SUM) | (lane == LANE_SUM + 1), ext, 0.0), axis=1, keepdims=True)
            inv = lax.rsqrt(squares / D + norm_eps)
            logits = (ext + pltpu.roll(ext, EXT - EXPERTS, 1)) * inv
            named = (pltpu.roll(piece, EXT - LANE_TAB, 1) > 0.0) & (lane < EXPERTS)
            gates = jnp.where(named, 1.0 / (1.0 + jnp.exp(-logits)), 0.0)
            norm = jnp.sum(gates, axis=1, keepdims=True)
            mine = jnp.sum(jnp.where(lane == own_expert, gates, 0.0), axis=1, keepdims=True)
            share = jnp.where(norm > 0.0, route_scale * mine / norm, 0.0)
            gate = both[:, :NC * UNITS] * inv
            upward = both[:, NC * UNITS:] * inv
            act = (gate / (1.0 + jnp.exp(-gate)) * upward * share).astype(BF16)
            spread = nn(place, act).astype(BF16)
            for i, r in enumerate(rows):
                act_s[r] = spread[i * ROW:(i + 1) * ROW]
                for m in range(NX):
                    send(act_s.at[r], act_v.at[r, :, act_at], s_act, r_row.at[r], idx(xwrap(x + m + 1), z, 1))

        experts([z])

        def step(k, carry):
            experts(list(up_down(k)))
            return carry
        lax.fori_loop(1, HALF, step, 0)
        experts([last])

        arrived(ctx_v.at[pl.ds(0, NX * NZ - 1)], s_ctx.at[0])
        arrived(ctx_v.at[pl.ds(0, NX * NZ - 1)], s_ctx.at[1])
        @pl.when(half == 0)
        def _():
            arrived(won_v.at[:, pl.ds(0, (NX - 1) * DX)], s_core.at[0])
        arrived(wo_v.at[pl.ds(0, VH // NC), :], s_wo)
        arrived(res_v.at[pl.ds(0, NX)], s_res)

        @pl.when(half == 0)
        def _():
            arrived(wdn_v.at[:, pl.ds(0, (NX - 1) * DX)], s_wd.at[0])
            arrived(wdn_v.at[:, pl.ds(0, DX)], s_wd.at[1])
        arrived(val_v, s_val)
        arrived(act_v, s_act)
        arrived(sum_v, r_out)

    @pl.when(main)
    def _main():
        gain_v[...] = gain_ref[...].astype(F32)
        rs_in[1, 1] = jnp.zeros((ROW, DX), BF16)
        rs2_in[1, 1] = jnp.zeros((ROW, DX), BF16)

        def twin_send(xx):
            view = wd_v.at[wd_rows(xx, half), :]
            send(view, view, s_wd.at[1], r_twin, twin)

        @pl.when(half == 0)
        def _():
            arrived(wd_v.at[wd_rows(x, half), :], r_wd.at[0])

        @pl.when(half == 1)
        def _():
            wd_copy.wait()
        twin_send(x)

        wo_copy.wait()
        arrived(wo_v.at[wo_rows(x, 0), :], r_wo)
        arrived(wo_v.at[pl.ds(0, (NX - 1) * (VH // NC)), :], r_woy)
        to_home()

        def attended(rows):
            for r in rows:
                arrived(val_v.at[r], r_row.at[r])
            stacked = jnp.concatenate([val_v[r] for r in rows], axis=0)
            for o, w in BLOCKS:
                part = nn(stacked, wo_v[:, o:o + w])
                for i, r in enumerate(rows):
                    part_v[r, :, pl.ds(o, w)] = part[i * ROW:(i + 1) * ROW]

        arrived(val_v.at[z], r_row.at[z])
        for i, (o, w) in enumerate(SUBS):
            chain_send(rs_in, rs_out, s_rs, slot_r, 0, 0, i, nn(val_v[z], wo_v[:, o:o + w]))
        attended(list(up_down(1)))

        def rs_step(s, carry):
            chain_step(rs_in, rs_out, s_rs, slot_r, s)

            @pl.when(s < HALF - 1)
            def _():
                attended(list(up_down(s + 1)))

            @pl.when(s == HALF // 2)
            def _():
                arrived(wd_v.at[pl.ds(0, (NX - 1) * UNITS), :], r_wd.at[1])
                for i in range(NX - 1):
                    twin_send(xwrap(x + i + 1))
            return carry
        lax.fori_loop(1, HALF, rs_step, 0)
        attended([last])

        arrived(res_v, r_res)
        resw_v[...] = res_v[...].reshape(DEV * MSG, 128).astype(F32)
        lane = iota((ROW, 128), 1)
        tabs = [resw_v[pl.ds(TOK * JX + t, DEV, stride=MSG), :] for t in range(TOK)]
        table_rows = jnp.concatenate(tabs, axis=0)
        router_copy.wait()

        def ag_send(r, i, way, k):
            view = ag_v.at[r, :, pl.ds(i * PIECE, PIECE)]
            send(view, view, s_ag.at[way], r_ring.at[way, slot_g(k), i], along(way))

        def ag_wait(r, i, way, k):
            arrived(ag_v.at[r, :, pl.ds(i * PIECE, PIECE)], r_ring.at[way, slot_g(k), i])

        bx_at = pl.ds(mo(DAE + x * BX, 128), BX)
        sums = jnp.zeros((ROW, 1), F32)
        logits = jnp.zeros((ROW, 128), F32)
        for i, (o, w) in enumerate(SUBS):
            attn = chain_end(rs_in, slot_r, i)
            att_v[:, pl.ds(o, w)] = attn
            hidden = attn + jnp.concatenate([
                jnp.concatenate([resw_v[pl.ds(t * JX + j, DEV, stride=MSG), :] for t in range(TOK)], axis=0)
                for j in range(o // 128, (o + w) // 128)], axis=1)
            gain = jnp.concatenate(
                [gain_v[pl.ds(x * JX + j, 1), :] for j in range(o // 128, (o + w) // 128)], axis=1)
            scaled = (hidden * gain).astype(BF16)
            if i == 0:
                ag_v[z, :, bx_at] = scaled
                view = ag_v.at[z, :, bx_at]
                for j in (1, 0, 2):
                    send(view, view, s_bx, r_bx, idx(xwrap(x + j + 1), z, 1))
            else:
                ag_v[z, :, pl.ds(o, w)] = scaled
                for piece in range(NPA - 1):
                    if o < (piece + 1) * PIECE <= o + w:
                        ag_send(z, piece, 0, 1)
                        ag_send(z, piece, 1, 1)
            sums = sums + jnp.sum(hidden * hidden, axis=1, keepdims=True)
            logits = logits + nt(scaled, rout_v[:, pl.ds(o, w)])
        high = logits.astype(BF16).astype(F32)
        sums_high = sums.astype(BF16).astype(F32)
        ext = high + pltpu.roll(logits - high, EXPERTS, 1)
        ext = jnp.where(lane == LANE_SUM, sums_high, ext)
        ext = jnp.where(lane == LANE_SUM + 1, sums - sums_high, ext)
        ag_v[z, :, pl.ds(DA, EXT)] = (ext + table_rows).astype(BF16)
        ag_send(z, NPA - 1, 0, 1)
        ag_send(z, NPA - 1, 1, 1)
        arrived(ag_v.at[z, :, pl.ds(DAE, (NX - 1) * BX)], r_bx)
        for i in range(NPA, NP):
            ag_send(z, i, 0, 1)
            ag_send(z, i, 1, 1)

        def dispatch(rows):
            n = len(rows)
            size = n * NX * SLOT
            jj, lane = iota((size, 128), 0), iota((size, 128), 1)
            wanted_lane = LANE_TAB + lax.rem(x + lax.rem(jj // SLOT, NX), NX) * QUAD + quad
            pick = jnp.where(lane == wanted_lane, 1.0, 0.0).astype(BF16)
            picked = nt(pick, jnp.concatenate([ag_v[r, :, pl.ds(DA, EXT)] for r in rows], axis=0))
            jj, tok = iota((size, n * ROW), 0), iota((size, n * ROW), 1)
            wanted = (lax.rem(jj, SLOT) // DEV + 1).astype(F32)
            hit = (picked == wanted) & (lax.rem(jj, DEV) == lax.rem(tok, DEV)) & (jj // (NX * SLOT) == tok // ROW)
            place = jnp.where(hit, 1.0, 0.0).astype(BF16)
            moved = nn(place, jnp.concatenate([ag_v[r, :, pl.ds(0, DAE)] for r in rows], axis=0)).astype(BF16)
            own = jnp.concatenate([place[i * NX * SLOT:i * NX * SLOT + SLOT] for i in range(n)], axis=0)
            shared = nn(own, jnp.concatenate([ag_v[r, :, pl.ds(DAE, NX * BX)] for r in rows], axis=0)).astype(BF16)
            for i, r in enumerate(rows):
                dsp_v[r, pl.ds(0, NX)] = moved[i * NX * SLOT:(i + 1) * NX * SLOT].reshape(NX, SLOT, DAE)
                dsp_v[r, NX] = shared[i * SLOT:(i + 1) * SLOT]
            for r in rows:
                for i in (2, 1, 3, 0):
                    send(dsp_v.at[r, i], d_v.at[r, x], s_dsp, r_row.at[r], idx(xwrap(x + i), z, 0))
                send(dsp_v.at[r, NX], d_v.at[r, NX], s_dsp, r_row.at[r], idx(x, z, 0))

        def returned(rows):
            for r in rows:
                arrived(act_v.at[r], r_row.at[r])
            return jnp.concatenate([act_v[r] for r in rows], axis=0)

        def down_blocks(rows, blocks):
            for o, w in blocks:
                at = pl.ds(o, w)
                part = nn(jnp.concatenate([act_v[r] for r in rows], axis=0), wd_v[:, o:o + w])
                for i, r in enumerate(rows):
                    part_v[r, :, at] = part[i * ROW:(i + 1) * ROW]

        def down_part(rows):
            returned(rows)
            down_blocks(rows, BLOCKS)

        def down_first():
            spread = returned([z])
            for o, w in BLOCKS:
                at = pl.ds(o, w)
                part_v[z, :, at] = nn(spread, wd_v[:, o:o + w]) + att_v[:, at]
        dispatch([z])

        def ag_step(k, carry):
            behind = list(up_down(k - 1))
            done = list(up_down(k - DOWN - 1))

            def pieces(i):
                for way in (early, 1 - early):
                    r = wrap(z - (1 - 2 * way) * k)
                    ag_wait(r, i, way, k)

                    @pl.when((way == 0) | (k < HALF - 1))
                    def _():
                        ag_send(r, i, way, k + 1)
            def follow(i):
                @pl.when(k > DOWN + 1)
                def _():
                    for way in (early, 1 - early):
                        chain_piece(rs2_in, rs2_out, s_rs2, slot_l, k - DOWN - 1, i, way)
            pieces(0)

            @pl.when(k >= 2)
            def _():
                dispatch(behind)
            pieces(1)

            @pl.when(k == DOWN)
            def _():
                arrived(wd_v.at[pl.ds(0, NX * UNITS), :], r_twin)
                down_first()

            @pl.when(k == DOWN + 1)
            def _():
                for i, (o, w) in enumerate(SUBS):
                    chain_send(rs2_in, rs2_out, s_rs2, slot_l, 0, 0, i, part_v[z, :, pl.ds(o, w)])

            @pl.when(k > DOWN + 1)
            def _():
                returned(done)
                down_blocks(done, BLOCKS[:1])
            pieces(2)

            @pl.when(k > DOWN + 1)
            def _():
                down_blocks(done, BLOCKS[1:])
            pieces(3)
            for i in range(NS):
                follow(i)
            return carry
        lax.fori_loop(1, HALF, ag_step, 0)
        dispatch(list(up_down(HALF - 1)))
        for i in range(NP):
            ag_wait(last, i, 0, HALF)
        dispatch([last])

        down_part(list(up_down(HALF - DOWN - 1)))

        def late(k, carry):
            chain_step(rs2_in, rs2_out, s_rs2, slot_l, k - 1)
            down_part(list(up_down(k)))
            return carry
        lax.fori_loop(HALF - DOWN, HALF, late, 0)
        chain_step(rs2_in, rs2_out, s_rs2, slot_l, HALF - 1)
        down_part([last])

        for t in range(TOK * JX, MSG):
            fin_v[pl.ds(t, DEV, stride=MSG), :] = jnp.zeros((DEV, 128), F32)
        for i, (o, w) in enumerate(SUBS):
            mixed = chain_end(rs2_in, slot_l, i)
            for t in range(TOK):
                for j in range(o // 128, (o + w) // 128):
                    fin_v[pl.ds(t * JX + j, DEV, stride=MSG), :] = (
                        mixed[t * DEV:(t + 1) * DEV, j * 128 - o:j * 128 - o + 128])
        fin_s[...] = fin_v[...].reshape(DEV, MSG, 128).astype(BF16)
        for i in range(DEV - 1):
            to = lax.rem(dev + i + 1, DEV)
            send(fin_s.at[to], sum_v.at[x], s_out, r_out, idx(to // NC, z, lax.rem(to, NC)))
        sum_v[x] = fin_s[dev]

        arrived(ctx_v, s_ctx.at[0])
        arrived(wo_v.at[pl.ds(0, 2 * (NX - 1) * (VH // NC)), :], s_wo)
        arrived(res_v.at[pl.ds(0, NX)], s_res)
        arrived(vu_v.at[pl.ds(0, VH // NC), :], s_core.at[0])
        arrived(wgu_v.at[:, pl.ds(0, UNITS)], s_core.at[1])
        arrived(wgu_v.at[:, pl.ds(0, UNITS)], s_core.at[2])
        arrived(wd_v.at[pl.ds(0, (NX - 1) * UNITS), :], s_wd.at[0])
        arrived(wd_v.at[pl.ds(0, NX * UNITS), :], s_wd.at[1])
        for way in range(2):
            arrived(rs_out.at[way, pl.ds(way, HALF - way)], s_rs.at[way])
            arrived(rs2_out.at[way, pl.ds(way, HALF - way)], s_rs2.at[way])
            arrived(ag_v.at[pl.ds(0, HALF - way)], s_ag.at[way])
        arrived(ag_v.at[z, :, pl.ds(DAE, (NX - 1) * BX)], s_bx)
        arrived(dsp_v, s_dsp)
        arrived(fin_s.at[pl.ds(0, DEV - 1)], s_out)
        arrived(sum_v.at[pl.ds(0, NX - 1)], r_out)

    resf_v[...] = sum_v[...].reshape(NX * MSG, 128).astype(F32) + resf_v[...]
    for t in range(TOK):
        rows = [resf_v[pl.ds(xx * MSG + t * JX, JX), :] for xx in range(NX)]
        outv_v[t] = jnp.concatenate(rows, axis=0).astype(BF16)
    out_copy = pltpu.make_async_copy(outv_v, out_ref, l_misc)
    out_copy.start()
    out_copy.wait()


def body(
    cache_kv, new_kv, queries, lengths, resid, value_up, out_proj, norm_gain, router, expert_ids, slots, w_gate, w_up,
    w_down,
):
    seqs, steps = resid.shape[:2]
    cache_len = cache_kv.shape[1]
    hbm = pl.BlockSpec(memory_space=pltpu.HBM)
    dma = pltpu.SemaphoreType.DMA
    regular = pltpu.SemaphoreType.REGULAR
    scratch = [
        pltpu.VMEM(new_kv.shape, BF16),
        pltpu.SMEM(lengths.shape, jnp.int32),
        pltpu.VMEM(resid.shape, BF16),
        pltpu.VMEM((D // 128, 128), BF16),
        pltpu.SMEM(expert_ids.shape, jnp.int32),
        pltpu.SMEM(slots.shape, jnp.int32),
        pltpu.VMEM((seqs, KV, cache_len), BF16),
        pltpu.VMEM((seqs, steps * H, KV), BF16),
        pltpu.VMEM((steps * H, cache_len), F32),
        pltpu.VMEM((H * 16, 128), F32),
        pltpu.VMEM((H, 16, 128), BF16),
        pltpu.VMEM((NZ, DEV, 16, 128), BF16),
        pltpu.VMEM((DEV * 16, 128), F32),
        pltpu.VMEM((VH, LAT), BF16),
        pltpu.VMEM((NZ, ROW, NX * VH), BF16),
        pltpu.VMEM((NX * VH, DX), BF16),
        pltpu.VMEM((H, 16, 128), BF16),
        pltpu.VMEM((VH // NC, D), BF16),
        pltpu.VMEM((2, HALF + 1, ROW, DX), BF16),
        pltpu.VMEM((2, HALF, ROW, DX), BF16),
        pltpu.VMEM((ROW, DX), F32),
        pltpu.VMEM((NX, MSG, 128), BF16),
        pltpu.VMEM((NX * MSG, 128), F32),
        pltpu.VMEM((DEV, MSG, 128), BF16),
        pltpu.VMEM((DEV * MSG, 128), F32),
        pltpu.VMEM((D // 128, 128), F32),
        pltpu.VMEM((128, DX), BF16),
        pltpu.VMEM((NZ, ROW, DG), BF16),
        pltpu.VMEM((NZ, NX + 1, SLOT, DAE), BF16),
        pltpu.VMEM((NZ, NX + 1, SLOT, DAE), BF16),
        pltpu.VMEM((D, 2 * NC * UNITS), BF16),
        pltpu.VMEM((NZ, ROW, NC * UNITS), BF16),
        pltpu.VMEM((NZ, ROW, NX * NC * UNITS), BF16),
        pltpu.VMEM((NX * NC * UNITS, DX), BF16),
        pltpu.VMEM((UNITS, D), BF16),
        pltpu.VMEM((2, HALF + 1, ROW, DX), BF16),
        pltpu.VMEM((2, HALF, ROW, DX), BF16),
        pltpu.VMEM((NZ, ROW, DX), F32),
        pltpu.VMEM((DEV * MSG, 128), F32),
        pltpu.VMEM((DEV, MSG, 128), BF16),
        pltpu.VMEM((NX, MSG, 128), BF16),
        pltpu.VMEM((TOK, NX * JX, 128), BF16),
        dma((seqs,)), dma, dma((3,)), dma((6,)),
        dma((2,)), dma, dma, dma((3,)), dma((2,)), dma, dma((2,)), dma((2,)), dma((2,)), dma, dma, dma, dma,
        dma, dma, dma((NX, 2)), dma, dma((4,)), dma((2,)), dma((NZ,)), dma((2, 6, max(NP, NS))), dma, dma, dma,
        regular, regular,
    ]
    out = pl.pallas_call(
        kernel,
        out_shape=jax.ShapeDtypeStruct((TOK, NX * JX, 128), BF16),
        in_specs=[hbm] * 14,
        out_specs=hbm,
        scratch_shapes=scratch,
        compiler_params=pltpu.CompilerParams(
            collective_id=0, has_side_effects=True, vmem_limit_bytes=(64 << 20) - (64 << 10)),
        name="layer",
    )(
        jnp.transpose(cache_kv, (0, 2, 1)), new_kv, queries.reshape(seqs, steps * H, KV), lengths, resid,
        value_up.T, out_proj, norm_gain.reshape(D // 128, 128), router.T, expert_ids, slots, w_gate, w_up, w_down,
    )
    return out.reshape(resid.shape)


def solution(mesh):
    return jax.shard_map(
        body,
        mesh=mesh,
        in_specs=(
            P(("rep", "ep"), None, None),
            P(("rep", "ep"), None, None),
            P(("rep", "ep"), None, None, None),
            P(("rep", "ep")),
            P(("rep", "ep"), None, None),
            P(None, "ep"),
            P("ep", None),
            P(),
            P(),
            P(("rep", "ep"), None, None),
            P(("rep", "ep"), None, None),
            P(None, "ep"),
            P(None, "ep"),
            P("ep", None),
        ),
        out_specs=P(("rep", "ep"), None, None),
        check_vma=False,
    )
```

```python
import functools
import math

import jax
import jax.numpy as jnp
from jax import lax
from jax.experimental import pallas as pl
from jax.experimental.pallas import tpu as pltpu
from jax.sharding import PartitionSpec as P

NX, NZ, NC = 4, 16, 2
DEV = NX * NC
HALF = NZ // 2

D = 7168
H = 64
LAT = 512
VH = 128
KV = 576
EXPERTS = 16
TOP = 8
CAP = 2
QK = 192
TOK = 4
UNITS = 128
ROW = DEV * TOK
SLOT = DEV * CAP
DX = D // NX
EXT = 128
JX = DX // 128
MSG = 64
LANE_SUM = 32
LANE_TOK = 48
LANE_TAB = 64
QUAD = EXPERTS // NX
CHIPS_PER = NZ // QUAD

route_scale = 2.827
norm_eps = 1e-06

CUBE = 4

BX = 128
DA = DX - BX
DAE = DA + EXT
DG = DAE + NX * BX
PIECES = ((0, 640), (640, 512), (1152, 640), (1792, 512))
SUBS = ((DA, BX), (0, 256), (256, 256), (512, 256), (768, 256), (1024, 256), (1280, 384))
NS = len(SUBS)
NP = len(PIECES)
NPA = sum(o < DAE for o, _ in PIECES)
BLOCKS = ((0, 512), (512, 512), (1024, 768))
DOWN = 4

F32 = jnp.float32
BF16 = jnp.bfloat16


def mo(value, by):
    return pl.multiple_of(value, by)


def nt(a, b):
    return lax.dot_general(a, b, (((1,), (1,)), ((), ())), preferred_element_type=F32)


def nn(a, b):
    return lax.dot_general(a, b, (((1,), (0,)), ((), ())), preferred_element_type=F32)


def iota(shape, axis):
    return lax.broadcasted_iota(jnp.int32, shape, axis)


def kernel(
    cache_h, new_h, q_h, len_h, resid_h, vu_h, wo_h, gain_h, router_h, ids_h, slots_h, wg_h, wu_h, wd_h,
    out_ref,
    new_ref, len_ref, resid_ref, gain_ref, ids_ref, slots_ref,
    cache_v, q_v, score_v, stage_v, ctx_v, arr_v, arrf_v, vu_v, val_v, wo_v, ctxn_v, won_v, rs_in, rs_out, att_v,
    ress_v, resf_v, res_v, resw_v, gain_v, rout_v, ag_v, dsp_v, shr_v, d_v, wgu_v, act_s, act_v, wd_v, wdn_v, rs2_in, rs2_out,
    part_v, fin_v, fin_s, sum_v, outv_v,
    l_cache, l_misc, l_weights, l_small,
    s_ctx, s_res, s_wo, s_core, s_wd, s_val, s_rs, s_ag, s_rs2, s_dsp, s_act, s_out, s_bx, s_shr,
    r_res, r_wo, r_wox, r_woy, r_core, r_wd, r_row, r_ring, r_out, r_bx, r_twin,
    row_sem, all_sem,
):
    me = lax.axis_index("ep")
    c = lax.rem(me, NC)
    z = lax.rem(me // NC, NZ)
    x = me // (NC * NZ)
    dev = x * NC + c
    quad = z // CHIPS_PER
    group = lax.axis_index("rep")
    half = lax.rem(group, 2)
    twin = {"rep": group + 1 - 2 * half, "ep": me}

    def idx(xx, zz, cc):
        return {"ep": (xx * NZ + zz) * NC + cc}

    def wrap(zz):
        return lax.rem(zz + 2 * NZ, NZ)

    def xwrap(xx):
        return lax.rem(xx, NX)

    def send(src, dst, ssem, rsem, to):
        pltpu.make_async_remote_copy(src_ref=src, dst_ref=dst, send_sem=ssem, recv_sem=rsem, device_id=to).start()

    def arrived(ref, sem):
        pltpu.make_async_copy(ref, ref, sem).wait()

    main = c == 1
    side = c == 0

    loads = [pltpu.make_async_copy(q_h, q_v, l_misc)]
    loads += [pltpu.make_async_copy(cache_h.at[b], cache_v.at[b], l_cache.at[b]) for b in range(2)]
    small = [
        pltpu.make_async_copy(src, dst, l_small.at[i]) for i, (src, dst) in enumerate((
            (new_h, new_ref), (len_h, len_ref), (resid_h, resid_ref), (gain_h, gain_ref), (ids_h, ids_ref),
            (slots_h, slots_ref)))
    ]
    for load in loads[:2] + small[:2] + loads[2:] + small[2:]:
        load.start()

    bar = pltpu.get_barrier_semaphore()

    @pl.when(side)
    def _():
        def greet(o, carry):
            far = HALF - (o + 1) // 2
            zz = wrap(jnp.where(lax.rem(o, 2) == 1, z + far, z - far))
            for xx in range(NX):
                pl.semaphore_signal(bar, inc=1, device_id=idx(xx, zz, 1))
            return carry
        lax.fori_loop(0, NZ, greet, 0)

    @pl.when(main)
    def _():
        for xx in range(NX):
            pl.semaphore_signal(bar, inc=1, device_id=idx(xx, z, 0))
            pl.semaphore_signal(bar, inc=1, device_id=idx(xx, wrap(z + HALF), 1))
        for step in (1, -1):
            pl.semaphore_signal(bar, inc=1, device_id=idx(x, wrap(z + step), 1))
        pl.semaphore_signal(bar, inc=1, device_id=twin)

    gate_at = pl.ds(mo(c * UNITS, UNITS), UNITS)
    up_at = pl.ds(mo((NC + c) * UNITS, UNITS), UNITS)
    vu_at = pl.ds(mo(c * (VH // NC), VH // NC), VH // NC)
    router_copy = pltpu.make_async_copy(
        router_h.at[:, pl.ds(mo(x * DX, 128), DX)], rout_v.at[pl.ds(0, EXPERTS), :], l_weights.at[1])
    gate_copy = pltpu.make_async_copy(wg_h, wgu_v.at[:, gate_at], l_weights.at[1])
    up_copy = pltpu.make_async_copy(wu_h, wgu_v.at[:, up_at], l_weights.at[2])
    vu_copy = pltpu.make_async_copy(vu_h, vu_v.at[vu_at, :], l_weights.at[0])

    def wo_rows(xx, cc):
        return pl.ds(mo(xx * VH + cc * (VH // NC), VH // NC), VH // NC)

    def own_columns(xx):
        return pl.ds(mo(xx * DX, 128), DX)

    def wd_rows(xx, cc):
        return pl.ds(mo((xx * NC + cc) * UNITS, UNITS), UNITS)

    wo_copy = pltpu.make_async_copy(wo_h.at[:, own_columns(x)], wo_v.at[wo_rows(x, 1), :], l_weights.at[0])
    wd_copy = pltpu.make_async_copy(wd_h.at[:, own_columns(x)], wd_v.at[wd_rows(x, half), :], l_weights.at[2])

    def wo_half(xx, h):
        return pl.ds(mo(xx * DX + h * (DX // 2), 128), DX // 2)

    def wo_send(source):
        for h in range(2):
            for i in range(NX - 1):
                xx = xwrap(x + i + 1)
                send(source.at[:, wo_half(xx, h)], wo_v.at[wo_rows(x, half), wo_half(0, h)], s_wo, r_wox.at[x, h],
                     idx(xx, z, 1))

    def row_next():
        @pl.when(main & (half == 0))
        def _():
            arrived(won_v.at[:, pl.ds(0, (NX - 1) * DX)], r_core.at[2])
            wo_send(won_v)

    def row_start():
        @pl.when(side)
        def _():
            pl.semaphore_wait(bar, NX)
            pl.semaphore_signal(row_sem, inc=1, device_id=idx(x, z, 1))

        @pl.when(main)
        def _():
            pl.semaphore_wait(row_sem, 1)

        @pl.when(main)
        def _():
            @pl.when(half == 1)
            def _():
                wo_send(wo_h)
            wo_copy.start()
            send(vu_h, vu_v.at[vu_at, :], s_core.at[0], r_core.at[0], idx(x, z, 0))
            rout_v[...] = jnp.zeros_like(rout_v)
            router_copy.start()

        @pl.when(side)
        def _():
            vu_copy.start()
            @pl.when(half == 0)
            def _():
                for i in range(NX - 1):
                    columns = own_columns(xwrap(x + i + 1))
                    send(wo_h.at[:, columns], won_v.at[:, columns], s_core.at[0], r_core.at[2], idx(x, z, 1))
            send(wo_h.at[:, own_columns(x)], wo_v.at[wo_rows(x, 0), :], s_wo, r_wo, idx(x, z, 1))

    scale = 1.0 / math.sqrt(QK)
    blk = 512
    nblk = cache_v.shape[2] // blk
    loads[0].wait()
    small[0].wait()
    small[1].wait()
    for b in range(2):
        qb = q_v[b]
        qf = qb.astype(F32)
        step_of = iota((2 * H, 1), 0) // H
        new_rows = [new_ref[b, pl.ds(t, 1), :].astype(F32) for t in range(2)]
        s_new = [jnp.sum(qf * row, axis=1, keepdims=True) * scale for row in new_rows]
        s_new[1] = jnp.where(step_of >= 1, s_new[1], -jnp.inf)
        peak = jnp.maximum(s_new[0], s_new[1])
        loads[1 + b].wait()
        for p in range(nblk):
            sc = nn(qb, cache_v[b, :, pl.ds(p * blk, blk)]) * scale
            pos = iota((2 * H, blk), 1) + p * blk
            sc = jnp.where(pos < len_ref[b], sc, -jnp.inf)
            score_v[:, pl.ds(p * blk, blk)] = sc
            peak = jnp.maximum(peak, jnp.max(sc, axis=1, keepdims=True))
        if b == 0:
            row_start()
        else:
            row_next()
        p_new = [jnp.exp(s - peak) for s in s_new]
        total = p_new[0] + p_new[1]
        acc = p_new[0].astype(BF16).astype(F32) * new_rows[0][:, :LAT]
        acc = acc + p_new[1].astype(BF16).astype(F32) * new_rows[1][:, :LAT]
        for p in range(nblk):
            pr = jnp.exp(score_v[:, pl.ds(p * blk, blk)] - peak)
            total = total + jnp.sum(pr, axis=1, keepdims=True)
            acc = acc + nt(pr.astype(BF16), cache_v[b, pl.ds(0, LAT), pl.ds(p * blk, blk)])
        ctx = acc / total
        for s in range(2):
            for j in range(LAT // 128):
                stage_v[pl.ds(j * TOK + b * 2 + s, H, stride=16), :] = ctx[s * H:(s + 1) * H, j * 128:(j + 1) * 128]
    ctx_v[...] = stage_v[...].reshape(H, 16, 128).astype(BF16)

    @pl.when(main)
    def _():
        send(ctx_v, ctxn_v, s_ctx.at[0], r_core.at[1], idx(x, z, 0))
        pl.semaphore_wait(bar, NX * NZ + NX + 3)
        pl.semaphore_signal(all_sem, inc=1, device_id=idx(x, z, 0))

    @pl.when(side)
    def _():
        arrived(ctxn_v, r_core.at[1])
        pl.semaphore_wait(all_sem, 1)

    def near(o):
        return wrap(jnp.where(lax.rem(o, 2) == 1, z - (o + 1) // 2, z + o // 2))

    def ctx_send(o, carry):
        zz = near(o)
        for i in range(NX):
            xx = xwrap(x + i + 1)
            own = (zz == z) & (xx == x)
            for core, tiles in ((0, ctx_v), (1, ctxn_v)):
                @pl.when(jnp.logical_not(own))
                def _():
                    send(tiles.at[xx * NZ + zz], arr_v.at[z, x * NC + core], s_ctx.at[core], r_row.at[z],
                         idx(xx, zz, 0))

                @pl.when(own)
                def _():
                    arr_v[z, x * NC + core] = tiles[xx * NZ + zz]
        return carry

    @pl.when(side)
    def _():
        lax.fori_loop(0, NZ, ctx_send, 0)

        @pl.when(half == 0)
        def _():
            for i in range(NX - 1):
                columns = own_columns(xwrap(x + i + 1))
                send(wd_h.at[:, columns], wdn_v.at[:, columns], s_wd.at[0], r_core.at[0], idx(x, z, 1))
            send(wd_h.at[:, own_columns(x)], wd_v.at[wd_rows(x, half), :], s_wd.at[1], r_wd.at[0], idx(x, z, 1))

    @pl.when(main)
    def _():
        for h in range(2):
            for i in range(NX - 1):
                xx = i + jnp.where(x <= i, 1, 0)
                view = wo_v.at[wo_rows(xx, half), wo_half(0, h)]
                arrived(view, r_wox.at[xx, h])
                send(view, view, s_wo, r_woy, twin)

        def wd_send(source):
            for i in range(NX - 1):
                xx = xwrap(x + i + 1)
                send(source.at[:, own_columns(xx)], wd_v.at[wd_rows(x, half), :], s_wd.at[0], r_wd.at[1], idx(xx, z, 1))

        @pl.when(half == 0)
        def _():
            arrived(wdn_v.at[:, pl.ds(0, (NX - 1) * DX)], r_core.at[0])
            wd_send(wdn_v)

        @pl.when(half == 1)
        def _():
            wd_copy.start()
            wd_send(wd_h)
        send(wg_h, wgu_v.at[:, gate_at], s_core.at[1], r_core.at[2], idx(x, z, 0))
        send(wu_h, wgu_v.at[:, up_at], s_core.at[2], r_core.at[3], idx(x, z, 0))

    @pl.when(side)
    def _():
        gate_copy.start()
        up_copy.start()

    for load in small[2:]:
        load.wait()

    rows8, lanes8 = iota((8, 128), 0), iota((8, 128), 1)
    table = jnp.where(lanes8 == LANE_TOK, (rows8 + 1).astype(F32), 0.0)
    for t in range(TOK):
        for k in range(TOP):
            hit = (rows8 == t) & (lanes8 == ids_ref[t // 2, t % 2, k] + LANE_TAB)
            table = jnp.where(hit, (slots_ref[t // 2, t % 2, k] + 1).astype(F32), table)
    resf_v[...] = jnp.zeros_like(resf_v)
    for t in range(TOK):
        row = resid_ref[t // 2, pl.ds(t % 2, 1), :].astype(F32)
        for xx in range(NX):
            for j in range(JX):
                col = xx * DX + j * 128
                resf_v[pl.ds(xx * MSG + t * JX + j, 1), :] = row[:, col:col + 128]
    for xx in range(NX):
        resf_v[pl.ds(xx * MSG + TOK * JX, 8), :] = table
    ress_v[...] = resf_v[...].reshape(NX, MSG, 128).astype(BF16)

    def to_home():
        for i in range(NX):
            xx = xwrap(x + i)
            send(ress_v.at[xx], res_v.at[dev], s_res, r_res, idx(xx, wrap(z + HALF), 1))

    def up_down(k):
        return wrap(z - k), wrap(z + k)

    early = jnp.where(lax.rem(z, CUBE) < CUBE // 2, 1, 0)
    last = wrap(z + HALF)

    def along(way):
        return idx(x, wrap(z + 1 - 2 * way), c)

    def ways(pieces):
        for i in range(pieces + 1):
            if i < pieces:
                yield i, early
            if i > 0:
                yield i - 1, 1 - early

    def slot_r(s):
        return lax.rem(s, 3)

    def slot_l(s):
        return 3 + lax.rem(s, 3)

    def slot_g(k):
        return lax.rem(k + 2, 3)

    def chain_send(in_ref, out_buf, ssem, slot, way, s, i, total):
        at = pl.ds(*SUBS[i])
        out_buf[way, s, :, at] = total.astype(BF16)
        send(out_buf.at[way, s, :, at], in_ref.at[way, s + 1, :, at], ssem.at[way], r_ring.at[way, slot(s + 1), i],
             along(way))

    def chain_piece(in_ref, out_buf, ssem, slot, s, i, way):
        at = pl.ds(*SUBS[i])
        r = wrap(z - (1 - 2 * way) * s)

        @pl.when((way == 0) | (s >= 2))
        def _():
            arrived(in_ref.at[way, s, :, at], r_ring.at[way, slot(s), i])
        chain_send(in_ref, out_buf, ssem, slot, way, s, i, part_v[r, :, at] + in_ref[way, s, :, at].astype(F32))

    def chain_step(in_ref, out_buf, ssem, slot, s):
        for i, way in ways(NS):
            chain_piece(in_ref, out_buf, ssem, slot, s, i, way)

    def chain_end(in_ref, slot, i):
        at = pl.ds(*SUBS[i])
        for way in range(2):
            arrived(in_ref.at[way, HALF, :, at], r_ring.at[way, slot(HALF), i])
        return part_v[last, :, at] + in_ref[0, HALF, :, at].astype(F32) + in_ref[1, HALF, :, at].astype(F32)

    @pl.when(side)
    def _side():
        vu_copy.wait()
        arrived(vu_v.at[pl.ds(0, VH // NC), :], r_core.at[0])
        own_lanes = pl.ds(mo(x * VH, VH), VH)

        def ctx_row(r):
            @pl.when(r == z)
            def _():
                arrived(arr_v.at[r, pl.ds(0, DEV - NC)], r_row.at[r])

            @pl.when(r != z)
            def _():
                arrived(arr_v.at[r], r_row.at[r])

            arrf_v[...] = arr_v[r].reshape(DEV * 16, 128).astype(F32)
            cols = []
            for j in range(LAT // 128):
                cols.append(jnp.concatenate(
                    [arrf_v[pl.ds(j * TOK + t, DEV, stride=16), :] for t in range(TOK)], axis=0))
            rows = jnp.concatenate(cols, axis=1).astype(BF16)
            val_v[r, :, own_lanes] = nt(rows, vu_v[...]).astype(BF16)
            view = val_v.at[r, :, own_lanes]
            for i in range(NX):
                send(view, view, s_val, r_row.at[r], idx(xwrap(x + i + 1), z, 1))

        def ctx_step(o, carry):
            ctx_row(near(o))

            return carry
        lax.fori_loop(0, NZ, ctx_step, 0)
        to_home()

        gate_copy.wait()
        up_copy.wait()
        arrived(wgu_v.at[:, pl.ds(0, UNITS)], r_core.at[2])
        arrived(wgu_v.at[:, pl.ds(0, UNITS)], r_core.at[3])

        own_expert = x * QUAD + quad
        act_at = pl.ds(mo(x * NC * UNITS, 128), NC * UNITS)

        def experts(rows):
            for r in rows:
                arrived(d_v.at[r], r_row.at[r])
            both = jnp.zeros((SLOT * len(rows), 2 * NC * UNITS), F32)
            ext = jnp.zeros((SLOT * len(rows), EXT), F32)
            shared = jnp.concatenate([d_v[r, :, pl.ds(NX * DAE, NX * BX)] for r in rows], axis=0)
            for xx in range(NX):
                both = both + nn(
                    jnp.concatenate([d_v[r, :, pl.ds(xx * DAE, DA)] for r in rows], axis=0),
                    wgu_v[xx * DX:xx * DX + DA, :])
                both = both + nn(shared[:, xx * BX:(xx + 1) * BX], wgu_v[xx * DX + DA:(xx + 1) * DX, :])
                piece = jnp.concatenate([d_v[r, :, pl.ds(xx * DAE + DA, EXT)] for r in rows], axis=0)
                ext = ext + piece.astype(F32)
            n = len(rows)
            token = nt(jnp.where(iota((n * ROW, 128), 1) == LANE_TOK, 1.0, 0.0).astype(BF16), piece)
            piece = piece.astype(F32)
            jj, tok = iota(token.shape, 1), iota(token.shape, 0)
            wanted = (lax.rem(tok, ROW) // DEV + 1).astype(F32)
            hit = (token == wanted) & (lax.rem(jj, DEV) == lax.rem(tok, DEV)) & (jj // SLOT == tok // ROW)
            place = jnp.where(hit, 1.0, 0.0).astype(BF16)
            lane = iota(ext.shape, 1)
            squares = jnp.sum(
                jnp.where((lane == LANE_SUM) | (lane == LANE_SUM + 1), ext, 0.0), axis=1, keepdims=True)
            inv = lax.rsqrt(squares / D + norm_eps)
            logits = (ext + pltpu.roll(ext, EXT - EXPERTS, 1)) * inv
            named = (pltpu.roll(piece, EXT - LANE_TAB, 1) > 0.0) & (lane < EXPERTS)
            gates = jnp.where(named, 1.0 / (1.0 + jnp.exp(-logits)), 0.0)
            norm = jnp.sum(gates, axis=1, keepdims=True)
            mine = jnp.sum(jnp.where(lane == own_expert, gates, 0.0), axis=1, keepdims=True)
            share = jnp.where(norm > 0.0, route_scale * mine / norm, 0.0)
            gate = both[:, :NC * UNITS] * inv
            upward = both[:, NC * UNITS:] * inv
            act = (gate / (1.0 + jnp.exp(-gate)) * upward * share).astype(BF16)
            spread = nn(place, act).astype(BF16)
            for i, r in enumerate(rows):
                act_s[r] = spread[i * ROW:(i + 1) * ROW]
                for m in range(NX):
                    send(act_s.at[r], act_v.at[r, :, act_at], s_act, r_row.at[r], idx(xwrap(x + m + 1), z, 1))

        experts([z])

        def step(k, carry):
            experts(list(up_down(k)))
            return carry
        lax.fori_loop(1, HALF, step, 0)
        experts([last])

        arrived(ctx_v.at[pl.ds(0, NX * NZ - 1)], s_ctx.at[0])
        arrived(ctx_v.at[pl.ds(0, NX * NZ - 1)], s_ctx.at[1])
        @pl.when(half == 0)
        def _():
            arrived(won_v.at[:, pl.ds(0, (NX - 1) * DX)], s_core.at[0])
        arrived(wo_v.at[pl.ds(0, VH // NC), :], s_wo)
        arrived(res_v.at[pl.ds(0, NX)], s_res)

        @pl.when(half == 0)
        def _():
            arrived(wdn_v.at[:, pl.ds(0, (NX - 1) * DX)], s_wd.at[0])
            arrived(wdn_v.at[:, pl.ds(0, DX)], s_wd.at[1])
        arrived(val_v, s_val)
        arrived(act_v, s_act)
        arrived(sum_v, r_out)

    @pl.when(main)
    def _main():
        gain_v[...] = gain_ref[...].astype(F32)
        rs_in[1, 1] = jnp.zeros((ROW, DX), BF16)
        rs2_in[1, 1] = jnp.zeros((ROW, DX), BF16)

        def twin_send(xx):
            view = wd_v.at[wd_rows(xx, half), :]
            send(view, view, s_wd.at[1], r_twin, twin)

        @pl.when(half == 0)
        def _():
            arrived(wd_v.at[wd_rows(x, half), :], r_wd.at[0])

        @pl.when(half == 1)
        def _():
            wd_copy.wait()
        twin_send(x)

        wo_copy.wait()
        arrived(wo_v.at[wo_rows(x, 0), :], r_wo)
        arrived(wo_v.at[pl.ds(0, (NX - 1) * (VH // NC)), :], r_woy)
        to_home()

        def attended(rows):
            for r in rows:
                arrived(val_v.at[r], r_row.at[r])
            stacked = jnp.concatenate([val_v[r] for r in rows], axis=0)
            for o, w in BLOCKS:
                part = nn(stacked, wo_v[:, o:o + w])
                for i, r in enumerate(rows):
                    part_v[r, :, pl.ds(o, w)] = part[i * ROW:(i + 1) * ROW]

        arrived(val_v.at[z], r_row.at[z])
        for i, (o, w) in enumerate(SUBS):
            chain_send(rs_in, rs_out, s_rs, slot_r, 0, 0, i, nn(val_v[z], wo_v[:, o:o + w]))
        attended(list(up_down(1)))

        def rs_step(s, carry):
            chain_step(rs_in, rs_out, s_rs, slot_r, s)

            @pl.when(s < HALF - 1)
            def _():
                attended(list(up_down(s + 1)))

            @pl.when(s == HALF // 2)
            def _():
                arrived(wd_v.at[pl.ds(0, (NX - 1) * UNITS), :], r_wd.at[1])
                for i in range(NX - 1):
                    twin_send(xwrap(x + i + 1))
            return carry
        lax.fori_loop(1, HALF, rs_step, 0)
        attended([last])

        arrived(res_v, r_res)
        resw_v[...] = res_v[...].reshape(DEV * MSG, 128).astype(F32)
        lane = iota((ROW, 128), 1)
        tabs = [resw_v[pl.ds(TOK * JX + t, DEV, stride=MSG), :] for t in range(TOK)]
        table_rows = jnp.concatenate(tabs, axis=0)
        router_copy.wait()

        def ag_send(r, i, way, k):
            view = ag_v.at[r, :, pl.ds(*PIECES[i])]
            send(view, view, s_ag.at[way], r_ring.at[way, slot_g(k), i], along(way))

        def ag_wait(r, i, way, k):
            arrived(ag_v.at[r, :, pl.ds(*PIECES[i])], r_ring.at[way, slot_g(k), i])

        bx_at = pl.ds(mo(DAE + x * BX, 128), BX)
        sums = jnp.zeros((ROW, 1), F32)
        logits = jnp.zeros((ROW, 128), F32)
        for i, (o, w) in enumerate(SUBS):
            attn = chain_end(rs_in, slot_r, i)
            att_v[:, pl.ds(o, w)] = attn
            hidden = attn + jnp.concatenate([
                jnp.concatenate([resw_v[pl.ds(t * JX + j, DEV, stride=MSG), :] for t in range(TOK)], axis=0)
                for j in range(o // 128, (o + w) // 128)], axis=1)
            gain = jnp.concatenate(
                [gain_v[pl.ds(x * JX + j, 1), :] for j in range(o // 128, (o + w) // 128)], axis=1)
            scaled = (hidden * gain).astype(BF16)
            if i == 0:
                ag_v[z, :, bx_at] = scaled
                view = ag_v.at[z, :, bx_at]
                for j in (1, 0, 2):
                    send(view, view, s_bx, r_bx, idx(xwrap(x + j + 1), z, 1))
            else:
                ag_v[z, :, pl.ds(o, w)] = scaled
                for piece, (start, size) in enumerate(PIECES[:NPA - 1]):
                    if o < start + size <= o + w:
                        ag_send(z, piece, 0, 1)
                        ag_send(z, piece, 1, 1)
            sums = sums + jnp.sum(hidden * hidden, axis=1, keepdims=True)
            logits = logits + nt(scaled, rout_v[:, pl.ds(o, w)])
        high = logits.astype(BF16).astype(F32)
        sums_high = sums.astype(BF16).astype(F32)
        ext = high + pltpu.roll(logits - high, EXPERTS, 1)
        ext = jnp.where(lane == LANE_SUM, sums_high, ext)
        ext = jnp.where(lane == LANE_SUM + 1, sums - sums_high, ext)
        ag_v[z, :, pl.ds(DA, EXT)] = (ext + table_rows).astype(BF16)
        ag_send(z, NPA - 1, 0, 1)
        ag_send(z, NPA - 1, 1, 1)
        arrived(ag_v.at[z, :, pl.ds(DAE, (NX - 1) * BX)], r_bx)
        for i in range(NPA, NP):
            ag_send(z, i, 0, 1)
            ag_send(z, i, 1, 1)

        d_at = pl.ds(mo(x * DAE, 128), DAE)

        def dispatch(rows):
            n = len(rows)
            size = n * NX * SLOT
            jj, lane = iota((size, 128), 0), iota((size, 128), 1)
            wanted_lane = LANE_TAB + lax.rem(x + lax.rem(jj // SLOT, NX), NX) * QUAD + quad
            pick = jnp.where(lane == wanted_lane, 1.0, 0.0).astype(BF16)
            picked = nt(pick, jnp.concatenate([ag_v[r, :, pl.ds(DA, EXT)] for r in rows], axis=0))
            jj, tok = iota((size, n * ROW), 0), iota((size, n * ROW), 1)
            wanted = (lax.rem(jj, SLOT) // DEV + 1).astype(F32)
            hit = (picked == wanted) & (lax.rem(jj, DEV) == lax.rem(tok, DEV)) & (jj // (NX * SLOT) == tok // ROW)
            place = jnp.where(hit, 1.0, 0.0).astype(BF16)
            moved = nn(place, jnp.concatenate([ag_v[r, :, pl.ds(0, DAE)] for r in rows], axis=0)).astype(BF16)
            own = jnp.concatenate([place[i * NX * SLOT:i * NX * SLOT + SLOT] for i in range(n)], axis=0)
            shared = nn(own, jnp.concatenate([ag_v[r, :, pl.ds(DAE, NX * BX)] for r in rows], axis=0)).astype(BF16)
            for i, r in enumerate(rows):
                dsp_v[r] = moved[i * NX * SLOT:(i + 1) * NX * SLOT].reshape(NX, SLOT, DAE)
                shr_v[r] = shared[i * SLOT:(i + 1) * SLOT]
            for r in rows:
                for i in (2, 1, 3, 0):
                    send(dsp_v.at[r, i], d_v.at[r, :, d_at], s_dsp, r_row.at[r], idx(xwrap(x + i), z, 0))
                send(shr_v.at[r], d_v.at[r, :, pl.ds(NX * DAE, NX * BX)], s_shr, r_row.at[r], idx(x, z, 0))

        def returned(rows):
            for r in rows:
                arrived(act_v.at[r], r_row.at[r])
            return jnp.concatenate([act_v[r] for r in rows], axis=0)

        def down_blocks(rows, blocks):
            for o, w in blocks:
                at = pl.ds(o, w)
                part = nn(jnp.concatenate([act_v[r] for r in rows], axis=0), wd_v[:, o:o + w])
                for i, r in enumerate(rows):
                    part_v[r, :, at] = part[i * ROW:(i + 1) * ROW]

        def down_part(rows):
            returned(rows)
            down_blocks(rows, BLOCKS)

        def down_first():
            spread = returned([z])
            for o, w in BLOCKS:
                at = pl.ds(o, w)
                part_v[z, :, at] = nn(spread, wd_v[:, o:o + w]) + att_v[:, at]
        dispatch([z])

        def ag_step(k, carry):
            behind = list(up_down(k - 1))
            done = list(up_down(k - DOWN - 1))

            def pieces(i):
                for way in (early, 1 - early):
                    r = wrap(z - (1 - 2 * way) * k)
                    ag_wait(r, i, way, k)

                    @pl.when((way == 0) | (k < HALF - 1))
                    def _():
                        ag_send(r, i, way, k + 1)
            def follow(i):
                @pl.when(k > DOWN + 1)
                def _():
                    for way in (early, 1 - early):
                        chain_piece(rs2_in, rs2_out, s_rs2, slot_l, k - DOWN - 1, i, way)
            pieces(0)

            @pl.when(k >= 2)
            def _():
                dispatch(behind)
            pieces(1)

            @pl.when(k == DOWN)
            def _():
                arrived(wd_v.at[pl.ds(0, NX * UNITS), :], r_twin)
                down_first()

            @pl.when(k == DOWN + 1)
            def _():
                for i, (o, w) in enumerate(SUBS):
                    chain_send(rs2_in, rs2_out, s_rs2, slot_l, 0, 0, i, part_v[z, :, pl.ds(o, w)])

            @pl.when(k > DOWN + 1)
            def _():
                returned(done)
                down_blocks(done, BLOCKS[:1])
            pieces(2)

            @pl.when(k > DOWN + 1)
            def _():
                down_blocks(done, BLOCKS[1:])
            pieces(3)
            for i in range(NS):
                follow(i)
            return carry
        lax.fori_loop(1, HALF, ag_step, 0)
        dispatch(list(up_down(HALF - 1)))
        for i in range(NP):
            ag_wait(last, i, 0, HALF)
        dispatch([last])

        down_part(list(up_down(HALF - DOWN - 1)))

        def late(k, carry):
            chain_step(rs2_in, rs2_out, s_rs2, slot_l, k - 1)
            down_part(list(up_down(k)))
            return carry
        lax.fori_loop(HALF - DOWN, HALF, late, 0)
        chain_step(rs2_in, rs2_out, s_rs2, slot_l, HALF - 1)
        down_part([last])

        for t in range(TOK * JX, MSG):
            fin_v[pl.ds(t, DEV, stride=MSG), :] = jnp.zeros((DEV, 128), F32)
        for i, (o, w) in enumerate(SUBS):
            mixed = chain_end(rs2_in, slot_l, i)
            for t in range(TOK):
                for j in range(o // 128, (o + w) // 128):
                    fin_v[pl.ds(t * JX + j, DEV, stride=MSG), :] = (
                        mixed[t * DEV:(t + 1) * DEV, j * 128 - o:j * 128 - o + 128])
        fin_s[...] = fin_v[...].reshape(DEV, MSG, 128).astype(BF16)
        for i in range(DEV - 1):
            to = lax.rem(dev + i + 1, DEV)
            send(fin_s.at[to], sum_v.at[x], s_out, r_out, idx(to // NC, z, lax.rem(to, NC)))
        sum_v[x] = fin_s[dev]

        arrived(ctx_v, s_ctx.at[0])
        arrived(wo_v.at[pl.ds(0, 2 * (NX - 1) * (VH // NC)), :], s_wo)
        arrived(res_v.at[pl.ds(0, NX)], s_res)
        arrived(vu_v.at[pl.ds(0, VH // NC), :], s_core.at[0])
        arrived(wgu_v.at[:, pl.ds(0, UNITS)], s_core.at[1])
        arrived(wgu_v.at[:, pl.ds(0, UNITS)], s_core.at[2])
        arrived(wd_v.at[pl.ds(0, (NX - 1) * UNITS), :], s_wd.at[0])
        arrived(wd_v.at[pl.ds(0, NX * UNITS), :], s_wd.at[1])
        for way in range(2):
            arrived(rs_out.at[way, pl.ds(way, HALF - way)], s_rs.at[way])
            arrived(rs2_out.at[way, pl.ds(way, HALF - way)], s_rs2.at[way])
            arrived(ag_v.at[pl.ds(0, HALF - way)], s_ag.at[way])
        arrived(ag_v.at[z, :, pl.ds(DAE, (NX - 1) * BX)], s_bx)
        arrived(dsp_v, s_dsp)
        arrived(shr_v, s_shr)
        arrived(fin_s.at[pl.ds(0, DEV - 1)], s_out)
        arrived(sum_v.at[pl.ds(0, NX - 1)], r_out)

    resf_v[...] = sum_v[...].reshape(NX * MSG, 128).astype(F32) + resf_v[...]
    for t in range(TOK):
        rows = [resf_v[pl.ds(xx * MSG + t * JX, JX), :] for xx in range(NX)]
        outv_v[t] = jnp.concatenate(rows, axis=0).astype(BF16)
    out_copy = pltpu.make_async_copy(outv_v, out_ref, l_misc)
    out_copy.start()
    out_copy.wait()


def body(
    cache_kv, new_kv, queries, lengths, resid, value_up, out_proj, norm_gain, router, expert_ids, slots, w_gate, w_up,
    w_down,
):
    seqs, steps = resid.shape[:2]
    cache_len = cache_kv.shape[1]
    hbm = pl.BlockSpec(memory_space=pltpu.HBM)
    dma = pltpu.SemaphoreType.DMA
    regular = pltpu.SemaphoreType.REGULAR
    scratch = [
        pltpu.VMEM(new_kv.shape, BF16),
        pltpu.SMEM(lengths.shape, jnp.int32),
        pltpu.VMEM(resid.shape, BF16),
        pltpu.VMEM((D // 128, 128), BF16),
        pltpu.SMEM(expert_ids.shape, jnp.int32),
        pltpu.SMEM(slots.shape, jnp.int32),
        pltpu.VMEM((seqs, KV, cache_len), BF16),
        pltpu.VMEM((seqs, steps * H, KV), BF16),
        pltpu.VMEM((steps * H, cache_len), F32),
        pltpu.VMEM((H * 16, 128), F32),
        pltpu.VMEM((H, 16, 128), BF16),
        pltpu.VMEM((NZ, DEV, 16, 128), BF16),
        pltpu.VMEM((DEV * 16, 128), F32),
        pltpu.VMEM((VH, LAT), BF16),
        pltpu.VMEM((NZ, ROW, NX * VH), BF16),
        pltpu.VMEM((NX * VH, DX), BF16),
        pltpu.VMEM((H, 16, 128), BF16),
        pltpu.VMEM((VH // NC, D), BF16),
        pltpu.VMEM((2, HALF + 1, ROW, DX), BF16),
        pltpu.VMEM((2, HALF, ROW, DX), BF16),
        pltpu.VMEM((ROW, DX), F32),
        pltpu.VMEM((NX, MSG, 128), BF16),
        pltpu.VMEM((NX * MSG, 128), F32),
        pltpu.VMEM((DEV, MSG, 128), BF16),
        pltpu.VMEM((DEV * MSG, 128), F32),
        pltpu.VMEM((D // 128, 128), F32),
        pltpu.VMEM((128, DX), BF16),
        pltpu.VMEM((NZ, ROW, DG), BF16),
        pltpu.VMEM((NZ, NX, SLOT, DAE), BF16),
        pltpu.VMEM((NZ, SLOT, NX * BX), BF16),
        pltpu.VMEM((NZ, SLOT, NX * (DAE + BX)), BF16),
        pltpu.VMEM((D, 2 * NC * UNITS), BF16),
        pltpu.VMEM((NZ, ROW, NC * UNITS), BF16),
        pltpu.VMEM((NZ, ROW, NX * NC * UNITS), BF16),
        pltpu.VMEM((NX * NC * UNITS, DX), BF16),
        pltpu.VMEM((UNITS, D), BF16),
        pltpu.VMEM((2, HALF + 1, ROW, DX), BF16),
        pltpu.VMEM((2, HALF, ROW, DX), BF16),
        pltpu.VMEM((NZ, ROW, DX), F32),
        pltpu.VMEM((DEV * MSG, 128), F32),
        pltpu.VMEM((DEV, MSG, 128), BF16),
        pltpu.VMEM((NX, MSG, 128), BF16),
        pltpu.VMEM((TOK, NX * JX, 128), BF16),
        dma((seqs,)), dma, dma((3,)), dma((6,)),
        dma((2,)), dma, dma, dma((3,)), dma((2,)), dma, dma((2,)), dma((2,)), dma((2,)), dma, dma, dma, dma, dma,
        dma, dma, dma((NX, 2)), dma, dma((4,)), dma((2,)), dma((NZ,)), dma((2, 6, max(NP, NS))), dma, dma, dma,
        regular, regular,
    ]
    out = pl.pallas_call(
        kernel,
        out_shape=jax.ShapeDtypeStruct((TOK, NX * JX, 128), BF16),
        in_specs=[hbm] * 14,
        out_specs=hbm,
        scratch_shapes=scratch,
        compiler_params=pltpu.CompilerParams(
            collective_id=0, has_side_effects=True, vmem_limit_bytes=(64 << 20) - (64 << 10)),
        name="layer",
    )(
        jnp.transpose(cache_kv, (0, 2, 1)), new_kv, queries.reshape(seqs, steps * H, KV), lengths, resid,
        value_up.T, out_proj, norm_gain.reshape(D // 128, 128), router.T, expert_ids, slots, w_gate, w_up, w_down,
    )
    return out.reshape(resid.shape)


def solution(mesh):
    return jax.shard_map(
        body,
        mesh=mesh,
        in_specs=(
            P(("rep", "ep"), None, None),
            P(("rep", "ep"), None, None),
            P(("rep", "ep"), None, None, None),
            P(("rep", "ep")),
            P(("rep", "ep"), None, None),
            P(None, "ep"),
            P("ep", None),
            P(),
            P(),
            P(("rep", "ep"), None, None),
            P(("rep", "ep"), None, None),
            P(None, "ep"),
            P(None, "ep"),
            P("ep", None),
        ),
        out_specs=P(("rep", "ep"), None, None),
        check_vma=False,
    )
```

```python
import functools
import math

import jax
import jax.numpy as jnp
from jax import lax
from jax.experimental import pallas as pl
from jax.experimental.pallas import tpu as pltpu
from jax.sharding import PartitionSpec as P

NX, NZ, NC = 4, 16, 2
DEV = NX * NC
HALF = NZ // 2

D = 7168
H = 64
LAT = 512
VH = 128
KV = 576
EXPERTS = 16
TOP = 8
CAP = 2
QK = 192
TOK = 4
UNITS = 128
ROW = DEV * TOK
SLOT = DEV * CAP
DX = D // NX
EXT = 128
JX = DX // 128
MSG = 64
LANE_SUM = 32
LANE_TOK = 48
LANE_TAB = 64
QUAD = EXPERTS // NX
CHIPS_PER = NZ // QUAD

route_scale = 2.827
norm_eps = 1e-06

CUBE = 4

BX = 128
DA = DX - BX
DAE = DA + EXT
DG = DAE + NX * BX
PIECES = ((0, 640), (640, 512), (1152, 640), (1792, 512))
SUBS = ((DA, BX), (0, 256), (256, 256), (512, 256), (768, 256), (1024, 256), (1280, 384))
NS = len(SUBS)
NP = len(PIECES)
NPA = sum(o < DAE for o, _ in PIECES)
BLOCKS = ((0, 512), (512, 512), (1024, 768))
DOWN = 4

F32 = jnp.float32
BF16 = jnp.bfloat16


def mo(value, by):
    return pl.multiple_of(value, by)


def nt(a, b):
    return lax.dot_general(a, b, (((1,), (1,)), ((), ())), preferred_element_type=F32)


def nn(a, b):
    return lax.dot_general(a, b, (((1,), (0,)), ((), ())), preferred_element_type=F32)


def iota(shape, axis):
    return lax.broadcasted_iota(jnp.int32, shape, axis)


def kernel(
    cache_h, new_h, q_h, len_h, resid_h, vu_h, wo_h, gain_h, router_h, ids_h, slots_h, wg_h, wu_h, wd_h,
    out_ref,
    new_ref, len_ref, resid_ref, gain_ref, ids_ref, slots_ref,
    cache_v, q_v, score_v, stage_v, ctx_v, arr_v, arrf_v, vu_v, val_v, wo_v, ctxn_v, won_v, rs_in, rs_out, att_v,
    ress_v, resf_v, res_v, resw_v, gain_v, rout_v, ag_v, dsp_v, shr_v, d_v, wgu_v, act_s, act_v, wd_v, wdn_v, rs2_in, rs2_out,
    part_v, fin_v, fin_s, sum_v, outv_v,
    l_cache, l_misc, l_weights, l_small,
    s_ctx, s_res, s_wo, s_core, s_wd, s_val, s_rs, s_ag, s_rs2, s_dsp, s_act, s_out, s_bx, s_shr,
    r_res, r_wo, r_wox, r_woy, r_core, r_wd, r_row, r_ring, r_out, r_bx, r_twin,
    row_sem, all_sem,
):
    me = lax.axis_index("ep")
    c = lax.rem(me, NC)
    z = lax.rem(me // NC, NZ)
    x = me // (NC * NZ)
    dev = x * NC + c
    quad = z // CHIPS_PER
    group = lax.axis_index("rep")
    half = lax.rem(group, 2)
    twin = {"rep": group + 1 - 2 * half, "ep": me}

    def idx(xx, zz, cc):
        return {"ep": (xx * NZ + zz) * NC + cc}

    def wrap(zz):
        return lax.rem(zz + 2 * NZ, NZ)

    def xwrap(xx):
        return lax.rem(xx, NX)

    def send(src, dst, ssem, rsem, to):
        pltpu.make_async_remote_copy(src_ref=src, dst_ref=dst, send_sem=ssem, recv_sem=rsem, device_id=to).start()

    def arrived(ref, sem):
        pltpu.make_async_copy(ref, ref, sem).wait()

    main = c == 1
    side = c == 0

    loads = [pltpu.make_async_copy(q_h, q_v, l_misc)]
    loads += [pltpu.make_async_copy(cache_h.at[b], cache_v.at[b], l_cache.at[b]) for b in range(2)]
    small = [
        pltpu.make_async_copy(src, dst, l_small.at[i]) for i, (src, dst) in enumerate((
            (new_h, new_ref), (len_h, len_ref), (resid_h, resid_ref), (gain_h, gain_ref), (ids_h, ids_ref),
            (slots_h, slots_ref)))
    ]
    for load in loads[:2] + small[:2] + loads[2:] + small[2:]:
        load.start()

    bar = pltpu.get_barrier_semaphore()

    @pl.when(side)
    def _():
        def greet(o, carry):
            far = HALF - (o + 1) // 2
            zz = wrap(jnp.where(lax.rem(o, 2) == 1, z + far, z - far))
            for xx in range(NX):
                pl.semaphore_signal(bar, inc=1, device_id=idx(xx, zz, 1))
            return carry
        lax.fori_loop(0, NZ, greet, 0)

    @pl.when(main)
    def _():
        for xx in range(NX):
            pl.semaphore_signal(bar, inc=1, device_id=idx(xx, z, 0))
            pl.semaphore_signal(bar, inc=1, device_id=idx(xx, wrap(z + HALF), 1))
        for step in (1, -1):
            pl.semaphore_signal(bar, inc=1, device_id=idx(x, wrap(z + step), 1))
        pl.semaphore_signal(bar, inc=1, device_id=twin)

    gate_at = pl.ds(mo(c * UNITS, UNITS), UNITS)
    up_at = pl.ds(mo((NC + c) * UNITS, UNITS), UNITS)
    vu_at = pl.ds(mo(c * (VH // NC), VH // NC), VH // NC)
    router_copy = pltpu.make_async_copy(
        router_h.at[:, pl.ds(mo(x * DX, 128), DX)], rout_v.at[pl.ds(0, EXPERTS), :], l_weights.at[1])
    gate_copy = pltpu.make_async_copy(wg_h, wgu_v.at[:, gate_at], l_weights.at[1])
    up_copy = pltpu.make_async_copy(wu_h, wgu_v.at[:, up_at], l_weights.at[2])
    vu_copy = pltpu.make_async_copy(vu_h, vu_v.at[vu_at, :], l_weights.at[0])

    def wo_rows(xx, cc):
        return pl.ds(mo(xx * VH + cc * (VH // NC), VH // NC), VH // NC)

    def own_columns(xx):
        return pl.ds(mo(xx * DX, 128), DX)

    def wd_rows(xx, cc):
        return pl.ds(mo((xx * NC + cc) * UNITS, UNITS), UNITS)

    wo_copy = pltpu.make_async_copy(wo_h.at[:, own_columns(x)], wo_v.at[wo_rows(x, 1), :], l_weights.at[0])
    wd_copy = pltpu.make_async_copy(wd_h.at[:, own_columns(x)], wd_v.at[wd_rows(x, half), :], l_weights.at[2])

    def wo_half(xx, h):
        return pl.ds(mo(xx * DX + h * (DX // 2), 128), DX // 2)

    def wo_send(source):
        for h in range(2):
            for i in range(NX - 1):
                xx = xwrap(x + i + 1)
                send(source.at[:, wo_half(xx, h)], wo_v.at[wo_rows(x, half), wo_half(0, h)], s_wo, r_wox.at[x, h],
                     idx(xx, z, 1))

    def row_next():
        @pl.when(main & (half == 0))
        def _():
            arrived(won_v.at[:, pl.ds(0, (NX - 1) * DX)], r_core.at[2])
            wo_send(won_v)

    def row_start():
        @pl.when(side)
        def _():
            pl.semaphore_wait(bar, NX)
            pl.semaphore_signal(row_sem, inc=1, device_id=idx(x, z, 1))

        @pl.when(main)
        def _():
            pl.semaphore_wait(row_sem, 1)

        @pl.when(main)
        def _():
            @pl.when(half == 1)
            def _():
                wo_send(wo_h)
            wo_copy.start()
            send(vu_h, vu_v.at[vu_at, :], s_core.at[0], r_core.at[0], idx(x, z, 0))
            rout_v[...] = jnp.zeros_like(rout_v)
            router_copy.start()

        @pl.when(side)
        def _():
            vu_copy.start()
            @pl.when(half == 0)
            def _():
                for i in range(NX - 1):
                    columns = own_columns(xwrap(x + i + 1))
                    send(wo_h.at[:, columns], won_v.at[:, columns], s_core.at[0], r_core.at[2], idx(x, z, 1))
            send(wo_h.at[:, own_columns(x)], wo_v.at[wo_rows(x, 0), :], s_wo, r_wo, idx(x, z, 1))

    scale = 1.0 / math.sqrt(QK)
    blk = 512
    nblk = cache_v.shape[2] // blk
    loads[0].wait()
    small[0].wait()
    small[1].wait()
    for b in range(2):
        qb = q_v[b]
        qf = qb.astype(F32)
        step_of = iota((2 * H, 1), 0) // H
        new_rows = [new_ref[b, pl.ds(t, 1), :].astype(F32) for t in range(2)]
        s_new = [jnp.sum(qf * row, axis=1, keepdims=True) * scale for row in new_rows]
        s_new[1] = jnp.where(step_of >= 1, s_new[1], -jnp.inf)
        peak = jnp.maximum(s_new[0], s_new[1])
        loads[1 + b].wait()
        for p in range(nblk):
            sc = nn(qb, cache_v[b, :, pl.ds(p * blk, blk)]) * scale
            pos = iota((2 * H, blk), 1) + p * blk
            sc = jnp.where(pos < len_ref[b], sc, -jnp.inf)
            score_v[:, pl.ds(p * blk, blk)] = sc
            peak = jnp.maximum(peak, jnp.max(sc, axis=1, keepdims=True))
        if b == 0:
            row_start()
        else:
            row_next()
        p_new = [jnp.exp(s - peak) for s in s_new]
        total = p_new[0] + p_new[1]
        acc = p_new[0].astype(BF16).astype(F32) * new_rows[0][:, :LAT]
        acc = acc + p_new[1].astype(BF16).astype(F32) * new_rows[1][:, :LAT]
        for p in range(nblk):
            pr = jnp.exp(score_v[:, pl.ds(p * blk, blk)] - peak)
            total = total + jnp.sum(pr, axis=1, keepdims=True)
            acc = acc + nt(pr.astype(BF16), cache_v[b, pl.ds(0, LAT), pl.ds(p * blk, blk)])
        ctx = acc / total
        for s in range(2):
            for j in range(LAT // 128):
                stage_v[pl.ds(j * TOK + b * 2 + s, H, stride=16), :] = ctx[s * H:(s + 1) * H, j * 128:(j + 1) * 128]
    ctx_v[...] = stage_v[...].reshape(H, 16, 128).astype(BF16)

    @pl.when(main)
    def _():
        send(ctx_v, ctxn_v, s_ctx.at[0], r_core.at[1], idx(x, z, 0))
        pl.semaphore_wait(bar, NX * NZ + NX + 3)
        pl.semaphore_signal(all_sem, inc=1, device_id=idx(x, z, 0))

    @pl.when(side)
    def _():
        arrived(ctxn_v, r_core.at[1])
        pl.semaphore_wait(all_sem, 1)

    def near(o):
        return wrap(jnp.where(lax.rem(o, 2) == 1, z - (o + 1) // 2, z + o // 2))

    def ctx_send(o, carry):
        zz = near(o)
        for i in range(NX):
            xx = xwrap(x + i + 1)
            own = (zz == z) & (xx == x)
            for core, tiles in ((0, ctx_v), (1, ctxn_v)):
                @pl.when(jnp.logical_not(own))
                def _():
                    send(tiles.at[xx * NZ + zz], arr_v.at[z, x * NC + core], s_ctx.at[core], r_row.at[z],
                         idx(xx, zz, 0))

                @pl.when(own)
                def _():
                    arr_v[z, x * NC + core] = tiles[xx * NZ + zz]
        return carry

    @pl.when(side)
    def _():
        lax.fori_loop(0, NZ, ctx_send, 0)

        @pl.when(half == 0)
        def _():
            for i in range(NX - 1):
                columns = own_columns(xwrap(x + i + 1))
                send(wd_h.at[:, columns], wdn_v.at[:, columns], s_wd.at[0], r_core.at[0], idx(x, z, 1))
            send(wd_h.at[:, own_columns(x)], wd_v.at[wd_rows(x, half), :], s_wd.at[1], r_wd.at[0], idx(x, z, 1))

    @pl.when(main)
    def _():
        for h in range(2):
            for i in range(NX - 1):
                xx = i + jnp.where(x <= i, 1, 0)
                view = wo_v.at[wo_rows(xx, half), wo_half(0, h)]
                arrived(view, r_wox.at[xx, h])
                send(view, view, s_wo, r_woy, twin)

        def wd_send(source):
            for i in range(NX - 1):
                xx = xwrap(x + i + 1)
                send(source.at[:, own_columns(xx)], wd_v.at[wd_rows(x, half), :], s_wd.at[0], r_wd.at[1], idx(xx, z, 1))

        @pl.when(half == 0)
        def _():
            arrived(wdn_v.at[:, pl.ds(0, (NX - 1) * DX)], r_core.at[0])
            wd_send(wdn_v)

        @pl.when(half == 1)
        def _():
            wd_copy.start()
            wd_send(wd_h)
        send(wg_h, wgu_v.at[:, gate_at], s_core.at[1], r_core.at[2], idx(x, z, 0))
        send(wu_h, wgu_v.at[:, up_at], s_core.at[2], r_core.at[3], idx(x, z, 0))

    @pl.when(side)
    def _():
        gate_copy.start()
        up_copy.start()

    for load in small[2:]:
        load.wait()

    rows8, lanes8 = iota((8, 128), 0), iota((8, 128), 1)
    table = jnp.where(lanes8 == LANE_TOK, (rows8 + 1).astype(F32), 0.0)
    for t in range(TOK):
        for k in range(TOP):
            hit = (rows8 == t) & (lanes8 == ids_ref[t // 2, t % 2, k] + LANE_TAB)
            table = jnp.where(hit, (slots_ref[t // 2, t % 2, k] + 1).astype(F32), table)
    resf_v[...] = jnp.zeros_like(resf_v)
    for t in range(TOK):
        row = resid_ref[t // 2, pl.ds(t % 2, 1), :].astype(F32)
        for xx in range(NX):
            for j in range(JX):
                col = xx * DX + j * 128
                resf_v[pl.ds(xx * MSG + t * JX + j, 1), :] = row[:, col:col + 128]
    for xx in range(NX):
        resf_v[pl.ds(xx * MSG + TOK * JX, 8), :] = table
    ress_v[...] = resf_v[...].reshape(NX, MSG, 128).astype(BF16)

    def to_home():
        for i in range(NX):
            xx = xwrap(x + i)
            send(ress_v.at[xx], res_v.at[dev], s_res, r_res, idx(xx, wrap(z + HALF), 1))

    def up_down(k):
        return wrap(z - k), wrap(z + k)

    early = jnp.where(lax.rem(z, CUBE) < CUBE // 2, 1, 0)
    last = wrap(z + HALF)

    def along(way):
        return idx(x, wrap(z + 1 - 2 * way), c)

    def ways(pieces):
        for i in range(pieces + 1):
            if i < pieces:
                yield i, early
            if i > 0:
                yield i - 1, 1 - early

    def slot_r(s):
        return lax.rem(s, 3)

    def slot_l(s):
        return 3 + lax.rem(s, 3)

    def slot_g(k):
        return lax.rem(k + 2, 3)

    def chain_send(in_ref, out_buf, ssem, slot, way, s, i, total):
        at = pl.ds(*SUBS[i])
        out_buf[way, s, :, at] = total.astype(BF16)
        send(out_buf.at[way, s, :, at], in_ref.at[way, s + 1, :, at], ssem.at[way], r_ring.at[way, slot(s + 1), i],
             along(way))

    def chain_piece(in_ref, out_buf, ssem, slot, s, i, way):
        at = pl.ds(*SUBS[i])
        r = wrap(z - (1 - 2 * way) * s)

        @pl.when((way == 0) | (s >= 2))
        def _():
            arrived(in_ref.at[way, s, :, at], r_ring.at[way, slot(s), i])
        chain_send(in_ref, out_buf, ssem, slot, way, s, i, part_v[r, :, at] + in_ref[way, s, :, at].astype(F32))

    def chain_step(in_ref, out_buf, ssem, slot, s):
        for i, way in ways(NS):
            chain_piece(in_ref, out_buf, ssem, slot, s, i, way)

    def chain_end(in_ref, slot, i):
        at = pl.ds(*SUBS[i])
        for way in range(2):
            arrived(in_ref.at[way, HALF, :, at], r_ring.at[way, slot(HALF), i])
        return part_v[last, :, at] + in_ref[0, HALF, :, at].astype(F32) + in_ref[1, HALF, :, at].astype(F32)

    @pl.when(side)
    def _side():
        vu_copy.wait()
        arrived(vu_v.at[pl.ds(0, VH // NC), :], r_core.at[0])
        own_lanes = pl.ds(mo(x * VH, VH), VH)

        def ctx_row(r):
            @pl.when(r == z)
            def _():
                arrived(arr_v.at[r, pl.ds(0, DEV - NC)], r_row.at[r])

            @pl.when(r != z)
            def _():
                arrived(arr_v.at[r], r_row.at[r])

            arrf_v[...] = arr_v[r].reshape(DEV * 16, 128).astype(F32)
            cols = []
            for j in range(LAT // 128):
                cols.append(jnp.concatenate(
                    [arrf_v[pl.ds(j * TOK + t, DEV, stride=16), :] for t in range(TOK)], axis=0))
            rows = jnp.concatenate(cols, axis=1).astype(BF16)
            val_v[r, :, own_lanes] = nt(rows, vu_v[...]).astype(BF16)
            view = val_v.at[r, :, own_lanes]
            for i in range(NX):
                send(view, view, s_val, r_row.at[r], idx(xwrap(x + i + 1), z, 1))

        def ctx_step(o, carry):
            ctx_row(near(o))

            return carry
        lax.fori_loop(0, NZ, ctx_step, 0)
        to_home()

        gate_copy.wait()
        up_copy.wait()
        arrived(wgu_v.at[:, pl.ds(0, UNITS)], r_core.at[2])
        arrived(wgu_v.at[:, pl.ds(0, UNITS)], r_core.at[3])

        own_expert = x * QUAD + quad
        act_at = pl.ds(mo(x * NC * UNITS, 128), NC * UNITS)

        def experts(rows):
            for r in rows:
                arrived(d_v.at[r], r_row.at[r])
            both = jnp.zeros((SLOT * len(rows), 2 * NC * UNITS), F32)
            ext = jnp.zeros((SLOT * len(rows), EXT), F32)
            shared = jnp.concatenate([d_v[r, :, pl.ds(NX * DAE, NX * BX)] for r in rows], axis=0)
            for xx in range(NX):
                both = both + nn(
                    jnp.concatenate([d_v[r, :, pl.ds(xx * DAE, DA)] for r in rows], axis=0),
                    wgu_v[xx * DX:xx * DX + DA, :])
                both = both + nn(shared[:, xx * BX:(xx + 1) * BX], wgu_v[xx * DX + DA:(xx + 1) * DX, :])
                piece = jnp.concatenate([d_v[r, :, pl.ds(xx * DAE + DA, EXT)] for r in rows], axis=0)
                ext = ext + piece.astype(F32)
            n = len(rows)
            token = nt(jnp.where(iota((n * ROW, 128), 1) == LANE_TOK, 1.0, 0.0).astype(BF16), piece)
            piece = piece.astype(F32)
            jj, tok = iota(token.shape, 1), iota(token.shape, 0)
            wanted = (lax.rem(tok, ROW) // DEV + 1).astype(F32)
            hit = (token == wanted) & (lax.rem(jj, DEV) == lax.rem(tok, DEV)) & (jj // SLOT == tok // ROW)
            place = jnp.where(hit, 1.0, 0.0).astype(BF16)
            lane = iota(ext.shape, 1)
            squares = jnp.sum(
                jnp.where((lane == LANE_SUM) | (lane == LANE_SUM + 1), ext, 0.0), axis=1, keepdims=True)
            inv = lax.rsqrt(squares / D + norm_eps)
            logits = (ext + pltpu.roll(ext, EXT - EXPERTS, 1)) * inv
            named = (pltpu.roll(piece, EXT - LANE_TAB, 1) > 0.0) & (lane < EXPERTS)
            gates = jnp.where(named, 1.0 / (1.0 + jnp.exp(-logits)), 0.0)
            norm = jnp.sum(gates, axis=1, keepdims=True)
            mine = jnp.sum(jnp.where(lane == own_expert, gates, 0.0), axis=1, keepdims=True)
            share = jnp.where(norm > 0.0, route_scale * mine / norm, 0.0)
            gate = both[:, :NC * UNITS] * inv
            upward = both[:, NC * UNITS:] * inv
            act = (gate / (1.0 + jnp.exp(-gate)) * upward * share).astype(BF16)
            spread = nn(place, act).astype(BF16)
            for i, r in enumerate(rows):
                act_s[r] = spread[i * ROW:(i + 1) * ROW]
                for m in range(NX):
                    send(act_s.at[r], act_v.at[r, :, act_at], s_act, r_row.at[r], idx(xwrap(x + m + 1), z, 1))

        experts([z])

        def step(k, carry):
            experts(list(up_down(k)))
            return carry
        lax.fori_loop(1, HALF, step, 0)
        experts([last])

        arrived(ctx_v.at[pl.ds(0, NX * NZ - 1)], s_ctx.at[0])
        arrived(ctx_v.at[pl.ds(0, NX * NZ - 1)], s_ctx.at[1])
        @pl.when(half == 0)
        def _():
            arrived(won_v.at[:, pl.ds(0, (NX - 1) * DX)], s_core.at[0])
        arrived(wo_v.at[pl.ds(0, VH // NC), :], s_wo)
        arrived(res_v.at[pl.ds(0, NX)], s_res)

        @pl.when(half == 0)
        def _():
            arrived(wdn_v.at[:, pl.ds(0, (NX - 1) * DX)], s_wd.at[0])
            arrived(wdn_v.at[:, pl.ds(0, DX)], s_wd.at[1])
        arrived(val_v, s_val)
        arrived(act_v, s_act)
        arrived(sum_v, r_out)

    @pl.when(main)
    def _main():
        gain_v[...] = gain_ref[...].astype(F32)
        rs_in[1, 1] = jnp.zeros((ROW, DX), BF16)
        rs2_in[1, 1] = jnp.zeros((ROW, DX), BF16)

        def twin_send(xx):
            view = wd_v.at[wd_rows(xx, half), :]
            send(view, view, s_wd.at[1], r_twin, twin)

        @pl.when(half == 0)
        def _():
            arrived(wd_v.at[wd_rows(x, half), :], r_wd.at[0])

        @pl.when(half == 1)
        def _():
            wd_copy.wait()
        twin_send(x)

        wo_copy.wait()
        arrived(wo_v.at[wo_rows(x, 0), :], r_wo)
        arrived(wo_v.at[pl.ds(0, (NX - 1) * (VH // NC)), :], r_woy)
        to_home()

        def attended(rows):
            for r in rows:
                arrived(val_v.at[r], r_row.at[r])
            stacked = jnp.concatenate([val_v[r] for r in rows], axis=0)
            for o, w in BLOCKS:
                part = nn(stacked, wo_v[:, o:o + w])
                for i, r in enumerate(rows):
                    part_v[r, :, pl.ds(o, w)] = part[i * ROW:(i + 1) * ROW]

        arrived(val_v.at[z], r_row.at[z])
        for i, (o, w) in enumerate(SUBS):
            chain_send(rs_in, rs_out, s_rs, slot_r, 0, 0, i, nn(val_v[z], wo_v[:, o:o + w]))
        attended(list(up_down(1)))

        def rs_step(s, carry):
            chain_step(rs_in, rs_out, s_rs, slot_r, s)

            @pl.when(s < HALF - 1)
            def _():
                attended(list(up_down(s + 1)))

            @pl.when(s == HALF // 2)
            def _():
                arrived(wd_v.at[pl.ds(0, (NX - 1) * UNITS), :], r_wd.at[1])
                for i in range(NX - 1):
                    twin_send(xwrap(x + i + 1))
            return carry
        lax.fori_loop(1, HALF, rs_step, 0)
        attended([last])

        arrived(res_v, r_res)
        resw_v[...] = res_v[...].reshape(DEV * MSG, 128).astype(F32)
        lane = iota((ROW, 128), 1)
        tabs = [resw_v[pl.ds(TOK * JX + t, DEV, stride=MSG), :] for t in range(TOK)]
        table_rows = jnp.concatenate(tabs, axis=0)
        router_copy.wait()

        def ag_send(r, i, way, k):
            view = ag_v.at[r, :, pl.ds(*PIECES[i])]
            send(view, view, s_ag.at[way], r_ring.at[way, slot_g(k), i], along(way))

        def ag_wait(r, i, way, k):
            arrived(ag_v.at[r, :, pl.ds(*PIECES[i])], r_ring.at[way, slot_g(k), i])

        bx_at = pl.ds(mo(DAE + x * BX, 128), BX)
        sums = jnp.zeros((ROW, 1), F32)
        logits = jnp.zeros((ROW, 128), F32)
        for i, (o, w) in enumerate(SUBS):
            attn = chain_end(rs_in, slot_r, i)
            att_v[:, pl.ds(o, w)] = attn
            hidden = attn + jnp.concatenate([
                jnp.concatenate([resw_v[pl.ds(t * JX + j, DEV, stride=MSG), :] for t in range(TOK)], axis=0)
                for j in range(o // 128, (o + w) // 128)], axis=1)
            gain = jnp.concatenate(
                [gain_v[pl.ds(x * JX + j, 1), :] for j in range(o // 128, (o + w) // 128)], axis=1)
            scaled = (hidden * gain).astype(BF16)
            if i == 0:
                ag_v[z, :, bx_at] = scaled
                view = ag_v.at[z, :, bx_at]
                for j in (1, 0, 2):
                    send(view, view, s_bx, r_bx, idx(xwrap(x + j + 1), z, 1))
            else:
                ag_v[z, :, pl.ds(o, w)] = scaled
                for piece, (start, size) in enumerate(PIECES[:NPA - 1]):
                    if o < start + size <= o + w:
                        ag_send(z, piece, 0, 1)
                        ag_send(z, piece, 1, 1)
            sums = sums + jnp.sum(hidden * hidden, axis=1, keepdims=True)
            logits = logits + nt(scaled, rout_v[:, pl.ds(o, w)])
        high = logits.astype(BF16).astype(F32)
        sums_high = sums.astype(BF16).astype(F32)
        ext = high + pltpu.roll(logits - high, EXPERTS, 1)
        ext = jnp.where(lane == LANE_SUM, sums_high, ext)
        ext = jnp.where(lane == LANE_SUM + 1, sums - sums_high, ext)
        ag_v[z, :, pl.ds(DA, EXT)] = (ext + table_rows).astype(BF16)
        ag_send(z, NPA - 1, 0, 1)
        ag_send(z, NPA - 1, 1, 1)
        arrived(ag_v.at[z, :, pl.ds(DAE, (NX - 1) * BX)], r_bx)
        for i in range(NPA, NP):
            ag_send(z, i, 0, 1)
            ag_send(z, i, 1, 1)

        d_at = pl.ds(mo(x * DAE, 128), DAE)

        def dispatch(rows):
            n = len(rows)
            size = n * NX * SLOT
            jj, lane = iota((size, 128), 0), iota((size, 128), 1)
            wanted_lane = LANE_TAB + lax.rem(x + lax.rem(jj // SLOT, NX), NX) * QUAD + quad
            pick = jnp.where(lane == wanted_lane, 1.0, 0.0).astype(BF16)
            picked = nt(pick, jnp.concatenate([ag_v[r, :, pl.ds(DA, EXT)] for r in rows], axis=0))
            jj, tok = iota((size, n * ROW), 0), iota((size, n * ROW), 1)
            wanted = (lax.rem(jj, SLOT) // DEV + 1).astype(F32)
            hit = (picked == wanted) & (lax.rem(jj, DEV) == lax.rem(tok, DEV)) & (jj // (NX * SLOT) == tok // ROW)
            place = jnp.where(hit, 1.0, 0.0).astype(BF16)
            moved = nn(place, jnp.concatenate([ag_v[r, :, pl.ds(0, DAE)] for r in rows], axis=0)).astype(BF16)
            own = jnp.concatenate([place[i * NX * SLOT:i * NX * SLOT + SLOT] for i in range(n)], axis=0)
            shared = nn(own, jnp.concatenate([ag_v[r, :, pl.ds(DAE, NX * BX)] for r in rows], axis=0)).astype(BF16)
            for i, r in enumerate(rows):
                dsp_v[r] = moved[i * NX * SLOT:(i + 1) * NX * SLOT].reshape(NX, SLOT, DAE)
                shr_v[r] = shared[i * SLOT:(i + 1) * SLOT]
            for r in rows:
                for i in (2, 1, 3, 0):
                    send(dsp_v.at[r, i], d_v.at[r, :, d_at], s_dsp, r_row.at[r], idx(xwrap(x + i), z, 0))
                send(shr_v.at[r], d_v.at[r, :, pl.ds(NX * DAE, NX * BX)], s_shr, r_row.at[r], idx(x, z, 0))

        def returned(rows):
            for r in rows:
                arrived(act_v.at[r], r_row.at[r])
            return jnp.concatenate([act_v[r] for r in rows], axis=0)

        def down_blocks(rows, blocks):
            for o, w in blocks:
                at = pl.ds(o, w)
                part = nn(jnp.concatenate([act_v[r] for r in rows], axis=0), wd_v[:, o:o + w])
                for i, r in enumerate(rows):
                    part_v[r, :, at] = part[i * ROW:(i + 1) * ROW]

        def down_part(rows):
            returned(rows)
            down_blocks(rows, BLOCKS)

        def down_first():
            spread = returned([z])
            for o, w in BLOCKS:
                at = pl.ds(o, w)
                part_v[z, :, at] = nn(spread, wd_v[:, o:o + w]) + att_v[:, at]
        dispatch([z])

        def ag_step(k, carry):
            behind = list(up_down(k - 1))
            done = list(up_down(k - DOWN - 1))

            def pieces(i):
                for way in (early, 1 - early):
                    r = wrap(z - (1 - 2 * way) * k)
                    ag_wait(r, i, way, k)

                    @pl.when((way == 0) | (k < HALF - 1))
                    def _():
                        ag_send(r, i, way, k + 1)
            def follow(i):
                @pl.when(k > DOWN + 1)
                def _():
                    for way in (early, 1 - early):
                        chain_piece(rs2_in, rs2_out, s_rs2, slot_l, k - DOWN - 1, i, way)
            pieces(0)

            @pl.when(k >= 2)
            def _():
                dispatch(behind)
            pieces(1)

            @pl.when(k == DOWN)
            def _():
                arrived(wd_v.at[pl.ds(0, NX * UNITS), :], r_twin)
                down_first()

            @pl.when(k == DOWN + 1)
            def _():
                for i, (o, w) in enumerate(SUBS):
                    chain_send(rs2_in, rs2_out, s_rs2, slot_l, 0, 0, i, part_v[z, :, pl.ds(o, w)])

            @pl.when(k > DOWN + 1)
            def _():
                returned(done)
                down_blocks(done, BLOCKS[:1])
            pieces(2)

            @pl.when(k > DOWN + 1)
            def _():
                down_blocks(done, BLOCKS[1:])
            for i in range(NS):
                follow(i)
            pieces(3)
            return carry
        lax.fori_loop(1, HALF, ag_step, 0)
        dispatch(list(up_down(HALF - 1)))
        for i in range(NP):
            ag_wait(last, i, 0, HALF)
        dispatch([last])

        down_part(list(up_down(HALF - DOWN - 1)))

        def late(k, carry):
            chain_step(rs2_in, rs2_out, s_rs2, slot_l, k - 1)
            down_part(list(up_down(k)))
            return carry
        lax.fori_loop(HALF - DOWN, HALF, late, 0)
        chain_step(rs2_in, rs2_out, s_rs2, slot_l, HALF - 1)
        down_part([last])

        for t in range(TOK * JX, MSG):
            fin_v[pl.ds(t, DEV, stride=MSG), :] = jnp.zeros((DEV, 128), F32)
        for i, (o, w) in enumerate(SUBS):
            mixed = chain_end(rs2_in, slot_l, i)
            for t in range(TOK):
                for j in range(o // 128, (o + w) // 128):
                    fin_v[pl.ds(t * JX + j, DEV, stride=MSG), :] = (
                        mixed[t * DEV:(t + 1) * DEV, j * 128 - o:j * 128 - o + 128])
        fin_s[...] = fin_v[...].reshape(DEV, MSG, 128).astype(BF16)
        for i in range(DEV - 1):
            to = lax.rem(dev + i + 1, DEV)
            send(fin_s.at[to], sum_v.at[x], s_out, r_out, idx(to // NC, z, lax.rem(to, NC)))
        sum_v[x] = fin_s[dev]

        arrived(ctx_v, s_ctx.at[0])
        arrived(wo_v.at[pl.ds(0, 2 * (NX - 1) * (VH // NC)), :], s_wo)
        arrived(res_v.at[pl.ds(0, NX)], s_res)
        arrived(vu_v.at[pl.ds(0, VH // NC), :], s_core.at[0])
        arrived(wgu_v.at[:, pl.ds(0, UNITS)], s_core.at[1])
        arrived(wgu_v.at[:, pl.ds(0, UNITS)], s_core.at[2])
        arrived(wd_v.at[pl.ds(0, (NX - 1) * UNITS), :], s_wd.at[0])
        arrived(wd_v.at[pl.ds(0, NX * UNITS), :], s_wd.at[1])
        for way in range(2):
            arrived(rs_out.at[way, pl.ds(way, HALF - way)], s_rs.at[way])
            arrived(rs2_out.at[way, pl.ds(way, HALF - way)], s_rs2.at[way])
            arrived(ag_v.at[pl.ds(0, HALF - way)], s_ag.at[way])
        arrived(ag_v.at[z, :, pl.ds(DAE, (NX - 1) * BX)], s_bx)
        arrived(dsp_v, s_dsp)
        arrived(shr_v, s_shr)
        arrived(fin_s.at[pl.ds(0, DEV - 1)], s_out)
        arrived(sum_v.at[pl.ds(0, NX - 1)], r_out)

    resf_v[...] = sum_v[...].reshape(NX * MSG, 128).astype(F32) + resf_v[...]
    for t in range(TOK):
        rows = [resf_v[pl.ds(xx * MSG + t * JX, JX), :] for xx in range(NX)]
        outv_v[t] = jnp.concatenate(rows, axis=0).astype(BF16)
    out_copy = pltpu.make_async_copy(outv_v, out_ref, l_misc)
    out_copy.start()
    out_copy.wait()


def body(
    cache_kv, new_kv, queries, lengths, resid, value_up, out_proj, norm_gain, router, expert_ids, slots, w_gate, w_up,
    w_down,
):
    seqs, steps = resid.shape[:2]
    cache_len = cache_kv.shape[1]
    hbm = pl.BlockSpec(memory_space=pltpu.HBM)
    dma = pltpu.SemaphoreType.DMA
    regular = pltpu.SemaphoreType.REGULAR
    scratch = [
        pltpu.VMEM(new_kv.shape, BF16),
        pltpu.SMEM(lengths.shape, jnp.int32),
        pltpu.VMEM(resid.shape, BF16),
        pltpu.VMEM((D // 128, 128), BF16),
        pltpu.SMEM(expert_ids.shape, jnp.int32),
        pltpu.SMEM(slots.shape, jnp.int32),
        pltpu.VMEM((seqs, KV, cache_len), BF16),
        pltpu.VMEM((seqs, steps * H, KV), BF16),
        pltpu.VMEM((steps * H, cache_len), F32),
        pltpu.VMEM((H * 16, 128), F32),
        pltpu.VMEM((H, 16, 128), BF16),
        pltpu.VMEM((NZ, DEV, 16, 128), BF16),
        pltpu.VMEM((DEV * 16, 128), F32),
        pltpu.VMEM((VH, LAT), BF16),
        pltpu.VMEM((NZ, ROW, NX * VH), BF16),
        pltpu.VMEM((NX * VH, DX), BF16),
        pltpu.VMEM((H, 16, 128), BF16),
        pltpu.VMEM((VH // NC, D), BF16),
        pltpu.VMEM((2, HALF + 1, ROW, DX), BF16),
        pltpu.VMEM((2, HALF, ROW, DX), BF16),
        pltpu.VMEM((ROW, DX), F32),
        pltpu.VMEM((NX, MSG, 128), BF16),
        pltpu.VMEM((NX * MSG, 128), F32),
        pltpu.VMEM((DEV, MSG, 128), BF16),
        pltpu.VMEM((DEV * MSG, 128), F32),
        pltpu.VMEM((D // 128, 128), F32),
        pltpu.VMEM((128, DX), BF16),
        pltpu.VMEM((NZ, ROW, DG), BF16),
        pltpu.VMEM((NZ, NX, SLOT, DAE), BF16),
        pltpu.VMEM((NZ, SLOT, NX * BX), BF16),
        pltpu.VMEM((NZ, SLOT, NX * (DAE + BX)), BF16),
        pltpu.VMEM((D, 2 * NC * UNITS), BF16),
        pltpu.VMEM((NZ, ROW, NC * UNITS), BF16),
        pltpu.VMEM((NZ, ROW, NX * NC * UNITS), BF16),
        pltpu.VMEM((NX * NC * UNITS, DX), BF16),
        pltpu.VMEM((UNITS, D), BF16),
        pltpu.VMEM((2, HALF + 1, ROW, DX), BF16),
        pltpu.VMEM((2, HALF, ROW, DX), BF16),
        pltpu.VMEM((NZ, ROW, DX), F32),
        pltpu.VMEM((DEV * MSG, 128), F32),
        pltpu.VMEM((DEV, MSG, 128), BF16),
        pltpu.VMEM((NX, MSG, 128), BF16),
        pltpu.VMEM((TOK, NX * JX, 128), BF16),
        dma((seqs,)), dma, dma((3,)), dma((6,)),
        dma((2,)), dma, dma, dma((3,)), dma((2,)), dma, dma((2,)), dma((2,)), dma((2,)), dma, dma, dma, dma, dma,
        dma, dma, dma((NX, 2)), dma, dma((4,)), dma((2,)), dma((NZ,)), dma((2, 6, max(NP, NS))), dma, dma, dma,
        regular, regular,
    ]
    out = pl.pallas_call(
        kernel,
        out_shape=jax.ShapeDtypeStruct((TOK, NX * JX, 128), BF16),
        in_specs=[hbm] * 14,
        out_specs=hbm,
        scratch_shapes=scratch,
        compiler_params=pltpu.CompilerParams(
            collective_id=0, has_side_effects=True, vmem_limit_bytes=(64 << 20) - (64 << 10)),
        name="layer",
    )(
        jnp.transpose(cache_kv, (0, 2, 1)), new_kv, queries.reshape(seqs, steps * H, KV), lengths, resid,
        value_up.T, out_proj, norm_gain.reshape(D // 128, 128), router.T, expert_ids, slots, w_gate, w_up, w_down,
    )
    return out.reshape(resid.shape)


def solution(mesh):
    return jax.shard_map(
        body,
        mesh=mesh,
        in_specs=(
            P(("rep", "ep"), None, None),
            P(("rep", "ep"), None, None),
            P(("rep", "ep"), None, None, None),
            P(("rep", "ep")),
            P(("rep", "ep"), None, None),
            P(None, "ep"),
            P("ep", None),
            P(),
            P(),
            P(("rep", "ep"), None, None),
            P(("rep", "ep"), None, None),
            P(None, "ep"),
            P(None, "ep"),
            P("ep", None),
        ),
        out_specs=P(("rep", "ep"), None, None),
        check_vma=False,
    )
```

```python
import functools
import math

import jax
import jax.numpy as jnp
from jax import lax
from jax.experimental import pallas as pl
from jax.experimental.pallas import tpu as pltpu
from jax.sharding import PartitionSpec as P

NX, NZ, NC = 4, 16, 2
DEV = NX * NC
HALF = NZ // 2

D = 7168
H = 64
LAT = 512
VH = 128
KV = 576
EXPERTS = 16
TOP = 8
CAP = 2
QK = 192
TOK = 4
UNITS = 128
ROW = DEV * TOK
SLOT = DEV * CAP
DX = D // NX
EXT = 128
JX = DX // 128
MSG = 64
LANE_SUM = 32
LANE_TOK = 48
LANE_TAB = 64
QUAD = EXPERTS // NX
CHIPS_PER = NZ // QUAD

route_scale = 2.827
norm_eps = 1e-06

CUBE = 4

BX = 128
DA = DX - BX
DAE = DA + EXT
DG = DAE + NX * BX
PIECES = ((0, 640), (640, 512), (1152, 640), (1792, 512))
SUBS = ((DA, BX), (0, 256), (256, 256), (512, 256), (768, 256), (1024, 256), (1280, 384))
NS = len(SUBS)
NP = len(PIECES)
NPA = sum(o < DAE for o, _ in PIECES)
BLOCKS = ((0, 512), (512, 512), (1024, 768))
DOWN = 4

F32 = jnp.float32
BF16 = jnp.bfloat16


def mo(value, by):
    return pl.multiple_of(value, by)


def nt(a, b):
    return lax.dot_general(a, b, (((1,), (1,)), ((), ())), preferred_element_type=F32)


def nn(a, b):
    return lax.dot_general(a, b, (((1,), (0,)), ((), ())), preferred_element_type=F32)


def iota(shape, axis):
    return lax.broadcasted_iota(jnp.int32, shape, axis)


def kernel(
    cache_h, new_h, q_h, len_h, resid_h, vu_h, wo_h, gain_h, router_h, ids_h, slots_h, wg_h, wu_h, wd_h,
    out_ref,
    new_ref, len_ref, resid_ref, gain_ref, ids_ref, slots_ref,
    cache_v, q_v, score_v, stage_v, ctx_v, arr_v, arrf_v, vu_v, val_v, wo_v, ctxn_v, won_v, rs_in, rs_out, att_v,
    ress_v, resf_v, res_v, resw_v, gain_v, rout_v, ag_v, dsp_v, shr_v, d_v, wgu_v, act_s, act_v, wd_v, wdn_v, rs2_in, rs2_out,
    part_v, fin_v, fin_s, sum_v, outv_v,
    l_cache, l_misc, l_weights, l_small,
    s_ctx, s_res, s_wo, s_core, s_wd, s_val, s_rs, s_ag, s_rs2, s_dsp, s_act, s_out, s_bx, s_shr,
    r_res, r_wo, r_wox, r_woy, r_core, r_wd, r_row, r_ring, r_out, r_bx, r_twin,
    row_sem, all_sem,
):
    me = lax.axis_index("ep")
    c = lax.rem(me, NC)
    z = lax.rem(me // NC, NZ)
    x = me // (NC * NZ)
    dev = x * NC + c
    quad = z // CHIPS_PER
    group = lax.axis_index("rep")
    half = lax.rem(group, 2)
    twin = {"rep": group + 1 - 2 * half, "ep": me}

    def idx(xx, zz, cc):
        return {"ep": (xx * NZ + zz) * NC + cc}

    def wrap(zz):
        return lax.rem(zz + 2 * NZ, NZ)

    def xwrap(xx):
        return lax.rem(xx, NX)

    def send(src, dst, ssem, rsem, to):
        pltpu.make_async_remote_copy(src_ref=src, dst_ref=dst, send_sem=ssem, recv_sem=rsem, device_id=to).start()

    def arrived(ref, sem):
        pltpu.make_async_copy(ref, ref, sem).wait()

    main = c == 1
    side = c == 0

    loads = [pltpu.make_async_copy(q_h, q_v, l_misc)]
    loads += [pltpu.make_async_copy(cache_h.at[b], cache_v.at[b], l_cache.at[b]) for b in range(2)]
    small = [
        pltpu.make_async_copy(src, dst, l_small.at[i]) for i, (src, dst) in enumerate((
            (new_h, new_ref), (len_h, len_ref), (resid_h, resid_ref), (gain_h, gain_ref), (ids_h, ids_ref),
            (slots_h, slots_ref)))
    ]
    for load in loads[:2] + small[:2] + loads[2:] + small[2:]:
        load.start()

    bar = pltpu.get_barrier_semaphore()

    @pl.when(side)
    def _():
        def greet(o, carry):
            far = HALF - (o + 1) // 2
            zz = wrap(jnp.where(lax.rem(o, 2) == 1, z + far, z - far))
            for xx in range(NX):
                pl.semaphore_signal(bar, inc=1, device_id=idx(xx, zz, 1))
            return carry
        lax.fori_loop(0, NZ, greet, 0)

    @pl.when(main)
    def _():
        for xx in range(NX):
            pl.semaphore_signal(bar, inc=1, device_id=idx(xx, z, 0))
            pl.semaphore_signal(bar, inc=1, device_id=idx(xx, wrap(z + HALF), 1))
        for step in (1, -1):
            pl.semaphore_signal(bar, inc=1, device_id=idx(x, wrap(z + step), 1))
        pl.semaphore_signal(bar, inc=1, device_id=twin)

    gate_at = pl.ds(mo(c * UNITS, UNITS), UNITS)
    up_at = pl.ds(mo((NC + c) * UNITS, UNITS), UNITS)
    vu_at = pl.ds(mo(c * (VH // NC), VH // NC), VH // NC)
    router_copy = pltpu.make_async_copy(
        router_h.at[:, pl.ds(mo(x * DX, 128), DX)], rout_v.at[pl.ds(0, EXPERTS), :], l_weights.at[1])
    gate_copy = pltpu.make_async_copy(wg_h, wgu_v.at[:, gate_at], l_weights.at[1])
    up_copy = pltpu.make_async_copy(wu_h, wgu_v.at[:, up_at], l_weights.at[2])
    vu_copy = pltpu.make_async_copy(vu_h, vu_v.at[vu_at, :], l_weights.at[0])

    def wo_rows(xx, cc):
        return pl.ds(mo(xx * VH + cc * (VH // NC), VH // NC), VH // NC)

    def own_columns(xx):
        return pl.ds(mo(xx * DX, 128), DX)

    def wd_rows(xx, cc):
        return pl.ds(mo((xx * NC + cc) * UNITS, UNITS), UNITS)

    wo_copy = pltpu.make_async_copy(wo_h.at[:, own_columns(x)], wo_v.at[wo_rows(x, 1), :], l_weights.at[0])
    wd_copy = pltpu.make_async_copy(wd_h.at[:, own_columns(x)], wd_v.at[wd_rows(x, half), :], l_weights.at[2])

    def wo_half(xx, h):
        return pl.ds(mo(xx * DX + h * (DX // 2), 128), DX // 2)

    def wo_send(source):
        for h in range(2):
            for i in range(NX - 1):
                xx = xwrap(x + i + 1)
                send(source.at[:, wo_half(xx, h)], wo_v.at[wo_rows(x, half), wo_half(0, h)], s_wo, r_wox.at[x, h],
                     idx(xx, z, 1))

    def row_next():
        @pl.when(main & (half == 0))
        def _():
            arrived(won_v.at[:, pl.ds(0, (NX - 1) * DX)], r_core.at[2])
            wo_send(won_v)

    def row_start():
        @pl.when(side)
        def _():
            pl.semaphore_wait(bar, NX)
            pl.semaphore_signal(row_sem, inc=1, device_id=idx(x, z, 1))

        @pl.when(main)
        def _():
            pl.semaphore_wait(row_sem, 1)

        @pl.when(main)
        def _():
            @pl.when(half == 1)
            def _():
                wo_send(wo_h)
            wo_copy.start()
            send(vu_h, vu_v.at[vu_at, :], s_core.at[0], r_core.at[0], idx(x, z, 0))
            rout_v[...] = jnp.zeros_like(rout_v)
            router_copy.start()

        @pl.when(side)
        def _():
            vu_copy.start()
            @pl.when(half == 0)
            def _():
                for i in range(NX - 1):
                    columns = own_columns(xwrap(x + i + 1))
                    send(wo_h.at[:, columns], won_v.at[:, columns], s_core.at[0], r_core.at[2], idx(x, z, 1))
            send(wo_h.at[:, own_columns(x)], wo_v.at[wo_rows(x, 0), :], s_wo, r_wo, idx(x, z, 1))

    scale = 1.0 / math.sqrt(QK)
    blk = 512
    nblk = cache_v.shape[2] // blk
    loads[0].wait()
    small[0].wait()
    small[1].wait()
    for b in range(2):
        qb = q_v[b]
        qf = qb.astype(F32)
        step_of = iota((2 * H, 1), 0) // H
        new_rows = [new_ref[b, pl.ds(t, 1), :].astype(F32) for t in range(2)]
        s_new = [jnp.sum(qf * row, axis=1, keepdims=True) * scale for row in new_rows]
        s_new[1] = jnp.where(step_of >= 1, s_new[1], -jnp.inf)
        peak = jnp.maximum(s_new[0], s_new[1])
        loads[1 + b].wait()
        for p in range(nblk):
            sc = nn(qb, cache_v[b, :, pl.ds(p * blk, blk)]) * scale
            pos = iota((2 * H, blk), 1) + p * blk
            sc = jnp.where(pos < len_ref[b], sc, -jnp.inf)
            score_v[:, pl.ds(p * blk, blk)] = sc
            peak = jnp.maximum(peak, jnp.max(sc, axis=1, keepdims=True))
        if b == 0:
            row_start()
        else:
            row_next()
        p_new = [jnp.exp(s - peak) for s in s_new]
        total = p_new[0] + p_new[1]
        acc = p_new[0].astype(BF16).astype(F32) * new_rows[0][:, :LAT]
        acc = acc + p_new[1].astype(BF16).astype(F32) * new_rows[1][:, :LAT]
        for p in range(nblk):
            pr = jnp.exp(score_v[:, pl.ds(p * blk, blk)] - peak)
            total = total + jnp.sum(pr, axis=1, keepdims=True)
            acc = acc + nt(pr.astype(BF16), cache_v[b, pl.ds(0, LAT), pl.ds(p * blk, blk)])
        ctx = acc / total
        for s in range(2):
            for j in range(LAT // 128):
                stage_v[pl.ds(j * TOK + b * 2 + s, H, stride=16), :] = ctx[s * H:(s + 1) * H, j * 128:(j + 1) * 128]
    ctx_v[...] = stage_v[...].reshape(H, 16, 128).astype(BF16)

    @pl.when(main)
    def _():
        send(ctx_v, ctxn_v, s_ctx.at[0], r_core.at[1], idx(x, z, 0))
        pl.semaphore_wait(bar, NX * NZ + NX + 3)
        pl.semaphore_signal(all_sem, inc=1, device_id=idx(x, z, 0))

    @pl.when(side)
    def _():
        arrived(ctxn_v, r_core.at[1])
        pl.semaphore_wait(all_sem, 1)

    def near(o):
        return wrap(jnp.where(lax.rem(o, 2) == 1, z - (o + 1) // 2, z + o // 2))

    def ctx_send(o, carry):
        zz = near(o)
        for i in range(NX):
            xx = xwrap(x + i + 1)
            own = (zz == z) & (xx == x)
            for core, tiles in ((0, ctx_v), (1, ctxn_v)):
                @pl.when(jnp.logical_not(own))
                def _():
                    send(tiles.at[xx * NZ + zz], arr_v.at[z, x * NC + core], s_ctx.at[core], r_row.at[z],
                         idx(xx, zz, 0))

                @pl.when(own)
                def _():
                    arr_v[z, x * NC + core] = tiles[xx * NZ + zz]
        return carry

    @pl.when(side)
    def _():
        lax.fori_loop(0, NZ, ctx_send, 0)

        @pl.when(half == 0)
        def _():
            for i in range(NX - 1):
                columns = own_columns(xwrap(x + i + 1))
                send(wd_h.at[:, columns], wdn_v.at[:, columns], s_wd.at[0], r_core.at[0], idx(x, z, 1))
            send(wd_h.at[:, own_columns(x)], wd_v.at[wd_rows(x, half), :], s_wd.at[1], r_wd.at[0], idx(x, z, 1))

    @pl.when(main)
    def _():
        for h in range(2):
            for i in range(NX - 1):
                xx = i + jnp.where(x <= i, 1, 0)
                view = wo_v.at[wo_rows(xx, half), wo_half(0, h)]
                arrived(view, r_wox.at[xx, h])
                send(view, view, s_wo, r_woy, twin)

        def wd_send(source):
            for i in range(NX - 1):
                xx = xwrap(x + i + 1)
                send(source.at[:, own_columns(xx)], wd_v.at[wd_rows(x, half), :], s_wd.at[0], r_wd.at[1], idx(xx, z, 1))

        @pl.when(half == 0)
        def _():
            arrived(wdn_v.at[:, pl.ds(0, (NX - 1) * DX)], r_core.at[0])
            wd_send(wdn_v)

        @pl.when(half == 1)
        def _():
            wd_copy.start()
            wd_send(wd_h)
        send(wg_h, wgu_v.at[:, gate_at], s_core.at[1], r_core.at[2], idx(x, z, 0))
        send(wu_h, wgu_v.at[:, up_at], s_core.at[2], r_core.at[3], idx(x, z, 0))

    @pl.when(side)
    def _():
        gate_copy.start()
        up_copy.start()

    for load in small[2:]:
        load.wait()

    rows8, lanes8 = iota((8, 128), 0), iota((8, 128), 1)
    table = jnp.where(lanes8 == LANE_TOK, (rows8 + 1).astype(F32), 0.0)
    for t in range(TOK):
        for k in range(TOP):
            hit = (rows8 == t) & (lanes8 == ids_ref[t // 2, t % 2, k] + LANE_TAB)
            table = jnp.where(hit, (slots_ref[t // 2, t % 2, k] + 1).astype(F32), table)
    resf_v[...] = jnp.zeros_like(resf_v)
    for t in range(TOK):
        row = resid_ref[t // 2, pl.ds(t % 2, 1), :].astype(F32)
        for xx in range(NX):
            for j in range(JX):
                col = xx * DX + j * 128
                resf_v[pl.ds(xx * MSG + t * JX + j, 1), :] = row[:, col:col + 128]
    for xx in range(NX):
        resf_v[pl.ds(xx * MSG + TOK * JX, 8), :] = table
    ress_v[...] = resf_v[...].reshape(NX, MSG, 128).astype(BF16)

    def to_home():
        for i in range(NX):
            xx = xwrap(x + i)
            send(ress_v.at[xx], res_v.at[dev], s_res, r_res, idx(xx, wrap(z + HALF), 1))

    def up_down(k):
        return wrap(z - k), wrap(z + k)

    early = jnp.where(lax.rem(z, CUBE) < CUBE // 2, 1, 0)
    last = wrap(z + HALF)

    def along(way):
        return idx(x, wrap(z + 1 - 2 * way), c)

    def ways(pieces):
        for i in range(pieces + 1):
            if i < pieces:
                yield i, early
            if i > 0:
                yield i - 1, 1 - early

    def slot_r(s):
        return lax.rem(s, 3)

    def slot_l(s):
        return 3 + lax.rem(s, 3)

    def slot_g(k):
        return lax.rem(k + 2, 3)

    def chain_send(in_ref, out_buf, ssem, slot, way, s, i, total):
        at = pl.ds(*SUBS[i])
        out_buf[way, s, :, at] = total.astype(BF16)
        send(out_buf.at[way, s, :, at], in_ref.at[way, s + 1, :, at], ssem.at[way], r_ring.at[way, slot(s + 1), i],
             along(way))

    def chain_piece(in_ref, out_buf, ssem, slot, s, i, way):
        at = pl.ds(*SUBS[i])
        r = wrap(z - (1 - 2 * way) * s)

        @pl.when((way == 0) | (s >= 2))
        def _():
            arrived(in_ref.at[way, s, :, at], r_ring.at[way, slot(s), i])
        chain_send(in_ref, out_buf, ssem, slot, way, s, i, part_v[r, :, at] + in_ref[way, s, :, at].astype(F32))

    def chain_step(in_ref, out_buf, ssem, slot, s):
        for i, way in ways(NS):
            chain_piece(in_ref, out_buf, ssem, slot, s, i, way)

    def chain_end(in_ref, slot, i):
        at = pl.ds(*SUBS[i])
        for way in range(2):
            arrived(in_ref.at[way, HALF, :, at], r_ring.at[way, slot(HALF), i])
        return part_v[last, :, at] + in_ref[0, HALF, :, at].astype(F32) + in_ref[1, HALF, :, at].astype(F32)

    @pl.when(side)
    def _side():
        vu_copy.wait()
        arrived(vu_v.at[pl.ds(0, VH // NC), :], r_core.at[0])
        own_lanes = pl.ds(mo(x * VH, VH), VH)

        def ctx_row(r):
            @pl.when(r == z)
            def _():
                arrived(arr_v.at[r, pl.ds(0, DEV - NC)], r_row.at[r])

            @pl.when(r != z)
            def _():
                arrived(arr_v.at[r], r_row.at[r])

            arrf_v[...] = arr_v[r].reshape(DEV * 16, 128).astype(F32)
            cols = []
            for j in range(LAT // 128):
                cols.append(jnp.concatenate(
                    [arrf_v[pl.ds(j * TOK + t, DEV, stride=16), :] for t in range(TOK)], axis=0))
            rows = jnp.concatenate(cols, axis=1).astype(BF16)
            val_v[r, :, own_lanes] = nt(rows, vu_v[...]).astype(BF16)
            view = val_v.at[r, :, own_lanes]
            for i in (2, 1, 3, 0):
                send(view, view, s_val, r_row.at[r], idx(xwrap(x + i), z, 1))

        def ctx_step(o, carry):
            ctx_row(near(o))

            return carry
        lax.fori_loop(0, NZ, ctx_step, 0)
        to_home()

        gate_copy.wait()
        up_copy.wait()
        arrived(wgu_v.at[:, pl.ds(0, UNITS)], r_core.at[2])
        arrived(wgu_v.at[:, pl.ds(0, UNITS)], r_core.at[3])

        own_expert = x * QUAD + quad
        act_at = pl.ds(mo(x * NC * UNITS, 128), NC * UNITS)

        def experts(rows):
            for r in rows:
                arrived(d_v.at[r], r_row.at[r])
            both = jnp.zeros((SLOT * len(rows), 2 * NC * UNITS), F32)
            ext = jnp.zeros((SLOT * len(rows), EXT), F32)
            shared = jnp.concatenate([d_v[r, :, pl.ds(NX * DAE, NX * BX)] for r in rows], axis=0)
            for xx in range(NX):
                both = both + nn(
                    jnp.concatenate([d_v[r, :, pl.ds(xx * DAE, DA)] for r in rows], axis=0),
                    wgu_v[xx * DX:xx * DX + DA, :])
                both = both + nn(shared[:, xx * BX:(xx + 1) * BX], wgu_v[xx * DX + DA:(xx + 1) * DX, :])
                piece = jnp.concatenate([d_v[r, :, pl.ds(xx * DAE + DA, EXT)] for r in rows], axis=0)
                ext = ext + piece.astype(F32)
            n = len(rows)
            token = nt(jnp.where(iota((n * ROW, 128), 1) == LANE_TOK, 1.0, 0.0).astype(BF16), piece)
            piece = piece.astype(F32)
            jj, tok = iota(token.shape, 1), iota(token.shape, 0)
            wanted = (lax.rem(tok, ROW) // DEV + 1).astype(F32)
            hit = (token == wanted) & (lax.rem(jj, DEV) == lax.rem(tok, DEV)) & (jj // SLOT == tok // ROW)
            place = jnp.where(hit, 1.0, 0.0).astype(BF16)
            lane = iota(ext.shape, 1)
            squares = jnp.sum(
                jnp.where((lane == LANE_SUM) | (lane == LANE_SUM + 1), ext, 0.0), axis=1, keepdims=True)
            inv = lax.rsqrt(squares / D + norm_eps)
            logits = (ext + pltpu.roll(ext, EXT - EXPERTS, 1)) * inv
            named = (pltpu.roll(piece, EXT - LANE_TAB, 1) > 0.0) & (lane < EXPERTS)
            gates = jnp.where(named, 1.0 / (1.0 + jnp.exp(-logits)), 0.0)
            norm = jnp.sum(gates, axis=1, keepdims=True)
            mine = jnp.sum(jnp.where(lane == own_expert, gates, 0.0), axis=1, keepdims=True)
            share = jnp.where(norm > 0.0, route_scale * mine / norm, 0.0)
            gate = both[:, :NC * UNITS] * inv
            upward = both[:, NC * UNITS:] * inv
            act = (gate / (1.0 + jnp.exp(-gate)) * upward * share).astype(BF16)
            spread = nn(place, act).astype(BF16)
            for i, r in enumerate(rows):
                act_s[r] = spread[i * ROW:(i + 1) * ROW]
                for m in (2, 1, 3, 0):
                    send(act_s.at[r], act_v.at[r, :, act_at], s_act, r_row.at[r], idx(xwrap(x + m), z, 1))

        experts([z])

        def step(k, carry):
            experts(list(up_down(k)))
            return carry
        lax.fori_loop(1, HALF, step, 0)
        experts([last])

        arrived(ctx_v.at[pl.ds(0, NX * NZ - 1)], s_ctx.at[0])
        arrived(ctx_v.at[pl.ds(0, NX * NZ - 1)], s_ctx.at[1])
        @pl.when(half == 0)
        def _():
            arrived(won_v.at[:, pl.ds(0, (NX - 1) * DX)], s_core.at[0])
        arrived(wo_v.at[pl.ds(0, VH // NC), :], s_wo)
        arrived(res_v.at[pl.ds(0, NX)], s_res)

        @pl.when(half == 0)
        def _():
            arrived(wdn_v.at[:, pl.ds(0, (NX - 1) * DX)], s_wd.at[0])
            arrived(wdn_v.at[:, pl.ds(0, DX)], s_wd.at[1])
        arrived(val_v, s_val)
        arrived(act_v, s_act)
        arrived(sum_v, r_out)

    @pl.when(main)
    def _main():
        gain_v[...] = gain_ref[...].astype(F32)
        rs_in[1, 1] = jnp.zeros((ROW, DX), BF16)
        rs2_in[1, 1] = jnp.zeros((ROW, DX), BF16)

        def twin_send(xx):
            view = wd_v.at[wd_rows(xx, half), :]
            send(view, view, s_wd.at[1], r_twin, twin)

        @pl.when(half == 0)
        def _():
            arrived(wd_v.at[wd_rows(x, half), :], r_wd.at[0])

        @pl.when(half == 1)
        def _():
            wd_copy.wait()
        twin_send(x)

        wo_copy.wait()
        arrived(wo_v.at[wo_rows(x, 0), :], r_wo)
        arrived(wo_v.at[pl.ds(0, (NX - 1) * (VH // NC)), :], r_woy)
        to_home()

        def attended(rows):
            for r in rows:
                arrived(val_v.at[r], r_row.at[r])
            stacked = jnp.concatenate([val_v[r] for r in rows], axis=0)
            for o, w in BLOCKS:
                part = nn(stacked, wo_v[:, o:o + w])
                for i, r in enumerate(rows):
                    part_v[r, :, pl.ds(o, w)] = part[i * ROW:(i + 1) * ROW]

        arrived(val_v.at[z], r_row.at[z])
        for i, (o, w) in enumerate(SUBS):
            chain_send(rs_in, rs_out, s_rs, slot_r, 0, 0, i, nn(val_v[z], wo_v[:, o:o + w]))
        attended(list(up_down(1)))

        def rs_step(s, carry):
            chain_step(rs_in, rs_out, s_rs, slot_r, s)

            @pl.when(s < HALF - 1)
            def _():
                attended(list(up_down(s + 1)))

            @pl.when(s == HALF // 2)
            def _():
                arrived(wd_v.at[pl.ds(0, (NX - 1) * UNITS), :], r_wd.at[1])
                for i in range(NX - 1):
                    twin_send(xwrap(x + i + 1))
            return carry
        lax.fori_loop(1, HALF, rs_step, 0)
        attended([last])

        arrived(res_v, r_res)
        resw_v[...] = res_v[...].reshape(DEV * MSG, 128).astype(F32)
        lane = iota((ROW, 128), 1)
        tabs = [resw_v[pl.ds(TOK * JX + t, DEV, stride=MSG), :] for t in range(TOK)]
        table_rows = jnp.concatenate(tabs, axis=0)
        router_copy.wait()

        def ag_send(r, i, way, k):
            view = ag_v.at[r, :, pl.ds(*PIECES[i])]
            send(view, view, s_ag.at[way], r_ring.at[way, slot_g(k), i], along(way))

        def ag_wait(r, i, way, k):
            arrived(ag_v.at[r, :, pl.ds(*PIECES[i])], r_ring.at[way, slot_g(k), i])

        bx_at = pl.ds(mo(DAE + x * BX, 128), BX)
        sums = jnp.zeros((ROW, 1), F32)
        logits = jnp.zeros((ROW, 128), F32)
        for i, (o, w) in enumerate(SUBS):
            attn = chain_end(rs_in, slot_r, i)
            att_v[:, pl.ds(o, w)] = attn
            hidden = attn + jnp.concatenate([
                jnp.concatenate([resw_v[pl.ds(t * JX + j, DEV, stride=MSG), :] for t in range(TOK)], axis=0)
                for j in range(o // 128, (o + w) // 128)], axis=1)
            gain = jnp.concatenate(
                [gain_v[pl.ds(x * JX + j, 1), :] for j in range(o // 128, (o + w) // 128)], axis=1)
            scaled = (hidden * gain).astype(BF16)
            if i == 0:
                ag_v[z, :, bx_at] = scaled
                view = ag_v.at[z, :, bx_at]
                for j in (1, 0, 2):
                    send(view, view, s_bx, r_bx, idx(xwrap(x + j + 1), z, 1))
            else:
                ag_v[z, :, pl.ds(o, w)] = scaled
                for piece, (start, size) in enumerate(PIECES[:NPA - 1]):
                    if o < start + size <= o + w:
                        ag_send(z, piece, 0, 1)
                        ag_send(z, piece, 1, 1)
            sums = sums + jnp.sum(hidden * hidden, axis=1, keepdims=True)
            logits = logits + nt(scaled, rout_v[:, pl.ds(o, w)])
        high = logits.astype(BF16).astype(F32)
        sums_high = sums.astype(BF16).astype(F32)
        ext = high + pltpu.roll(logits - high, EXPERTS, 1)
        ext = jnp.where(lane == LANE_SUM, sums_high, ext)
        ext = jnp.where(lane == LANE_SUM + 1, sums - sums_high, ext)
        ag_v[z, :, pl.ds(DA, EXT)] = (ext + table_rows).astype(BF16)
        ag_send(z, NPA - 1, 0, 1)
        ag_send(z, NPA - 1, 1, 1)
        arrived(ag_v.at[z, :, pl.ds(DAE, (NX - 1) * BX)], r_bx)
        for i in range(NPA, NP):
            ag_send(z, i, 0, 1)
            ag_send(z, i, 1, 1)

        d_at = pl.ds(mo(x * DAE, 128), DAE)

        def dispatch(rows):
            n = len(rows)
            size = n * NX * SLOT
            jj, lane = iota((size, 128), 0), iota((size, 128), 1)
            wanted_lane = LANE_TAB + lax.rem(x + lax.rem(jj // SLOT, NX), NX) * QUAD + quad
            pick = jnp.where(lane == wanted_lane, 1.0, 0.0).astype(BF16)
            picked = nt(pick, jnp.concatenate([ag_v[r, :, pl.ds(DA, EXT)] for r in rows], axis=0))
            jj, tok = iota((size, n * ROW), 0), iota((size, n * ROW), 1)
            wanted = (lax.rem(jj, SLOT) // DEV + 1).astype(F32)
            hit = (picked == wanted) & (lax.rem(jj, DEV) == lax.rem(tok, DEV)) & (jj // (NX * SLOT) == tok // ROW)
            place = jnp.where(hit, 1.0, 0.0).astype(BF16)
            moved = nn(place, jnp.concatenate([ag_v[r, :, pl.ds(0, DAE)] for r in rows], axis=0)).astype(BF16)
            own = jnp.concatenate([place[i * NX * SLOT:i * NX * SLOT + SLOT] for i in range(n)], axis=0)
            shared = nn(own, jnp.concatenate([ag_v[r, :, pl.ds(DAE, NX * BX)] for r in rows], axis=0)).astype(BF16)
            for i, r in enumerate(rows):
                dsp_v[r] = moved[i * NX * SLOT:(i + 1) * NX * SLOT].reshape(NX, SLOT, DAE)
                shr_v[r] = shared[i * SLOT:(i + 1) * SLOT]
            for r in rows:
                for i in (2, 1, 3, 0):
                    send(dsp_v.at[r, i], d_v.at[r, :, d_at], s_dsp, r_row.at[r], idx(xwrap(x + i), z, 0))
                send(shr_v.at[r], d_v.at[r, :, pl.ds(NX * DAE, NX * BX)], s_shr, r_row.at[r], idx(x, z, 0))

        def returned(rows):
            for r in rows:
                arrived(act_v.at[r], r_row.at[r])
            return jnp.concatenate([act_v[r] for r in rows], axis=0)

        def down_blocks(rows, blocks):
            for o, w in blocks:
                at = pl.ds(o, w)
                part = nn(jnp.concatenate([act_v[r] for r in rows], axis=0), wd_v[:, o:o + w])
                for i, r in enumerate(rows):
                    part_v[r, :, at] = part[i * ROW:(i + 1) * ROW]

        def down_part(rows):
            returned(rows)
            down_blocks(rows, BLOCKS)

        def down_first():
            spread = returned([z])
            for o, w in BLOCKS:
                at = pl.ds(o, w)
                part_v[z, :, at] = nn(spread, wd_v[:, o:o + w]) + att_v[:, at]
        dispatch([z])

        def ag_step(k, carry):
            behind = list(up_down(k - 1))
            done = list(up_down(k - DOWN - 1))

            def pieces(i):
                for way in (early, 1 - early):
                    r = wrap(z - (1 - 2 * way) * k)
                    ag_wait(r, i, way, k)

                    @pl.when((way == 0) | (k < HALF - 1))
                    def _():
                        ag_send(r, i, way, k + 1)
            def follow(i):
                @pl.when(k > DOWN + 1)
                def _():
                    for way in (early, 1 - early):
                        chain_piece(rs2_in, rs2_out, s_rs2, slot_l, k - DOWN - 1, i, way)
            pieces(0)

            @pl.when(k >= 2)
            def _():
                dispatch(behind)
            pieces(1)

            @pl.when(k == DOWN)
            def _():
                arrived(wd_v.at[pl.ds(0, NX * UNITS), :], r_twin)
                down_first()

            @pl.when(k == DOWN + 1)
            def _():
                for i, (o, w) in enumerate(SUBS):
                    chain_send(rs2_in, rs2_out, s_rs2, slot_l, 0, 0, i, part_v[z, :, pl.ds(o, w)])

            @pl.when(k > DOWN + 1)
            def _():
                returned(done)
                down_blocks(done, BLOCKS[:1])
            pieces(2)

            @pl.when(k > DOWN + 1)
            def _():
                down_blocks(done, BLOCKS[1:])
            for i in range(NS):
                follow(i)
            pieces(3)
            return carry
        lax.fori_loop(1, HALF, ag_step, 0)
        dispatch(list(up_down(HALF - 1)))
        for i in range(NP):
            ag_wait(last, i, 0, HALF)
        dispatch([last])

        down_part(list(up_down(HALF - DOWN - 1)))

        def late(k, carry):
            chain_step(rs2_in, rs2_out, s_rs2, slot_l, k - 1)
            down_part(list(up_down(k)))
            return carry
        lax.fori_loop(HALF - DOWN, HALF, late, 0)
        chain_step(rs2_in, rs2_out, s_rs2, slot_l, HALF - 1)
        down_part([last])

        for t in range(TOK * JX, MSG):
            fin_v[pl.ds(t, DEV, stride=MSG), :] = jnp.zeros((DEV, 128), F32)
        for i, (o, w) in enumerate(SUBS):
            mixed = chain_end(rs2_in, slot_l, i)
            for t in range(TOK):
                for j in range(o // 128, (o + w) // 128):
                    fin_v[pl.ds(t * JX + j, DEV, stride=MSG), :] = (
                        mixed[t * DEV:(t + 1) * DEV, j * 128 - o:j * 128 - o + 128])
        fin_s[...] = fin_v[...].reshape(DEV, MSG, 128).astype(BF16)
        for i in (4, 3, 5, 2, 6, 1, 7):
            to = lax.rem(dev + i, DEV)
            send(fin_s.at[to], sum_v.at[x], s_out, r_out, idx(to // NC, z, lax.rem(to, NC)))
        sum_v[x] = fin_s[dev]

        arrived(ctx_v, s_ctx.at[0])
        arrived(wo_v.at[pl.ds(0, 2 * (NX - 1) * (VH // NC)), :], s_wo)
        arrived(res_v.at[pl.ds(0, NX)], s_res)
        arrived(vu_v.at[pl.ds(0, VH // NC), :], s_core.at[0])
        arrived(wgu_v.at[:, pl.ds(0, UNITS)], s_core.at[1])
        arrived(wgu_v.at[:, pl.ds(0, UNITS)], s_core.at[2])
        arrived(wd_v.at[pl.ds(0, (NX - 1) * UNITS), :], s_wd.at[0])
        arrived(wd_v.at[pl.ds(0, NX * UNITS), :], s_wd.at[1])
        for way in range(2):
            arrived(rs_out.at[way, pl.ds(way, HALF - way)], s_rs.at[way])
            arrived(rs2_out.at[way, pl.ds(way, HALF - way)], s_rs2.at[way])
            arrived(ag_v.at[pl.ds(0, HALF - way)], s_ag.at[way])
        arrived(ag_v.at[z, :, pl.ds(DAE, (NX - 1) * BX)], s_bx)
        arrived(dsp_v, s_dsp)
        arrived(shr_v, s_shr)
        arrived(fin_s.at[pl.ds(0, DEV - 1)], s_out)
        arrived(sum_v.at[pl.ds(0, NX - 1)], r_out)

    resf_v[...] = sum_v[...].reshape(NX * MSG, 128).astype(F32) + resf_v[...]
    for t in range(TOK):
        rows = [resf_v[pl.ds(xx * MSG + t * JX, JX), :] for xx in range(NX)]
        outv_v[t] = jnp.concatenate(rows, axis=0).astype(BF16)
    out_copy = pltpu.make_async_copy(outv_v, out_ref, l_misc)
    out_copy.start()
    out_copy.wait()


def body(
    cache_kv, new_kv, queries, lengths, resid, value_up, out_proj, norm_gain, router, expert_ids, slots, w_gate, w_up,
    w_down,
):
    seqs, steps = resid.shape[:2]
    cache_len = cache_kv.shape[1]
    hbm = pl.BlockSpec(memory_space=pltpu.HBM)
    dma = pltpu.SemaphoreType.DMA
    regular = pltpu.SemaphoreType.REGULAR
    scratch = [
        pltpu.VMEM(new_kv.shape, BF16),
        pltpu.SMEM(lengths.shape, jnp.int32),
        pltpu.VMEM(resid.shape, BF16),
        pltpu.VMEM((D // 128, 128), BF16),
        pltpu.SMEM(expert_ids.shape, jnp.int32),
        pltpu.SMEM(slots.shape, jnp.int32),
        pltpu.VMEM((seqs, KV, cache_len), BF16),
        pltpu.VMEM((seqs, steps * H, KV), BF16),
        pltpu.VMEM((steps * H, cache_len), F32),
        pltpu.VMEM((H * 16, 128), F32),
        pltpu.VMEM((H, 16, 128), BF16),
        pltpu.VMEM((NZ, DEV, 16, 128), BF16),
        pltpu.VMEM((DEV * 16, 128), F32),
        pltpu.VMEM((VH, LAT), BF16),
        pltpu.VMEM((NZ, ROW, NX * VH), BF16),
        pltpu.VMEM((NX * VH, DX), BF16),
        pltpu.VMEM((H, 16, 128), BF16),
        pltpu.VMEM((VH // NC, D), BF16),
        pltpu.VMEM((2, HALF + 1, ROW, DX), BF16),
        pltpu.VMEM((2, HALF, ROW, DX), BF16),
        pltpu.VMEM((ROW, DX), F32),
        pltpu.VMEM((NX, MSG, 128), BF16),
        pltpu.VMEM((NX * MSG, 128), F32),
        pltpu.VMEM((DEV, MSG, 128), BF16),
        pltpu.VMEM((DEV * MSG, 128), F32),
        pltpu.VMEM((D // 128, 128), F32),
        pltpu.VMEM((128, DX), BF16),
        pltpu.VMEM((NZ, ROW, DG), BF16),
        pltpu.VMEM((NZ, NX, SLOT, DAE), BF16),
        pltpu.VMEM((NZ, SLOT, NX * BX), BF16),
        pltpu.VMEM((NZ, SLOT, NX * (DAE + BX)), BF16),
        pltpu.VMEM((D, 2 * NC * UNITS), BF16),
        pltpu.VMEM((NZ, ROW, NC * UNITS), BF16),
        pltpu.VMEM((NZ, ROW, NX * NC * UNITS), BF16),
        pltpu.VMEM((NX * NC * UNITS, DX), BF16),
        pltpu.VMEM((UNITS, D), BF16),
        pltpu.VMEM((2, HALF + 1, ROW, DX), BF16),
        pltpu.VMEM((2, HALF, ROW, DX), BF16),
        pltpu.VMEM((NZ, ROW, DX), F32),
        pltpu.VMEM((DEV * MSG, 128), F32),
        pltpu.VMEM((DEV, MSG, 128), BF16),
        pltpu.VMEM((NX, MSG, 128), BF16),
        pltpu.VMEM((TOK, NX * JX, 128), BF16),
        dma((seqs,)), dma, dma((3,)), dma((6,)),
        dma((2,)), dma, dma, dma((3,)), dma((2,)), dma, dma((2,)), dma((2,)), dma((2,)), dma, dma, dma, dma, dma,
        dma, dma, dma((NX, 2)), dma, dma((4,)), dma((2,)), dma((NZ,)), dma((2, 6, max(NP, NS))), dma, dma, dma,
        regular, regular,
    ]
    out = pl.pallas_call(
        kernel,
        out_shape=jax.ShapeDtypeStruct((TOK, NX * JX, 128), BF16),
        in_specs=[hbm] * 14,
        out_specs=hbm,
        scratch_shapes=scratch,
        compiler_params=pltpu.CompilerParams(
            collective_id=0, has_side_effects=True, vmem_limit_bytes=(64 << 20) - (64 << 10)),
        name="layer",
    )(
        jnp.transpose(cache_kv, (0, 2, 1)), new_kv, queries.reshape(seqs, steps * H, KV), lengths, resid,
        value_up.T, out_proj, norm_gain.reshape(D // 128, 128), router.T, expert_ids, slots, w_gate, w_up, w_down,
    )
    return out.reshape(resid.shape)


def solution(mesh):
    return jax.shard_map(
        body,
        mesh=mesh,
        in_specs=(
            P(("rep", "ep"), None, None),
            P(("rep", "ep"), None, None),
            P(("rep", "ep"), None, None, None),
            P(("rep", "ep")),
            P(("rep", "ep"), None, None),
            P(None, "ep"),
            P("ep", None),
            P(),
            P(),
            P(("rep", "ep"), None, None),
            P(("rep", "ep"), None, None),
            P(None, "ep"),
            P(None, "ep"),
            P("ep", None),
        ),
        out_specs=P(("rep", "ep"), None, None),
        check_vma=False,
    )
```
